128 devices in a mesh: rep: 1, dp: 128 (over x, y, z, core).
Axes of the slice: x: 4, y: 4, z: 4, core: 2. Of those that a mesh axis runs over, the one named last changes fastest.
Arguments:
- x: bfloat16 [128, 1024, 640], P(('rep', 'dp'))
- dy: bfloat16 [128, 1024, 640], P(('rep', 'dp'))
- wq: bfloat16 [1, 640, 1024], replicated
- wk: bfloat16 [1, 640, 128], replicated
- wv: bfloat16 [1, 640, 128], replicated
- wo: bfloat16 [1, 1024, 640], replicated
- w_gate: bfloat16 [1, 640, 3200], replicated
- w_up: bfloat16 [1, 640, 3200], replicated
- w_down: bfloat16 [1, 3200, 640], replicated
- m_wq: float32 [1, 640, 1024], P(None, 'dp')
- m_wk: float32 [1, 640, 128], P(None, 'dp')
- m_wv: float32 [1, 640, 128], P(None, 'dp')
- m_wo: float32 [1, 1024, 640], P(None, 'dp')
- m_w_gate: float32 [1, 640, 3200], P(None, 'dp')
- m_w_up: float32 [1, 640, 3200], P(None, 'dp')
- m_w_down: float32 [1, 3200, 640], P(None, 'dp')
- v_wq: float32 [1, 640, 1024], P(None, 'dp')
- v_wk: float32 [1, 640, 128], P(None, 'dp')
- v_wv: float32 [1, 640, 128], P(None, 'dp')
- v_wo: float32 [1, 1024, 640], P(None, 'dp')
- v_w_gate: float32 [1, 640, 3200], P(None, 'dp')
- v_w_up: float32 [1, 640, 3200], P(None, 'dp')
- v_w_down: float32 [1, 3200, 640], P(None, 'dp')
Outputs:
- output 1: bfloat16 [1, 640, 1024], P('rep')
- output 2: bfloat16 [1, 640, 128], P('rep')
- output 3: bfloat16 [1, 640, 128], P('rep')
- output 4: bfloat16 [1, 1024, 640], P('rep')
- output 5: bfloat16 [1, 640, 3200], P('rep')
- output 6: bfloat16 [1, 640, 3200], P('rep')
- output 7: bfloat16 [1, 3200, 640], P('rep')
- output 8: float32 [1, 640, 1024], P('rep', 'dp')
- output 9: float32 [1, 640, 128], P('rep', 'dp')
- output 10: float32 [1, 640, 128], P('rep', 'dp')
- output 11: float32 [1, 1024, 640], P('rep', 'dp')
- output 12: float32 [1, 640, 3200], P('rep', 'dp')
- output 13: float32 [1, 640, 3200], P('rep', 'dp')
- output 14: float32 [1, 3200, 640], P('rep', 'dp')
- output 15: float32 [1, 640, 1024], P('rep', 'dp')
- output 16: float32 [1, 640, 128], P('rep', 'dp')
- output 17: float32 [1, 640, 128], P('rep', 'dp')
- output 18: float32 [1, 1024, 640], P('rep', 'dp')
- output 19: float32 [1, 640, 3200], P('rep', 'dp')
- output 20: float32 [1, 640, 3200], P('rep', 'dp')
- output 21: float32 [1, 3200, 640], P('rep', 'dp')
All inputs are finite; a program needn't handle non-finite values.
Results may differ from the reference program's by a relative error of at most 0.0254.
Values are sent between devices in bfloat16 or wider.
A program may use at most 1.5 GiB of HBM per device.

```python
import jax
import jax.numpy as jnp
from jax import lax

SEQUENCES = 128
TOKENS = 1024
D = 640
HEADS = 8
KV_HEADS = 1
HEAD = 128
FF = 3200
LAYERS = 1
THETA = 10000
NAMES = ("wq", "wk", "wv", "wo", "w_gate", "w_up", "w_down")
SHAPES = {
    "wq": (LAYERS, D, HEADS * HEAD),
    "wk": (LAYERS, D, KV_HEADS * HEAD),
    "wv": (LAYERS, D, KV_HEADS * HEAD),
    "wo": (LAYERS, HEADS * HEAD, D),
    "w_gate": (LAYERS, D, FF),
    "w_up": (LAYERS, D, FF),
    "w_down": (LAYERS, FF, D),
}


def bump(key, n, height):
    away = (jnp.arange(n, dtype=jnp.int32) - jax.random.randint(key, (), 0, n, jnp.int32)) % n
    return jnp.where(away < n // 8, height, 1.0)


def together(key, own, strength):
    shared = jax.random.normal(key, own.shape[1:], jnp.float32)
    return (own + strength * shared) * lax.rsqrt(1 + strength * strength)


def setup_inputs(seed: int = 0, part: int = 0) -> dict:
    kx, kdy, ka, kb, kz, kf, kh, kl, *keys = jax.random.split(jax.random.key(seed), 8 + 3 * len(NAMES))
    kx, kdy, ka, kb = (jax.random.fold_in(k, part) for k in (kx, kdy, ka, kb))
    kw, km, kv = (keys[i::3] for i in range(3))
    shape = (SEQUENCES, TOKENS, D)
    much_x, much_dy = jax.random.uniform(kz, (2,), jnp.float32, 0.0, 1.0)
    loud = 2.0 ** jax.random.uniform(jax.random.fold_in(kz, 1), (), jnp.float32, -1.0, 2.0)
    layers = 2.0 ** jax.random.uniform(kl, (LAYERS, 1, 1), jnp.float32, -1.0, 1.0)
    times = {"wq": 1.0, "wk": 1.0, "wv": 2.0, "wo": layers, "w_gate": 1.0, "w_up": bump(kh, FF, 4.0), "w_down": layers}
    x = together(ka, jax.random.normal(kx, shape, jnp.float32), much_x) * bump(kf, D, 4.0)
    dy = together(kb, jax.random.normal(kdy, shape, jnp.float32), much_dy)
    drawn = {"x": x.astype(jnp.bfloat16), "dy": (loud * dy * (SEQUENCES * TOKENS) ** -0.5).astype(jnp.bfloat16)}
    for key, name in zip(kw, NAMES, strict=True):
        drawn[name] = (jax.random.normal(key, SHAPES[name], jnp.float32) * SHAPES[name][1] ** -0.5 * times[name]).astype(jnp.bfloat16)
    for key, name in zip(km, NAMES, strict=True):
        drawn[f"m_{name}"] = 0.1 * jax.random.normal(key, SHAPES[name], jnp.float32)
    for key, name in zip(kv, NAMES, strict=True):
        drawn[f"v_{name}"] = jax.random.uniform(key, SHAPES[name], jnp.float32, 0.02, 0.06)
    return drawn


def matmul(a, w):
    return jnp.dot(a, w, preferred_element_type=jnp.float32).astype(jnp.bfloat16)


def normed(h):
    wide = h.astype(jnp.float32)
    scale = lax.rsqrt(jnp.mean(wide**2, -1, keepdims=True) + 1e-6)
    return (wide * scale).astype(jnp.bfloat16)


def turned(t, theta):
    half = t.shape[-1] // 2
    angle = jnp.arange(t.shape[0], dtype=jnp.float32)[:, None] * theta ** (-jnp.arange(half, dtype=jnp.float32) / half)
    cos, sin = jnp.cos(angle)[:, None], jnp.sin(angle)[:, None]
    a, b = t[..., :half].astype(jnp.float32), t[..., half:].astype(jnp.float32)
    return jnp.concatenate([a * cos - b * sin, b * cos + a * sin], -1).astype(jnp.bfloat16)


def seen_by(q, k, v):
    tokens, kv = q.shape[0], k.shape[1]
    q = q.reshape(tokens, kv, -1, q.shape[-1])
    scores = jnp.einsum("tgsd,ugd->gstu", q.astype(jnp.float32), k.astype(jnp.float32)) * q.shape[-1] ** -0.5
    place = jnp.arange(tokens)
    weights = jax.nn.softmax(jnp.where(place[:, None] >= place, scores, -jnp.inf), -1).astype(jnp.bfloat16)
    return jnp.einsum("gstu,ugd->tgsd", weights.astype(jnp.float32), v.astype(jnp.float32)).astype(jnp.bfloat16).reshape(tokens, -1)


def layer(h, w):
    a = normed(h)
    q, k = (turned(matmul(a, w[name]).reshape(h.shape[0], -1, HEAD), THETA) for name in ("wq", "wk"))
    h = h + matmul(seen_by(q, k, matmul(a, w["wv"]).reshape(h.shape[0], -1, HEAD)), w["wo"])
    b = normed(h)
    gate = jnp.dot(b, w["w_gate"], preferred_element_type=jnp.float32)
    up = jnp.dot(b, w["w_up"], preferred_element_type=jnp.float32)
    return h + matmul((jax.nn.silu(gate) * up).astype(jnp.bfloat16), w["w_down"])


def adamw(w, m, v, g):
    m = 0.9 * m + 0.1 * g
    v = 0.95 * v + 0.05 * g * g
    step = m * lax.rsqrt(v + 1e-8) + 0.1 * w
    return (w - 0.02 * step).astype(jnp.bfloat16), m, v


def clipped(gradients, sum_of_squares, count):
    factor = jnp.minimum(1.0, 0.5 * lax.rsqrt(sum_of_squares / count + 1e-30))
    return [g * factor for g in gradients]


def stack(weights, h):
    return lax.scan(lambda h, w: (layer(h, w), None), h, weights)[0]


def reference(x, dy, wq, wk, wv, wo, w_gate, w_up, w_down, m_wq, m_wk, m_wv, m_wo, m_w_gate, m_w_up, m_w_down, v_wq, v_wk, v_wv, v_wo, v_w_gate, v_w_up, v_w_down):
    weights = dict(zip(NAMES, (wq, wk, wv, wo, w_gate, w_up, w_down), strict=True))

    def take(so_far, sequence):
        h, by_y = sequence
        _, back = jax.vjp(stack, weights, h)
        by_weights, by_h = back(by_y)
        return jax.tree.map(lambda total, term: total + term.astype(jnp.float32), so_far, by_weights), by_h

    none_yet = {name: jnp.zeros(w.shape, jnp.float32) for name, w in weights.items()}
    by_weights, by_x = lax.scan(take, none_yet, (x, dy))
    gradients = [by_weights[name].astype(jnp.bfloat16).astype(jnp.float32) for name in NAMES]
    gradients = clipped(gradients, sum(jnp.sum(g * g) for g in gradients), sum(g.size for g in gradients))
    first = (m_wq, m_wk, m_wv, m_wo, m_w_gate, m_w_up, m_w_down)
    second = (v_wq, v_wk, v_wv, v_wo, v_w_gate, v_w_up, v_w_down)
    new = [adamw(weights[name].astype(jnp.float32), m, v, g) for name, m, v, g in zip(NAMES, first, second, gradients, strict=True)]
    return tuple(one[which] for which in range(3) for one in new)
```

```python
import functools

import jax
import jax.numpy as jnp
import numpy as np
from jax import lax
from jax.experimental import pallas as pl
from jax.experimental.pallas import tpu as pltpu
from jax.sharding import PartitionSpec as P

NEG = -1e30
HIDDEN = 2 * NEG
LOG2E = 1.4426950408889634
VMEM = 56 * 2**20
NAMES = ("wq", "wk", "wv", "wo", "w_gate", "w_up", "w_down")
TOKENS, D, HEADS, HEAD, FF = 1024, 640, 8, 128, 3200
SCALE = HEAD**-0.5
E = SCALE * LOG2E
THETA = 10000
f32, bf16 = jnp.float32, jnp.bfloat16


def _dot(a, b, ca=1, cb=0):
    return lax.dot_general(a, b, (((ca,), (cb,)), ((), ())), preferred_element_type=f32)


def _normed(wide):
    return wide * lax.rsqrt(jnp.mean(wide * wide, -1, keepdims=True) + 1e-6)


def _angles():
    half = HEAD // 2
    angle = np.arange(TOKENS, dtype=np.float32)[:, None] * np.float32(THETA) ** (-np.arange(half, dtype=np.float32) / np.float32(half))
    return np.cos(angle).astype(np.float32), np.sin(angle).astype(np.float32)
LANES, GROUPS = 128, 16
COLOURS, RING, FAMILY, MATRICES, CHUNKS = 3, 4, 8, 7, 12


BQ, BK = 512, 256


def _attend(x_ref, cos_ref, sin_ref, wq_ref, wk_ref, wv_ref, wo_ref, a_ref, q_ref, k_ref, v_ref, ot_ref, lse_ref, h_ref, ks, vts, top_s, mix_s):
    i = pl.program_id(0)
    a = _normed(x_ref[...].astype(f32)).astype(bf16)
    a_ref[...] = a
    cos, sin = cos_ref[...], sin_ref[...]

    def turned(t):
        t = t.astype(bf16).astype(f32)
        return (t * cos + pltpu.roll(t, HEAD // 2, 1) * sin).astype(bf16)

    k = turned(_dot(a, wk_ref[...]))
    v = _dot(a, wv_ref[...]).astype(bf16)
    k_ref[...] = k
    v_ref[...] = v
    here = pl.ds(pl.multiple_of(i * BQ, BQ), BQ)
    ks[here, :] = k
    vts[:HEAD, here] = v.T
    vts[HEAD:, here] = jnp.ones((8, BQ), bf16)
    q = _dot(a, wq_ref[...])
    for n in range(HEADS):
        q_ref[n] = turned(q[:, n * HEAD : (n + 1) * HEAD])
    top_s[...] = jnp.full(top_s.shape, NEG, f32)
    mix_s[...] = jnp.zeros(mix_s.shape, f32)

    def block(j, low, masked):
        keys = pl.ds(pl.multiple_of(j * BK, BK), BK)
        scores = [_dot(ks[keys, :], q_ref[n, low:, :], 1, 1) for n in range(HEADS)]
        if masked:
            hidden = lax.broadcasted_iota(jnp.int32, (BK, BQ - low), 1) < lax.broadcasted_iota(jnp.int32, (BK, BQ - low), 0)
        values = vts[:, keys]
        weights, keeps = [], []
        for n, s in enumerate(scores):
            if masked:
                s = jnp.where(hidden, HIDDEN, s)
            old = top_s[n : n + 1, low:]
            top = jnp.maximum(old, s.max(axis=0, keepdims=True))
            top_s[n : n + 1, low:] = top
            weights.append(jnp.exp2((s - top) * E).astype(bf16))
            keeps.append(jnp.exp2((old - top) * E))
        for n, (p, keep) in enumerate(zip(weights, keeps)):
            mix_s[n, :, low:] = mix_s[n, :, low:] * keep + _dot(values, p)

    per = BQ // BK
    lax.fori_loop(0, per * i, lambda j, _: block(j, 0, False), None)
    for n in range(per):
        block(per * i + n, n * BK, True)
    outs = []
    for n in range(HEADS):
        total = mix_s[n, HEAD : HEAD + 1, :]
        out = (mix_s[n, :HEAD, :] * (1 / total)).astype(bf16)
        ot_ref[n * HEAD : (n + 1) * HEAD, :] = out
        outs.append(out.T)
        lse_ref[n : n + 1, :] = top_s[n : n + 1, :] * SCALE + jnp.log(total)
    more = _dot(jnp.concatenate(outs, axis=1), wo_ref[...]).astype(bf16)
    h_ref[...] = (x_ref[...].astype(f32) + more.astype(f32)).astype(bf16)


def attend(x, w):
    cos, sin = _angles()
    cos, sin = np.concatenate([cos, cos], 1), np.concatenate([-sin, sin], 1)
    whole = pl.BlockSpec(memory_space=pltpu.VMEM)
    rows = lambda width: pl.BlockSpec((BQ, width), lambda i: (i, 0))
    columns = lambda height: pl.BlockSpec((height, BQ), lambda i: (0, i))
    shape = jax.ShapeDtypeStruct
    return pl.pallas_call(
        _attend,
        grid=(TOKENS // BQ,),
        in_specs=[rows(D), rows(HEAD), rows(HEAD)] + [whole] * 4,
        out_specs=[rows(D), pl.BlockSpec((HEADS, BQ, HEAD), lambda i: (0, i, 0)), rows(HEAD), rows(HEAD), columns(HEADS * HEAD), columns(HEADS), rows(D)],
        out_shape=[shape((TOKENS, D), bf16), shape((HEADS, TOKENS, HEAD), bf16), shape((TOKENS, HEAD), bf16), shape((TOKENS, HEAD), bf16),
                   shape((HEADS * HEAD, TOKENS), bf16), shape((HEADS, TOKENS), f32), shape((TOKENS, D), bf16)],
        scratch_shapes=[pltpu.VMEM((TOKENS, HEAD), bf16), pltpu.VMEM((HEAD + 8, TOKENS), bf16), pltpu.VMEM((HEADS, BQ), f32),
                        pltpu.VMEM((HEADS, HEAD + 8, BQ), f32)],
        compiler_params=pltpu.CompilerParams(dimension_semantics=("arbitrary",), vmem_limit_bytes=VMEM),
    )(x, cos, sin, *[w[name] for name in ("wq", "wk", "wv", "wo")])


BF = 256
LAST = FF // BF
CHUNK = 512


def _gated(h_ref, dy_ref, wg_ref, wu_ref, wd_ref, g_ref, dh_ref, b_s, bt_s, dyt_s, acc_s, hid_s, dg_s, du_s, stage, down_s, zero_s, sem, end_sem):
    j = pl.program_id(0)
    slot = lax.rem(j, 2)
    firsts = [TABLE[NAMES.index(name)][0] for name in ("w_gate", "w_up", "w_down")]
    rows = D // GROUPS
    ends = firsts[2] + FF * D // GROUPS // LANES

    def put(n, at, size):
        where = pl.ds(pl.multiple_of(firsts[n] + at * (rows * BF // LANES), 8), size)
        return pltpu.make_async_copy(stage.at[n, slot, :, pl.ds(0, size)], g_ref.at[:, where], sem.at[n, slot])

    @pl.when(j == 0)
    def _():
        b = _normed(h_ref[...].astype(f32)).astype(bf16)
        b_s[...] = b
        bt_s[...] = b.T
        dyt_s[...] = dy_ref[...].T
        acc_s[...] = jnp.zeros(acc_s.shape, f32)
        zero_s[...] = jnp.zeros(zero_s.shape, bf16)
        pltpu.make_async_copy(zero_s, g_ref.at[:, pl.ds(ends, FLAT - ends)], end_sem.at[0]).start()

    left = FF - j * BF
    wg = jnp.where(lax.broadcasted_iota(jnp.int32, (D, BF), 1) < left, wg_ref[0], jnp.zeros((), bf16))
    wu = jnp.where(lax.broadcasted_iota(jnp.int32, (D, BF), 1) < left, wu_ref[0], jnp.zeros((), bf16))
    wd = jnp.where(lax.broadcasted_iota(jnp.int32, (BF, D), 0) < left, wd_ref[0], jnp.zeros((), bf16))
    for at in range(0, TOKENS, CHUNK):
        here = slice(at, at + CHUNK)
        gate, up = _dot(b_s[here, :], wg), _dot(b_s[here, :], wu)
        dhid = _dot(dy_ref[here, :], wd, 1, 1).astype(bf16).astype(f32)
        share = 1 / (1 + jnp.exp(-gate))
        silu = gate * share
        hid_s[here, :] = (silu * up).astype(bf16)
        dgate = (dhid * up * (share * (1 + gate * (1 - share)))).astype(bf16)
        dup = (dhid * silu).astype(bf16)
        dg_s[here, :] = dgate
        du_s[here, :] = dup
        acc_s[here, :] += _dot(dgate, wg, 1, 1) + _dot(dup, wu, 1, 1)

    @pl.when(j >= 2)
    def _():
        for n in range(2):
            put(n, j - 2, rows * BF // LANES).wait()

    for n, one in enumerate((dg_s, du_s)):
        term = _dot(bt_s[...], one[...])
        for k in range(BF // LANES):
            stage[n, slot, :, k * rows : (k + 1) * rows, :] = term[:, k * LANES : (k + 1) * LANES].astype(bf16).reshape(GROUPS, rows, LANES)
    term = _dot(dyt_s[...], hid_s[...]).T
    for k in range(D // LANES):
        down_s[k, pl.ds(pl.multiple_of(j * BF, BF), BF), :] = term[:, k * LANES : (k + 1) * LANES].astype(bf16)

    @pl.when(j < LAST)
    def _():
        for n in range(2):
            put(n, j, rows * BF // LANES).start()

    @pl.when(j == LAST)
    def _():
        for n in range(2):
            put(n, j, rows * (FF % BF) // LANES).start()
        per = FF // GROUPS
        for k in range(D // LANES):
            for n in range(GROUPS):
                pltpu.make_async_copy(down_s.at[k, pl.ds(n * per, per)], g_ref.at[n, pl.ds(firsts[2] + k * per, per)], end_sem.at[1]).start()
        for at in range(0, TOKENS, CHUNK):
            here = slice(at, at + CHUNK)
            db = acc_s[here, :].astype(bf16).astype(f32)
            h = h_ref[here, :].astype(f32)
            s = lax.rsqrt(jnp.mean(h * h, -1, keepdims=True) + 1e-6)
            through = db * s - h * (s * s * s * jnp.mean(db * h, -1, keepdims=True))
            dh_ref[here, :] = (dy_ref[here, :].astype(f32) + through.astype(bf16).astype(f32)).astype(bf16)
        for n in range(2):
            put(n, j, rows * (FF % BF) // LANES).wait()
            pltpu.make_async_copy(stage.at[n, 1 - slot], stage.at[n, 1 - slot], sem.at[n, 1 - slot]).wait()
        pltpu.make_async_copy(zero_s, g_ref.at[:, pl.ds(ends, FLAT - ends)], end_sem.at[0]).wait()
        whole = g_ref.at[:, pl.ds(firsts[2], ends - firsts[2])]
        pltpu.make_async_copy(whole, whole, end_sem.at[1]).wait()


def gated(h, dy, w):
    vmem = pltpu.VMEM
    whole = pl.BlockSpec(memory_space=vmem)
    across = pl.BlockSpec((1, D, BF), lambda j: (0, 0, j))
    pad = FLAT - TABLE[-1][0] - FF * D // GROUPS // LANES
    return pl.pallas_call(
        _gated,
        grid=(LAST + 1,),
        in_specs=[whole, whole, across, across, pl.BlockSpec((1, BF, D), lambda j: (0, j, 0))],
        out_specs=[pl.BlockSpec(memory_space=pl.ANY), whole],
        out_shape=[jax.ShapeDtypeStruct((GROUPS, FLAT, LANES), bf16), jax.ShapeDtypeStruct((TOKENS, D), bf16)],
        scratch_shapes=[vmem((TOKENS, D), bf16), vmem((D, TOKENS), bf16), vmem((D, TOKENS), bf16), vmem((TOKENS, D), f32),
                        vmem((TOKENS, BF), bf16), vmem((TOKENS, BF), bf16), vmem((TOKENS, BF), bf16),
                        vmem((2, 2, GROUPS, D // GROUPS * BF // LANES, LANES), bf16), vmem((D // LANES, (LAST + 1) * BF, LANES), bf16), vmem((GROUPS, pad, LANES), bf16),
                        pltpu.SemaphoreType.DMA((2, 2)), pltpu.SemaphoreType.DMA((2,))],
        compiler_params=pltpu.CompilerParams(dimension_semantics=("arbitrary",), vmem_limit_bytes=VMEM),
    )(h, dy, *[w[name] for name in ("w_gate", "w_up", "w_down")])


BACK = 256


def _attend_back(dh_ref, all_dh_ref, a_ref, q_ref, k_ref, v_ref, ot_ref, all_ot_ref, lse_ref, cos_ref, sin_ref, cost_ref, sint_ref, wo_ref, g_in, g_ref,
                 dqkv_s, dqt_s, dk_s, dv_s, do_s, stage, sem):
    i = pl.program_id(0)
    low = 0

    @pl.when(i == 0)
    def _():
        dk_s[...] = jnp.zeros(dk_s.shape, f32)
        dv_s[...] = jnp.zeros(dv_s.shape, f32)

    dqt_s[...] = jnp.zeros(dqt_s.shape, f32)
    dh, wo = dh_ref[...], wo_ref[...]
    dot = _dot(wo, dh, 1, 1).astype(bf16).astype(f32) * ot_ref[...].astype(f32)
    delta = [dot[n * HEAD : (n + 1) * HEAD, :].sum(axis=0, keepdims=True) for n in range(HEADS)]
    dout = _dot(dh, wo, 1, 1).astype(bf16)
    for n in range(HEADS):
        do_s[n] = dout[:, n * HEAD : (n + 1) * HEAD]
    pairs = range(0, HEADS, 2)
    beside = lambda rows, n: jnp.concatenate([rows[n], rows[n + 1]], axis=1)
    lses = [lse_ref[n : n + 1, :] * LOG2E for n in range(HEADS)]

    def block(j, masked):
        keys = pl.ds(pl.multiple_of(j * BACK, BACK), BACK)
        k, v = k_ref[keys, :], v_ref[keys, :]
        kt = k.T
        qs = [q_ref[n : n + 2].reshape(2 * BACK, HEAD) for n in pairs]
        dos = [do_s[n : n + 2].reshape(2 * BACK, HEAD) for n in pairs]
        scores = [_dot(k, q, 1, 1) for q in qs]
        dps = [_dot(v, one, 1, 1) for one in dos]
        if masked:
            place = lax.broadcasted_iota(jnp.int32, (BACK, 2 * BACK), 1)
            hidden = jnp.where(place < BACK, place, place - BACK) < lax.broadcasted_iota(jnp.int32, (BACK, 2 * BACK), 0)
        for n in pairs:
            p = jnp.exp2(scores[n // 2] * E - beside(lses, n))
            if masked:
                p = jnp.where(hidden, 0.0, p)
            ds = (p * (dps[n // 2] - beside(delta, n))).astype(bf16)
            dv_s[keys, :] += _dot(p.astype(bf16), dos[n // 2])
            dk_s[keys, :] += _dot(ds, qs[n // 2])
            dqt_s[:, n * BACK : (n + 2) * BACK] += _dot(kt, ds)

    lax.fori_loop(0, i, lambda j, _: block(j, False), None)
    block(i, True)
    here = pl.ds(pl.multiple_of(i * BACK, BACK), BACK)
    cost, sint = cost_ref[...], sint_ref[...]
    half = HEAD // 2
    for n in range(HEADS):
        t = (dqt_s[:, n * BACK : (n + 1) * BACK] * SCALE).astype(bf16).astype(f32)
        one, two = t[:half], t[half:]
        t = jnp.concatenate([one * cost + two * sint, two * cost - one * sint], axis=0)
        dqkv_s[here, n * HEAD : (n + 1) * HEAD] = t.astype(bf16).T

    wide = HEADS * HEAD

    @pl.when(i == pl.num_programs(0) - 1)
    def _():
        t = (dk_s[...] * SCALE).astype(bf16).astype(f32)
        dqkv_s[:, wide : wide + HEAD] = (t * cos_ref[...] - pltpu.roll(t, half, 1) * sin_ref[...]).astype(bf16)
        dqkv_s[:, wide + HEAD :] = dv_s[...].astype(bf16)
        term = _dot(a_ref[...].T, dqkv_s[...])
        rows, end = D // GROUPS, TABLE[3][0]
        for k in range(end // rows):
            stage[:, k * rows : (k + 1) * rows, :] = term[:, k * LANES : (k + 1) * LANES].astype(bf16).reshape(GROUPS, rows, LANES)
        one = pltpu.make_async_copy(stage.at[:, pl.ds(0, end)], g_ref.at[:, pl.ds(0, end)], sem.at[0])
        one.start()
        term = _dot(all_ot_ref[...], all_dh_ref[...])
        rows, last = wide // GROUPS, TABLE[4][0]
        for k in range(D // LANES):
            stage[:, end + k * rows : end + (k + 1) * rows, :] = term[:, k * LANES : (k + 1) * LANES].astype(bf16).reshape(GROUPS, rows, LANES)
        two = pltpu.make_async_copy(stage.at[:, pl.ds(end, last - end)], g_ref.at[:, pl.ds(end, last - end)], sem.at[1])
        two.start()
        one.wait()
        two.wait()


def attend_back(dh, a, q, k, v, ot, lse, wo, g):
    cos, sin = _angles()
    wide_cos, wide_sin = np.concatenate([cos, cos], 1), np.concatenate([-sin, sin], 1)
    vmem = pltpu.VMEM
    whole = pl.BlockSpec(memory_space=vmem)
    hbm = pl.BlockSpec(memory_space=pl.ANY)
    columns = lambda height: pl.BlockSpec((height, BACK), lambda i: (0, i))
    return pl.pallas_call(
        _attend_back,
        grid=(TOKENS // BACK,),
        in_specs=[pl.BlockSpec((BACK, D), lambda i: (i, 0)), whole, whole, pl.BlockSpec((HEADS, BACK, HEAD), lambda i: (0, i, 0)), whole, whole,
                  columns(HEADS * HEAD), whole, columns(HEADS), whole, whole, columns(HEAD // 2), columns(HEAD // 2), whole, hbm],
        out_specs=hbm,
        out_shape=jax.ShapeDtypeStruct(g.shape, bf16),
        input_output_aliases={14: 0},
        scratch_shapes=[vmem((TOKENS, (HEADS + 2) * HEAD), bf16), vmem((HEAD, HEADS * BACK), f32), vmem((TOKENS, HEAD), f32), vmem((TOKENS, HEAD), f32),
                        vmem((HEADS, BACK, HEAD), bf16), vmem((GROUPS, TABLE[4][0], LANES), bf16), pltpu.SemaphoreType.DMA((2,))],
        compiler_params=pltpu.CompilerParams(dimension_semantics=("arbitrary",), vmem_limit_bytes=VMEM),
    )(dh, dh, a, q, k, v, ot, ot, lse, wide_cos, wide_sin, np.ascontiguousarray(cos.T), np.ascontiguousarray(sin.T), wo, g)


MESH, ALL = pl.DeviceIdType.MESH, slice(None)
SHAPE = {"wq": (640, 1024), "wk": (640, 128), "wv": (640, 128), "wo": (1024, 640), "w_gate": (640, 3200), "w_up": (640, 3200), "w_down": (3200, 640)}
UNIT = 160
FLAT = 24 * UNIT
ORDER = ((0, 1, 2), (1, 2, 0), (2, 0, 1))


def _table():
    table, flat, own = [], 0, 0
    for name in NAMES:
        rows, cols = SHAPE[name]
        step = -(-(rows // LANES) // FAMILY) * FAMILY
        table.append((flat, cols // LANES, rows // GROUPS, rows // LANES, own, step))
        flat += (cols // LANES) * (rows // GROUPS)
        own += (cols // LANES) * step
    return tuple(table), own


TABLE, OWN = _table()


def _at(k, lanes):
    return (ALL, lanes) if TABLE[k][COLOURS] % FAMILY == 0 else (ALL, 0, lanes)


def _rows(moments):
    return [one[0] if one.shape[1] % FAMILY == 0 else one.transpose(1, 0, 2) for one in moments]


def _comm(g_ref, *rest):
    w_refs, rest = rest[:MATRICES], rest[MATRICES:]
    m_refs, v_refs, rest = rest[:MATRICES], rest[MATRICES:14], rest[14:]
    out_ref, gq_ref, rest = rest[0], rest[1], rest[2:]
    wn_refs, rest = rest[:MATRICES], rest[MATRICES:]
    (s_ref, r0_ref, ra_ref, f_ref, rb_ref, sb_ref, f2_ref, rc_ref, sc_ref, piece_ref, gb_ref, gf_ref, wf_ref, ou_ref, ob_ref, wb_ref, wbf_ref,
     wv_ref, ps_ref, px_ref, py_ref, p8_ref, ring_send, ring_recv, d2d_send, d2d_recv, load_sem, w_sem, g8_send, g8_recv, ps_send, ps_recv,
     w8_send, w8_recv, od_send, od_recv, ol_sem) = rest
    f32, bf16 = jnp.float32, jnp.bfloat16
    me = lax.axis_index("dp")
    core = lax.rem(me, 2)
    at = [lax.rem(lax.div(me, 32), RING), lax.rem(lax.div(me, FAMILY), RING), lax.rem(lax.div(me, 2), RING)]
    group = lax.div(me, FAMILY)
    mine = lax.rem(me, FAMILY)

    def device(axis, by):
        place = [32, FAMILY, 2][axis]
        return me + (lax.rem(at[axis] + by, RING) - at[axis]) * place

    partner = me + 1 - 2 * core
    family = [group * FAMILY + lax.rem(mine + k, FAMILY) for k in range(1, FAMILY)]
    friends = [device(axis, by) for axis in (0, 1) for by in (1, 2, COLOURS)] + family
    barrier = pltpu.get_barrier_semaphore()
    for one in friends:
        pl.semaphore_signal(barrier, inc=1, device_id={"dp": one}, device_id_type=MESH)

    def remote(src, dst, send, recv, to):
        return pltpu.make_async_remote_copy(src_ref=src, dst_ref=dst, send_sem=send, recv_sem=recv, device_id={"dp": to}, device_id_type=MESH)

    def near(q):
        return lax.rem(q, RING)

    def where(axis, q, first=ALL):
        return ((q, first, ALL), (first, q, ALL), (first, ALL, q))[axis]

    def place(axis, q, a, b):
        return ((q, a, b), (a, q, b), (a, b, q))[axis]

    def half(h):
        return pl.ds(2 * h, 2)

    loads, swaps = {}, {}
    for k, rel in enumerate((2, 1, COLOURS, 0)):
        for col in range(COLOURS):
            axis = ORDER[col][0]
            q = near(at[axis] + rel)
            loads[col, rel] = pltpu.make_async_copy(g_ref.at[(*where(axis, q), core, col)], s_ref.at[(*where(axis, q), col)], load_sem.at[col * RING + k])
            loads[col, rel].start()
    for k in range(MATRICES):
        pltpu.make_async_copy(w_refs[k].at[group], wn_refs[k], w_sem.at[k]).start()
    pl.semaphore_wait(barrier, len(friends))
    for k, rel in enumerate((2, 1, COLOURS, 0)):
        for col in range(COLOURS):
            axis = ORDER[col][0]
            q = near(at[axis] + rel)
            swaps[col, rel] = remote(g_ref.at[(*where(axis, q), 1 - core, col)], r0_ref.at[(*where(axis, q), col)],
                                     d2d_send.at[col * RING + k], d2d_recv.at[col * RING + k], partner)
            swaps[col, rel].start()

    def ring_sem(phase, col, d, slot):
        return ((phase * COLOURS + col) * 2 + d) * COLOURS + slot

    def hop(phase, col, axis, d, slot, src, dst):
        n = ring_sem(phase, col, d, slot)
        return remote(src, dst, ring_send.at[n], ring_recv.at[n], device(axis, 1 if d == 0 else COLOURS))

    pending = []

    def sum_phase(phase, units, term, source, store, inbox, value, final, ready):
        def start(col, d, slot, rel, h):
            copy = hop(phase, col, ORDER[col][phase], d, slot, source(col, rel, h), inbox(col, d, slot))
            copy.start()
            pending.append(copy)

        def arrived(col, d, slot):
            hop(phase, col, ORDER[col][phase], d, slot, inbox(col, d, slot), inbox(col, d, slot)).wait_recv()

        def each(body):
            if units == 1:
                body(0)
            else:
                lax.fori_loop(0, units, lambda u, _: body(u), None)

        for col in range(COLOURS):
            ready(col, 2)
            for d in range(2):
                each(lambda u: store(col, 2, d, u, term(col, 2, d, u)))
                start(col, d, 0, 2, d)
        for col in range(COLOURS):
            for d, rel in ((0, 1), (1, COLOURS)):
                ready(col, rel)
                each(lambda u: store(col, rel, 1 - d, u, term(col, rel, 1 - d, u)))
                start(col, d, 1, rel, 1 - d)
        for col in range(COLOURS):
            for d, rel in ((0, 1), (1, COLOURS)):
                arrived(col, d, 0)
                each(lambda u: store(col, rel, d, u, term(col, rel, d, u) + value(col, d, 0, u)))
                start(col, d, 2, rel, d)
        for col in range(COLOURS):
            ready(col, 0)
            for d in range(2):
                for slot in (1, 2):
                    arrived(col, d, slot)
            for h in range(2):
                each(lambda u: final(col, h, u, term(col, 0, h, u) + value(col, 0, 2 - h, u) + value(col, 1, 1 + h, u)))

    def spot(col, rel, h, u):
        axis = ORDER[col][0]
        return place(axis, near(at[axis] + rel), 2 * h + lax.div(u, RING), lax.rem(u, RING))

    def first_term(col, rel, h, u):
        here = (*spot(col, rel, h, u), col)
        return s_ref[here].astype(f32) + r0_ref[here].astype(f32)

    def first_store(col, rel, h, u, x):
        s_ref[(*spot(col, rel, h, u), col)] = x.astype(bf16)

    def first_source(col, rel, h):
        axis = ORDER[col][0]
        return s_ref.at[(*where(axis, near(at[axis] + rel), half(h)), col)]

    def first_final(col, h, u, x):
        a, b = 2 * h + lax.div(u, RING), lax.rem(u, RING)
        f_ref[(col, b, a) if col == 1 else (col, a, b)] = x

    def first_ready(col, rel):
        loads[col, rel].wait()
        swaps[col, rel].wait_recv()

    sum_phase(0, FAMILY, first_term, first_source, first_store, lambda col, d, slot: ra_ref.at[col, d, slot],
              lambda col, d, slot, u: ra_ref[col, d, slot, lax.div(u, RING), lax.rem(u, RING)].astype(f32), first_final, first_ready)

    for k, (flat, blocks, rows, _, _, _) in enumerate(TABLE):
        pltpu.make_async_copy(w_refs[k].at[group], wn_refs[k], w_sem.at[k]).wait()
        for j in range(blocks):
            wf_ref[flat + j * rows : flat + (j + 1) * rows, :] = wn_refs[k][:, j * LANES : (j + 1) * LANES].astype(f32)

    def second_store(col, rel, h, u, x):
        sb_ref[col, rel - 1, 2 * h + u] = x.astype(bf16)

    def second_final(col, h, u, x):
        f2_ref[col, 2 * h + u] = x

    sum_phase(1, 2, lambda col, rel, h, u: f_ref[col, near(at[ORDER[col][1]] + rel), 2 * h + u],
              lambda col, rel, h: sb_ref.at[col, rel - 1, half(h)], second_store, lambda col, d, slot: rb_ref.at[col, d, slot],
              lambda col, d, slot, u: rb_ref[col, d, slot, u].astype(f32), second_final, lambda col, rel: None)

    cut = UNIT // 2

    def third_store(col, rel, h, u, x):
        sc_ref[col, rel - 1, h * cut : (h + 1) * cut] = x.astype(bf16)

    squares = []

    def third_final(col, h, u, x):
        x = x.astype(bf16)
        piece_ref[col * UNIT + h * cut : col * UNIT + (h + 1) * cut, :] = x
        x = x.astype(f32)
        squares.append(jnp.sum((x * x).reshape(cut // FAMILY, FAMILY, LANES), axis=0))

    sum_phase(2, 1, lambda col, rel, h, u: f2_ref[col, near(at[ORDER[col][2]] + rel), h * cut : (h + 1) * cut],
              lambda col, rel, h: sc_ref.at[col, rel - 1, h * cut : (h + 1) * cut], third_store, lambda col, d, slot: rc_ref.at[col, d, slot],
              lambda col, d, slot, u: rc_ref[col, d, slot].astype(f32), third_final, lambda col, rel: None)

    mine_rows = COLOURS * UNIT
    g8 = []
    for k in range(MATRICES):
        copy = remote(piece_ref, gb_ref.at[pl.ds(mine * mine_rows, mine_rows)], g8_send.at[k], g8_recv.at[6 - k], family[k])
        copy.start()
        g8.append(copy)

    def swap_squares(total, base, targets, box):
        n = len(targets)
        ps_ref[0 if base == 0 else (1 if base == COLOURS else 2)] = total
        src = ps_ref.at[0 if base == 0 else (1 if base == COLOURS else 2)]
        copies = []
        for k, to in enumerate(targets):
            copy = remote(src, box.at[n - 1 - k], ps_send.at[base + k], ps_recv.at[base + n - 1 - k], to)
            copy.start()
            copies.append(copy)
        pending.extend(copies)
        for k in range(n):
            remote(box.at[k], box.at[k], ps_send.at[base + k], ps_recv.at[base + k], targets[0]).wait_recv()
            total = total + box[k]
        return total

    total = sum(squares[1:], squares[0])
    total = swap_squares(total, 0, [device(0, by) for by in (1, 2, COLOURS)], px_ref)
    total = swap_squares(total, COLOURS, [device(1, by) for by in (1, 2, COLOURS)], py_ref)
    total = swap_squares(total, 6, family, p8_ref)
    mean = jnp.sum(total) / float(sum(a * b for a, b in SHAPE.values()))
    factor = jnp.minimum(1.0, 0.5 * lax.rsqrt(jnp.full((FAMILY, LANES), mean, f32) + 1e-30))

    gf_ref[pl.ds(pl.multiple_of(mine * mine_rows, FAMILY), mine_rows), :] = piece_ref[...].astype(f32)
    for k in range(MATRICES):
        other = lax.rem(mine + k + 1, FAMILY)
        here = pl.ds(pl.multiple_of(other * mine_rows, GROUPS), mine_rows)
        remote(piece_ref, gb_ref.at[here], g8_send.at[k], g8_recv.at[k], family[k]).wait_recv()
        gf_ref[here, :] = gb_ref[here, :].astype(f32)

    for k, (flat, blocks, rows, own, first, step) in enumerate(TABLE):
        for j in range(blocks):
            here = pl.ds(flat + j * rows + mine * own, own)
            lanes = slice(j * LANES, (j + 1) * LANES)
            g = gf_ref[here, :] * factor[:1]
            w = wf_ref[here, :]
            m = 0.9 * m_refs[k][_at(k, lanes)] + 0.1 * g
            v = 0.95 * v_refs[k][_at(k, lanes)] + 0.05 * g * g
            to = slice(first + j * step, first + j * step + own)
            ou_ref[to, :] = w - 0.02 * (m * lax.rsqrt(v + 1e-8) + 0.1 * w)
            gq_ref[to, :] = g
    ob_ref[...] = ou_ref[...].astype(bf16)

    w8 = []
    for k in range(MATRICES):
        copy = remote(ob_ref, wb_ref.at[mine], w8_send.at[k], w8_recv.at[6 - k], family[k])
        copy.start()
        w8.append(copy)
    wbf_ref[mine] = ob_ref[...].astype(f32)
    for k in range(MATRICES):
        other = lax.rem(mine + k + 1, FAMILY)
        remote(ob_ref, wb_ref.at[other], w8_send.at[k], w8_recv.at[k], family[k]).wait_recv()
        wbf_ref[other] = wb_ref[other].astype(f32)
    for k, (flat, blocks, rows, own, first, step) in enumerate(TABLE):
        for j in range(blocks):
            for n in range(FAMILY):
                gf_ref[flat + j * rows + n * own : flat + j * rows + (n + 1) * own, :] = wbf_ref[n, first + j * step : first + j * step + own, :]
    here = tuple(at)
    for col in range(COLOURS):
        wv_ref[(*here, col)] = gf_ref[pl.ds(pl.multiple_of(mine * mine_rows, FAMILY) + col * UNIT, UNIT), :].astype(bf16)

    outs = []

    def hand_on(col, rel):
        axis = ORDER[col][0]
        q = near(at[axis] + rel)
        src, dst = wv_ref.at[(*where(axis, q), col)], out_ref.at[(*where(axis, q), core, col)]
        n = col * RING + rel
        copy = remote(src, dst, od_send.at[n], od_recv.at[n], partner)
        copy.start()
        local = pltpu.make_async_copy(src, dst, ol_sem.at[n])
        local.start()
        outs.append((copy, local))

    def gather_phase(phase, chunk, done):
        axes = [ORDER[col][phase] for col in range(COLOURS)]

        def start(col, d, slot, rel, h):
            copy = hop(5 - phase, col, axes[col], d, slot, chunk(col, rel, h), chunk(col, rel, h))
            copy.start()
            pending.append(copy)

        def arrived(col, d, slot, rel, h):
            hop(5 - phase, col, axes[col], d, slot, chunk(col, rel, h), chunk(col, rel, h)).wait_recv()

        for slot in range(2):
            for col in range(COLOURS):
                for d in range(2):
                    start(col, d, slot, 0, d if slot == 0 else 1 - d)
        for col in range(COLOURS):
            done(col, 0)
        for col in range(COLOURS):
            for d, rel in ((0, COLOURS), (1, 1)):
                arrived(col, d, 0, rel, d)
                start(col, d, 2, rel, d)
        for col in range(COLOURS):
            for d, rel in ((0, COLOURS), (1, 1)):
                arrived(col, d, 1, rel, 1 - d)
                done(col, rel)
        for col in range(COLOURS):
            for d in range(2):
                arrived(col, d, 2, 2, d)
            done(col, 2)

    def last_chunk(col, rel, h):
        spot = list(at)
        spot[ORDER[col][2]] = near(at[ORDER[col][2]] + rel)
        return wv_ref.at[(*spot, col, pl.ds(h * cut, cut))]

    def middle_chunk(col, rel, h):
        spot = list(at)
        spot[ORDER[col][1]] = near(at[ORDER[col][1]] + rel)
        spot[ORDER[col][2]] = half(h)
        return wv_ref.at[(*spot, col)]

    def whole_chunk(col, rel, h):
        axis = ORDER[col][0]
        return wv_ref.at[(*where(axis, near(at[axis] + rel), half(h)), col)]

    gather_phase(2, last_chunk, lambda col, rel: None)
    gather_phase(1, middle_chunk, lambda col, rel: None)
    gather_phase(0, whole_chunk, hand_on)

    for copy in swaps.values():
        copy.wait_send()
    for copy in pending + g8 + w8:
        copy.wait_send()
    for copy, local in outs:
        copy.wait_send()
        local.wait()
    for col in range(COLOURS):
        axis = ORDER[col][0]
        for rel in range(RING):
            n = col * RING + rel
            dst = out_ref.at[(*where(axis, near(at[axis] + rel)), 1 - core, col)]
            remote(dst, dst, od_send.at[n], od_recv.at[n], partner).wait_recv()


def sum_step_gather(g, weights, m, v):
    f32, bf16, vmem, dma = jnp.float32, jnp.bfloat16, pltpu.VMEM, pltpu.SemaphoreType.DMA
    hbm, local = pl.BlockSpec(memory_space=pl.ANY), pl.BlockSpec(memory_space=pltpu.VMEM)
    scratch = [vmem((SHAPE[name][0] // GROUPS, SHAPE[name][1]), bf16) for name in NAMES]
    scratch += [
        vmem((RING, RING, RING, COLOURS, UNIT, LANES), bf16), vmem((RING, RING, RING, COLOURS, UNIT, LANES), bf16), vmem((COLOURS, 2, COLOURS, 2, RING, UNIT, LANES), bf16),
        vmem((COLOURS, RING, RING, UNIT, LANES), f32), vmem((COLOURS, 2, COLOURS, 2, UNIT, LANES), bf16), vmem((COLOURS, COLOURS, RING, UNIT, LANES), bf16),
        vmem((COLOURS, RING, UNIT, LANES), f32), vmem((COLOURS, 2, COLOURS, UNIT // 2, LANES), bf16), vmem((COLOURS, COLOURS, UNIT, LANES), bf16),
        vmem((COLOURS * UNIT, LANES), bf16), vmem((FLAT, LANES), bf16), vmem((FLAT, LANES), f32), vmem((FLAT, LANES), f32),
        vmem((OWN, LANES), f32), vmem((OWN, LANES), bf16), vmem((FAMILY, OWN, LANES), bf16), vmem((FAMILY, OWN, LANES), f32),
        vmem((RING, RING, RING, COLOURS, UNIT, LANES), bf16), vmem((COLOURS, FAMILY, LANES), f32), vmem((COLOURS, FAMILY, LANES), f32), vmem((COLOURS, FAMILY, LANES), f32), vmem((MATRICES, FAMILY, LANES), f32),
        dma((108,)), dma((108,)), dma((CHUNKS,)), dma((CHUNKS,)), dma((CHUNKS,)), dma((MATRICES,)), dma((MATRICES,)), dma((MATRICES,)), dma((13,)), dma((13,)),
        dma((MATRICES,)), dma((MATRICES,)), dma((CHUNKS,)), dma((CHUNKS,)), dma((CHUNKS,)),
    ]
    return pl.pallas_call(
        _comm,
        out_shape=[jax.ShapeDtypeStruct(g.shape, bf16), jax.ShapeDtypeStruct((OWN, LANES), f32)],
        in_specs=[hbm] * FAMILY + [local] * 14,
        out_specs=[hbm, local],
        scratch_shapes=scratch,
        compiler_params=pltpu.CompilerParams(collective_id=0, has_side_effects=True, vmem_limit_bytes=62 * 2**20),
    )(g, *[w.reshape(GROUPS, w.shape[1] // GROUPS, w.shape[2]) for w in weights], *_rows(m), *_rows(v))


def _finish(flat_ref, gq_ref, *rest):
    m_refs, v_refs, w_refs, mo_refs, vo_refs = (rest[i : i + MATRICES] for i in range(0, 35, MATRICES))

    @pl.when(pl.program_id(0) == 0)
    def _():
        for k, (_, blocks, _, own, first, step) in enumerate(TABLE):
            for j in range(blocks):
                at = _at(k, slice(j * LANES, (j + 1) * LANES))
                g = gq_ref[first + j * step : first + j * step + own, :]
                mo_refs[k][at] = 0.9 * m_refs[k][at] + 0.1 * g
                vo_refs[k][at] = 0.95 * v_refs[k][at] + 0.05 * g * g

    for k, (flat, blocks, rows, _, _, _) in enumerate(TABLE):
        for j in range(blocks):
            w_refs[k][0, :, j * LANES : (j + 1) * LANES] = flat_ref[0, flat + j * rows : flat + (j + 1) * rows, :]


def finish(flat, gq, m, v):
    whole = pl.BlockSpec(memory_space=pltpu.VMEM)
    old = [*_rows(m), *_rows(v)]
    shapes = [(1, *SHAPE[name]) for name in NAMES]
    out = pl.pallas_call(
        _finish,
        grid=(GROUPS,),
        out_shape=[jax.ShapeDtypeStruct(shape, jnp.bfloat16) for shape in shapes] + [jax.ShapeDtypeStruct(a.shape, a.dtype) for a in old],
        in_specs=[pl.BlockSpec((1, FLAT, LANES), lambda i: (i, 0, 0)), whole] + [whole] * 14,
        out_specs=[pl.BlockSpec((1, shape[1] // GROUPS, shape[2]), lambda i: (0, i, 0)) for shape in shapes] + [whole] * 14,
        compiler_params=pltpu.CompilerParams(vmem_limit_bytes=VMEM),
    )(flat.reshape(GROUPS, FLAT, LANES), gq, *old)
    moments = [new.reshape(1, *new.shape) if new.ndim == 2 else new.transpose(1, 0, 2) for new in out[MATRICES:]]
    return (*out[:MATRICES], *moments)


def terms(x, dy, w):
    plain = {name: w[name][0] for name in ("wq", "wk", "wv", "wo")}
    a, q, k, v, ot, lse, h = attend(x, plain)
    g, dh = gated(h, dy, w)
    return attend_back(dh, a, q, k, v, ot, lse, plain["wo"], g)


def solution(mesh):
    def step(x, dy, *arrays):
        weights, m, v = (arrays[i : i + MATRICES] for i in (0, MATRICES, 14))
        g = terms(x[0], dy[0], dict(zip(NAMES, weights, strict=True)))
        flat, gq = sum_step_gather(g.reshape(RING, RING, RING, 2, COLOURS, UNIT, LANES), weights, m, v)
        return finish(flat, gq, m, v)

    states, all_of, cut = P(("rep", "dp")), P(), P(None, "dp")
    return jax.shard_map(
        step,
        mesh=mesh,
        in_specs=(states, states) + (all_of,) * MATRICES + (cut,) * 14,
        out_specs=(P("rep"),) * MATRICES + (P("rep", "dp"),) * 14,
        check_vma=False,
    )
```

```python
import functools

import jax
import jax.numpy as jnp
import numpy as np
from jax import lax
from jax.experimental import pallas as pl
from jax.experimental.pallas import tpu as pltpu
from jax.sharding import PartitionSpec as P

NEG = -1e30
HIDDEN = 2 * NEG
LOG2E = 1.4426950408889634
VMEM = 56 * 2**20
NAMES = ("wq", "wk", "wv", "wo", "w_gate", "w_up", "w_down")
TOKENS, D, HEADS, HEAD, FF = 1024, 640, 8, 128, 3200
SCALE = HEAD**-0.5
E = SCALE * LOG2E
THETA = 10000
f32, bf16 = jnp.float32, jnp.bfloat16


def _dot(a, b, ca=1, cb=0):
    return lax.dot_general(a, b, (((ca,), (cb,)), ((), ())), preferred_element_type=f32)


def _dot_t(a, b):
    return _dot(a, b, 1, 1)


def _lanes(k):
    return slice(k * 128, (k + 1) * 128)


def _scale(wide):
    return lax.rsqrt(jnp.mean(wide * wide, -1, keepdims=True) + 1e-6)


def _normed(wide):
    return wide * _scale(wide)


HALF = HEAD // 2


def _angles():
    angle = np.arange(TOKENS, dtype=np.float32)[:, None] * np.float32(THETA) ** (-np.arange(HALF, dtype=np.float32) / np.float32(HALF))
    return np.concatenate([np.cos(angle), np.sin(angle)], 1).astype(np.float32)


def _spread(angles):
    other = pltpu.roll(angles, HALF, 1)
    low = lax.broadcasted_iota(jnp.int32, angles.shape, 1) < HALF
    return jnp.where(low, angles, other), jnp.where(low, -other, angles)
LANES, GROUPS = 128, 16
COLOURS, RING, FAMILY, MATRICES, CHUNKS = 3, 4, 8, 7, 12


BQ, BK = 512, 256


def _attend(x_ref, angle_ref, wq_ref, wk_ref, wv_ref, wo_ref, a_ref, q_ref, k_ref, v_ref, ot_ref, lse_ref, h_ref, ks, vts, top_s, mix_s):
    i = pl.program_id(0)
    a = _normed(x_ref[...].astype(f32)).astype(bf16)
    a_ref[...] = a
    cos, sin = _spread(angle_ref[...])

    def turned(t):
        t = t.astype(bf16).astype(f32)
        return (t * cos + pltpu.roll(t, HALF, 1) * sin).astype(bf16)

    k = turned(_dot(a, wk_ref[...]))
    v = _dot(a, wv_ref[...]).astype(bf16)
    k_ref[...] = k
    v_ref[...] = v
    here = pl.ds(pl.multiple_of(i * BQ, BQ), BQ)
    ks[here, :] = k
    vts[:HEAD, here] = v.T
    vts[HEAD:, here] = jnp.ones((8, BQ), bf16)
    q = _dot(a, wq_ref[...])
    for n in range(HEADS):
        q_ref[n] = turned(q[:, _lanes(n)])
    top_s[...] = jnp.full(top_s.shape, NEG, f32)
    mix_s[...] = jnp.zeros(mix_s.shape, f32)

    def block(j, low, masked):
        keys = pl.ds(pl.multiple_of(j * BK, BK), BK)
        scores = [_dot_t(ks[keys, :], q_ref[n, low:, :]) for n in range(HEADS)]
        if masked:
            hidden = lax.broadcasted_iota(jnp.int32, (BK, BQ - low), 1) < lax.broadcasted_iota(jnp.int32, (BK, BQ - low), 0)
        values = vts[:, keys]
        weights, keeps = [], []
        for n, s in enumerate(scores):
            if masked:
                s = jnp.where(hidden, HIDDEN, s)
            old = top_s[n : n + 1, low:]
            top = jnp.maximum(old, s.max(axis=0, keepdims=True))
            top_s[n : n + 1, low:] = top
            weights.append(jnp.exp2((s - top) * E).astype(bf16))
            keeps.append(jnp.exp2((old - top) * E))
        for n, (p, keep) in enumerate(zip(weights, keeps)):
            mix_s[n, :, low:] = mix_s[n, :, low:] * keep + _dot(values, p)

    per = BQ // BK
    lax.fori_loop(0, per * i, lambda j, _: block(j, 0, False), None)
    for n in range(per):
        block(per * i + n, n * BK, True)
    outs = []
    for n in range(HEADS):
        total = mix_s[n, HEAD : HEAD + 1, :]
        out = (mix_s[n, :HEAD, :] * (1 / total)).astype(bf16)
        ot_ref[_lanes(n), :] = out
        outs.append(out.T)
        lse_ref[n : n + 1, :] = top_s[n : n + 1, :] * SCALE + jnp.log(total)
    more = _dot(jnp.concatenate(outs, axis=1), wo_ref[...]).astype(bf16)
    h_ref[...] = (x_ref[...].astype(f32) + more.astype(f32)).astype(bf16)


def attend(x, w):
    whole = pl.BlockSpec(memory_space=pltpu.VMEM)
    rows = lambda width: pl.BlockSpec((BQ, width), lambda i: (i, 0))
    columns = lambda height: pl.BlockSpec((height, BQ), lambda i: (0, i))
    shape = jax.ShapeDtypeStruct
    return pl.pallas_call(
        _attend,
        grid=(TOKENS // BQ,),
        in_specs=[rows(D), rows(HEAD)] + [whole] * 4,
        out_specs=[rows(D), pl.BlockSpec((HEADS, BQ, HEAD), lambda i: (0, i, 0)), rows(HEAD), rows(HEAD), columns(HEADS * HEAD), columns(HEADS), rows(D)],
        out_shape=[shape((TOKENS, D), bf16), shape((HEADS, TOKENS, HEAD), bf16), shape((TOKENS, HEAD), bf16), shape((TOKENS, HEAD), bf16),
                   shape((HEADS * HEAD, TOKENS), bf16), shape((HEADS, TOKENS), f32), shape((TOKENS, D), bf16)],
        scratch_shapes=[pltpu.VMEM((TOKENS, HEAD), bf16), pltpu.VMEM((HEAD + 8, TOKENS), bf16), pltpu.VMEM((HEADS, BQ), f32),
                        pltpu.VMEM((HEADS, HEAD + 8, BQ), f32)],
        compiler_params=pltpu.CompilerParams(dimension_semantics=("arbitrary",), vmem_limit_bytes=VMEM),
    )(x, _angles(), *[w[name] for name in ("wq", "wk", "wv", "wo")])


BF = 256
LAST = FF // BF
CHUNK = 512


def _gated(h_ref, dy_ref, wg_ref, wu_ref, wd_ref, g_ref, dh_ref, b_s, bt_s, dyt_s, acc_s, hid_s, dg_s, du_s, stage, down_s, zero_s, sem, end_sem):
    j = pl.program_id(0)
    slot = lax.rem(j, 2)
    firsts = [TABLE[NAMES.index(name)][0] for name in ("w_gate", "w_up", "w_down")]
    rows = D // GROUPS
    ends = 3 * FF * D // GROUPS // LANES

    def put(n, at, size):
        where = pl.ds(pl.multiple_of(firsts[n] + at * (rows * BF // LANES), 8), size)
        return pltpu.make_async_copy(stage.at[n, slot, :, pl.ds(0, size)], g_ref.at[:, where], sem.at[n, slot])

    @pl.when(j == 0)
    def _():
        b = _normed(h_ref[...].astype(f32)).astype(bf16)
        b_s[...] = b
        bt_s[...] = b.T
        dyt_s[...] = dy_ref[...].T
        acc_s[...] = jnp.zeros(acc_s.shape, f32)
        zero_s[...] = jnp.zeros(zero_s.shape, bf16)
        pltpu.make_async_copy(zero_s, g_ref.at[:, pl.ds(ends, GATED - ends)], end_sem.at[0]).start()

    left = FF - j * BF
    inside = lax.broadcasted_iota(jnp.int32, (D, BF), 1) < left
    wg, wu = (jnp.where(inside, ref[0], jnp.zeros((), bf16)) for ref in (wg_ref, wu_ref))
    wd = jnp.where(lax.broadcasted_iota(jnp.int32, (BF, D), 0) < left, wd_ref[0], jnp.zeros((), bf16))
    for at in range(0, TOKENS, CHUNK):
        here = slice(at, at + CHUNK)
        gate, up = _dot(b_s[here, :], wg), _dot(b_s[here, :], wu)
        dhid = _dot_t(dy_ref[here, :], wd).astype(bf16).astype(f32)
        share = 1 / (1 + jnp.exp(-gate))
        silu = gate * share
        hid_s[here, :] = (silu * up).astype(bf16)
        dgate = (dhid * up * (share * (1 + gate * (1 - share)))).astype(bf16)
        dup = (dhid * silu).astype(bf16)
        dg_s[here, :] = dgate
        du_s[here, :] = dup
        acc_s[here, :] += _dot_t(dgate, wg) + _dot_t(dup, wu)

    @pl.when(j >= 2)
    def _():
        for n in range(2):
            put(n, j - 2, rows * BF // LANES).wait()

    for n, one in enumerate((dg_s, du_s)):
        term = _dot(bt_s[...], one[...])
        for k in range(BF // LANES):
            stage[n, slot, :, k * rows : (k + 1) * rows, :] = term[:, _lanes(k)].reshape(GROUPS, rows, LANES).astype(bf16)
    term = _dot(dyt_s[...], hid_s[...]).T
    for k in range(D // LANES):
        down_s[k, pl.ds(pl.multiple_of(j * BF, BF), BF), :] = term[:, _lanes(k)].astype(bf16)

    @pl.when(j < LAST)
    def _():
        for n in range(2):
            put(n, j, rows * BF // LANES).start()

    @pl.when(j == LAST)
    def _():
        for n in range(2):
            put(n, j, rows * (FF % BF) // LANES).start()
        per = FF // GROUPS
        for k in range(D // LANES):
            for n in range(GROUPS):
                pltpu.make_async_copy(down_s.at[k, pl.ds(n * per, per)], g_ref.at[n, pl.ds(firsts[2] + k * per, per)], end_sem.at[1]).start()
        for at in range(0, TOKENS, CHUNK):
            here = slice(at, at + CHUNK)
            db = acc_s[here, :].astype(bf16).astype(f32)
            h = h_ref[here, :].astype(f32)
            s = _scale(h)
            through = db * s - h * (s * s * s * jnp.mean(db * h, -1, keepdims=True))
            dh_ref[here, :] = (dy_ref[here, :].astype(f32) + through.astype(bf16).astype(f32)).astype(bf16)
        for n in range(2):
            put(n, j, rows * (FF % BF) // LANES).wait()
            pltpu.make_async_copy(stage.at[n, 1 - slot], stage.at[n, 1 - slot], sem.at[n, 1 - slot]).wait()
        pltpu.make_async_copy(zero_s, g_ref.at[:, pl.ds(ends, GATED - ends)], end_sem.at[0]).wait()
        whole = g_ref.at[:, pl.ds(firsts[2], ends - firsts[2])]
        pltpu.make_async_copy(whole, whole, end_sem.at[1]).wait()


def gated(h, dy, w):
    vmem = pltpu.VMEM
    whole = pl.BlockSpec(memory_space=vmem)
    across = pl.BlockSpec((1, D, BF), lambda j: (0, 0, j))
    pad = GATED - 3 * FF * D // GROUPS // LANES
    return pl.pallas_call(
        _gated,
        grid=(LAST + 1,),
        in_specs=[whole, whole, across, across, pl.BlockSpec((1, BF, D), lambda j: (0, j, 0))],
        out_specs=[pl.BlockSpec(memory_space=pl.ANY), whole],
        out_shape=[jax.ShapeDtypeStruct((GROUPS, GATED, LANES), bf16), jax.ShapeDtypeStruct((TOKENS, D), bf16)],
        scratch_shapes=[vmem((TOKENS, D), bf16), vmem((D, TOKENS), bf16), vmem((D, TOKENS), bf16), vmem((TOKENS, D), f32),
                        vmem((TOKENS, BF), bf16), vmem((TOKENS, BF), bf16), vmem((TOKENS, BF), bf16),
                        vmem((2, 2, GROUPS, D // GROUPS * BF // LANES, LANES), bf16), vmem((D // LANES, (LAST + 1) * BF, LANES), bf16), vmem((GROUPS, pad, LANES), bf16),
                        pltpu.SemaphoreType.DMA((2, 2)), pltpu.SemaphoreType.DMA((2,))],
        compiler_params=pltpu.CompilerParams(dimension_semantics=("arbitrary",), vmem_limit_bytes=VMEM),
    )(h, dy, *[w[name] for name in ("w_gate", "w_up", "w_down")])


BACK = 256


def _back_step(i, dh_ref, q_ref, k_ref, v_ref, ot_ref, lse_ref, angle_ref, wo_ref, dqkv_s, dqt_s, dk_s, dv_s, do_s):
    here = slice(i * BACK, (i + 1) * BACK)
    if i == 0:
        dk_s[...] = jnp.zeros(dk_s.shape, f32)
        dv_s[...] = jnp.zeros(dv_s.shape, f32)
    dqt_s[...] = jnp.zeros(dqt_s.shape, f32)
    dh, wo = dh_ref[here, :], wo_ref[...]
    dot = _dot_t(wo, dh).astype(bf16).astype(f32) * ot_ref[:, here].astype(f32)
    delta = [dot[_lanes(n), :].sum(axis=0, keepdims=True) for n in range(HEADS)]
    dout = _dot_t(dh, wo).astype(bf16)
    for n in range(HEADS):
        do_s[n] = dout[:, _lanes(n)]
    pairs = range(0, HEADS, 2)
    beside = lambda rows, n: jnp.concatenate([rows[n], rows[n + 1]], axis=1)
    lses = [lse_ref[n : n + 1, here] * LOG2E for n in range(HEADS)]

    def block(j, masked):
        keys = pl.ds(j * BACK if masked else pl.multiple_of(j * BACK, BACK), BACK)
        k, v = k_ref[keys, :], v_ref[keys, :]
        kt = k.T
        if masked:
            place = lax.broadcasted_iota(jnp.int32, (BACK, 2 * BACK), 1)
            hidden = jnp.where(place < BACK, place, place - BACK) < lax.broadcasted_iota(jnp.int32, (BACK, 2 * BACK), 0)
        for some in (pairs[:2], pairs[2:]):
            qs = [q_ref[n : n + 2, here, :].reshape(2 * BACK, HEAD) for n in some]
            dos = [do_s[n : n + 2].reshape(2 * BACK, HEAD) for n in some]
            scores = [_dot_t(k, q) for q in qs]
            dps = [_dot_t(v, one) for one in dos]
            for n, q, do, score, dp in zip(some, qs, dos, scores, dps):
                p = jnp.exp2(score * E - beside(lses, n))
                if masked:
                    p = jnp.where(hidden, 0.0, p)
                ds = (p * (dp - beside(delta, n))).astype(bf16)
                dv_s[keys, :] += _dot(p.astype(bf16), do)
                dk_s[keys, :] += _dot(ds, q)
                dqt_s[:, n * BACK : (n + 2) * BACK] += _dot(kt, ds)

    lax.fori_loop(0, i, lambda j, _: block(j, False), None)
    block(i, True)
    both = angle_ref[here, :].T
    cost, sint = both[:HALF], both[HALF:]
    for n in range(HEADS):
        t = (dqt_s[:, n * BACK : (n + 1) * BACK] * SCALE).astype(bf16).astype(f32)
        one, two = t[:HALF], t[HALF:]
        t = jnp.concatenate([one * cost + two * sint, two * cost - one * sint], axis=0)
        dqkv_s[here, _lanes(n)] = t.astype(bf16).T


def _back_put(put, term, first):
    rows = term.shape[0] // GROUPS
    for k in range(term.shape[1] // LANES):
        put(first + k * rows, term[:, _lanes(k)].reshape(GROUPS, rows, LANES))


def _back_qkv(put, a_ref, angle_ref, dqkv_s, dk_s, dv_s):
    wide = HEADS * HEAD
    cos, sin = _spread(angle_ref[...])
    t = (dk_s[...] * SCALE).astype(bf16).astype(f32)
    dqkv_s[:, wide : wide + HEAD] = (t * cos - pltpu.roll(t, HALF, 1) * sin).astype(bf16)
    dqkv_s[:, wide + HEAD :] = dv_s[...].astype(bf16)
    _back_put(put, _dot(a_ref[...].T, dqkv_s[...]), TABLE[0][0])


MESH, ALL = pl.DeviceIdType.MESH, slice(None)
SHAPE = {"wq": (640, 1024), "wk": (640, 128), "wv": (640, 128), "wo": (1024, 640), "w_gate": (640, 3200), "w_up": (640, 3200), "w_down": (3200, 640)}
UNIT = 160
UNITS = (LANES, 32)
GATED, OTHERS = 24 * UNITS[0], 24 * UNITS[1]
FLAT = GATED + OTHERS
ORDER = ((0, 1, 2), (1, 2, 0), (2, 0, 1))
AHEAD, BEHIND = ((0, 1), (1, COLOURS)), ((0, COLOURS), (1, 1))
WAY = (2, 1, COLOURS, 0)


def _table():
    table, flat, own = [], 0, 0
    for name in NAMES:
        rows, cols = SHAPE[name]
        flat = 0 if name == "w_gate" else flat
        step = -(-(rows // LANES) // FAMILY) * FAMILY
        table.append((flat, cols // LANES, rows // GROUPS, rows // LANES, own, step))
        flat += (cols // LANES) * (rows // GROUPS)
        own += (cols // LANES) * step
    return tuple(table), own


TABLE, OWN = _table()


def _flat(k):
    return TABLE[k][0] + (GATED if k < RING else 0)


def _at(k, lanes):
    return (ALL, lanes) if TABLE[k][COLOURS] % FAMILY == 0 else (ALL, 0, lanes)


def _rows(moments):
    return [one[0] if one.shape[1] % FAMILY == 0 else one.transpose(1, 0, 2) for one in moments]


def _near(q):
    return lax.rem(q, RING)


def _where(axis, q, first=ALL):
    return ((q, first, ALL), (first, q, ALL), (first, ALL, q))[axis]


def _place(axis, q, a, b):
    return ((q, a, b), (a, q, b), (a, b, q))[axis]


def _half(h):
    return pl.ds(2 * h, 2)


class _Sum:
    def __init__(self, unit, at, hop, swaps, own, other, boxes, final):
        self.unit, self.at, self.hop, self.swaps, self.own, self.other, self.last = unit, at, hop, swaps, own, other, final
        self.ra, self.f, self.rb, self.sb, self.f2, self.rc, self.sc = boxes
        self.sent, self.cut = [], unit // 2

    def spot(self, col, rel, h, u):
        axis = ORDER[col][0]
        return _place(axis, _near(self.at[axis] + rel), 2 * h + lax.div(u, RING), lax.rem(u, RING))

    def chunk(self, phase, col, rel):
        return _near(self.at[ORDER[col][phase]] + rel)

    def rows(self, h):
        return slice(h * self.cut, (h + 1) * self.cut)

    def term(self, phase, col, rel, h, u):
        if phase == 0:
            here = self.spot(col, rel, h, u)
            return self.own(here, col)[...].astype(f32) + self.other[(*here, col)].astype(f32)
        if phase == 1:
            return self.f[col, self.chunk(1, col, rel), 2 * h + u]
        return self.f2[col, self.chunk(2, col, rel), self.rows(h)]

    def source(self, phase, col, rel, h):
        if phase == 0:
            axis = ORDER[col][0]
            return self.own(_where(axis, self.chunk(0, col, rel), _half(h)), col)
        return self.sb.at[col, rel - 1, _half(h)] if phase == 1 else self.sc.at[col, rel - 1, self.rows(h)]

    def store(self, phase, col, rel, h, u, x):
        x = x.astype(bf16)
        if phase == 0:
            self.own(self.spot(col, rel, h, u), col)[...] = x
        elif phase == 1:
            self.sb[col, rel - 1, 2 * h + u] = x
        else:
            self.sc[col, rel - 1, self.rows(h)] = x

    def inbox(self, phase, col, d, slot):
        return (self.ra, self.rb, self.rc)[phase].at[col, d, slot]

    def value(self, phase, col, d, slot, u):
        box = self.inbox(phase, col, d, slot)
        box = (box.at[lax.div(u, RING), lax.rem(u, RING)] if phase == 0 else box.at[u] if phase == 1 else box)
        return box[...].astype(f32)

    def final(self, phase, col, h, u, x):
        if phase == 0:
            a, b = 2 * h + lax.div(u, RING), lax.rem(u, RING)
            self.f[(col, b, a) if col == 1 else (col, a, b)] = x
        elif phase == 1:
            self.f2[col, 2 * h + u] = x
        else:
            self.last(col, h, x)

    def each(self, phase, body):
        units = (FAMILY, 2, 1)[phase]
        if units == 1:
            body(0)
        else:
            lax.fori_loop(0, units, lambda u, _: body(u), None)

    def start(self, phase, col, d, slot, rel, h):
        copy = self.hop(phase, col, d, slot, self.source(phase, col, rel, h), self.inbox(phase, col, d, slot))
        copy.start()
        self.sent.append(copy)

    def arrived(self, phase, col, d, slot):
        box = self.inbox(phase, col, d, slot)
        self.hop(phase, col, d, slot, box, box).wait_recv()

    def ready(self, phase, col, rel):
        if phase == 0:
            for wait in self.swaps[col, rel]:
                wait()

    def far(self, phase):
        for col in range(COLOURS):
            self.ready(phase, col, 2)
            for d in range(2):
                self.each(phase, lambda u: self.store(phase, col, 2, d, u, self.term(phase, col, 2, d, u)))
                self.start(phase, col, d, 0, 2, d)

    def straight(self, phase):
        for col in range(COLOURS):
            for d, rel in AHEAD:
                self.ready(phase, col, rel)
                self.each(phase, lambda u: self.store(phase, col, rel, 1 - d, u, self.term(phase, col, rel, 1 - d, u)))
                self.start(phase, col, d, 1, rel, 1 - d)

    def through(self, phase):
        for col in range(COLOURS):
            for d, rel in AHEAD:
                self.arrived(phase, col, d, 0)
                self.each(phase, lambda u: self.store(phase, col, rel, d, u, self.term(phase, col, rel, d, u) + self.value(phase, col, d, 0, u)))
                self.start(phase, col, d, 2, rel, d)

    def close(self, phase):
        for col in range(COLOURS):
            self.ready(phase, col, 0)
            for d in range(2):
                for slot in (1, 2):
                    self.arrived(phase, col, d, slot)
            for h in range(2):
                self.each(phase, lambda u: self.final(phase, col, h, u, self.term(phase, col, 0, h, u) + self.value(phase, col, 0, 2 - h, u)
                                                      + self.value(phase, col, 1, 1 + h, u)))


def _comm(g_ref, *rest):
    w_refs, rest = rest[:MATRICES], rest[MATRICES:]
    m_refs, v_refs, rest = rest[:MATRICES], rest[MATRICES:14], rest[14:]
    dh_ref, a_ref, q_ref, k_ref, v_ref, ot_ref, lse_ref, angle_ref, wo_ref, out_ref, gq_ref, *rest = rest
    wn_refs, rest = rest[:MATRICES], rest[MATRICES:]
    boxes, rest = (rest[:MATRICES], rest[MATRICES:14]), rest[14:]
    (s_ref, r0_ref, mine_ref, r1_ref, piece_ref, gb_ref, gf_ref, wt_ref, ow_ref, ou_ref, ob_ref, wb_ref, wv_ref, ps_ref, px_ref, py_ref, p8_ref,
     dqkv_s, dqt_s, dk_s, dv_s, do_s, ring_send, ring_recv, d2d_send, d2d_recv, load_sem, w_sem, g8_send, g8_recv, ps_send, ps_recv,
     w8_send, w8_recv, od_send, od_recv, ol_sem) = rest
    me = lax.axis_index("dp")
    core = lax.rem(me, 2)
    at = [lax.rem(lax.div(me, 32), RING), lax.rem(lax.div(me, FAMILY), RING), lax.rem(lax.div(me, 2), RING)]
    group = lax.div(me, FAMILY)
    mine = lax.rem(me, FAMILY)

    def device(axis, by):
        return me + (lax.rem(at[axis] + by, RING) - at[axis]) * (32, FAMILY, 2)[axis]

    partner = me + 1 - 2 * core
    family = [group * FAMILY + lax.rem(mine + k, FAMILY) for k in range(1, FAMILY)]
    friends = [device(axis, by) for axis in (0, 1) for by in (1, 2, COLOURS)] + family
    barrier = pltpu.get_barrier_semaphore()
    for one in friends:
        pl.semaphore_signal(barrier, inc=1, device_id={"dp": one}, device_id_type=MESH)

    def remote(src, dst, send, recv, to):
        return pltpu.make_async_remote_copy(src_ref=src, dst_ref=dst, send_sem=send, recv_sem=recv, device_id={"dp": to}, device_id_type=MESH)

    def hop(base):
        def make(phase, col, d, slot, src, dst):
            n = (((base * COLOURS + phase) * COLOURS + col) * 2 + d) * COLOURS + slot
            return remote(src, dst, ring_send.at[n], ring_recv.at[n], device(ORDER[col][phase], 1 if d == 0 else COLOURS))

        return make

    chunks = [(n, col, rel, _where(ORDER[col][0], _near(at[ORDER[col][0]] + rel))) for n, (rel, col) in enumerate((r, c) for r in WAY for c in range(COLOURS))]
    loads, swaps = {}, []
    for n, col, rel, here in chunks:
        loads[n] = pltpu.make_async_copy(g_ref.at[(*here, core, col)], s_ref.at[(*here, col)], load_sem.at[n])
        loads[n].start()
    for k in range(MATRICES):
        pltpu.make_async_copy(w_refs[k].at[group], wn_refs[k], w_sem.at[k]).start()
    pl.semaphore_wait(barrier, len(friends))
    first = {}
    for n, col, rel, here in chunks:
        copy = remote(g_ref.at[(*here, 1 - core, col)], r0_ref.at[(*here, col)], d2d_send.at[n], d2d_recv.at[n], partner)
        copy.start()
        swaps.append(copy)
        first[col, rel] = (loads[n].wait, copy.wait_recv)

    squares = []

    def final(base, unit):
        def put(col, h, x):
            x = x.astype(bf16)
            at_row = base + col * unit + h * (unit // 2)
            piece_ref[at_row : at_row + unit // 2, :] = x
            x = x.astype(f32)
            squares.append(jnp.sum((x * x).reshape(unit // GROUPS, FAMILY, LANES), axis=0))

        return put

    part = UNITS[0] * COLOURS
    gated_sum = _Sum(UNITS[0], at, hop(0), first, lambda here, col: s_ref.at[(*here, col)], r0_ref, boxes[0], final(0, UNITS[0]))

    def put(row, x):
        unit, end = UNITS[1], row + x.shape[1]
        begin = row
        while row < end:
            n, low = row // unit, row % unit
            size = min(unit - low, end - row)
            z, c, col = n // 6, n // COLOURS % 2, n % COLOURS
            mine_ref[:, :, z, c, col, low : low + size, :] = x[:, row - begin : row - begin + size].reshape(RING, RING, size, LANES).astype(bf16)
            row += size

    def back(i):
        _back_step(i, dh_ref, q_ref, k_ref, v_ref, ot_ref, lse_ref, angle_ref, wo_ref, dqkv_s, dqt_s, dk_s, dv_s, do_s)

    back(0)
    _back_put(put, _dot(ot_ref[...], dh_ref[...]), TABLE[COLOURS][0])
    put(OTHERS - 48, jnp.zeros((GROUPS, 48, LANES), f32))
    gated_sum.far(0)
    back(1)
    gated_sum.straight(0)
    back(2)
    gated_sum.through(0)
    back(COLOURS)
    gated_sum.close(0)
    gated_sum.far(1)
    gated_sum.straight(1)
    _back_qkv(put, a_ref, angle_ref, dqkv_s, dk_s, dv_s)

    second = {}
    for n, col, rel, here in chunks:
        copy = remote(mine_ref.at[(*here, 1 - core, col)], r1_ref.at[(*here, col)], d2d_send.at[CHUNKS + n], d2d_recv.at[CHUNKS + n], partner)
        copy.start()
        swaps.append(copy)
        second[col, rel] = (copy.wait_recv,)
    gated_sum.through(1)
    other_sum = _Sum(UNITS[1], at, hop(1), second, lambda here, col: mine_ref.at[(*here[:COLOURS], core, col)], r1_ref, boxes[1], final(part, UNITS[1]))
    other_sum.far(0)
    gated_sum.close(1)
    gated_sum.far(2)
    gated_sum.straight(2)
    other_sum.straight(0)
    other_sum.through(0)
    gated_sum.through(2)
    other_sum.close(0)
    other_sum.far(1)
    other_sum.straight(1)
    gated_sum.close(2)

    for k, (_, blocks, rows, own, begin, step) in enumerate(TABLE):
        pltpu.make_async_copy(w_refs[k].at[group], wn_refs[k], w_sem.at[k]).wait()
        for j in range(blocks):
            wt_ref[j % RING, :rows, :] = wn_refs[k][:, _lanes(j)].astype(f32)
            ow_ref[begin + j * step : begin + j * step + own, :] = wt_ref[j % RING, pl.ds(mine * own, own), :]
    other_sum.through(1)
    other_sum.close(1)
    other_sum.far(2)
    other_sum.straight(2)
    other_sum.through(2)
    other_sum.close(2)

    size = COLOURS * UNIT
    pending, g8, w8 = [], [], []
    for k in range(MATRICES):
        copy = remote(piece_ref, gb_ref.at[mine], g8_send.at[k], g8_recv.at[6 - k], family[k])
        copy.start()
        g8.append(copy)

    def swap_squares(total, which, targets, box):
        n, base = len(targets), COLOURS * which
        ps_ref[which] = total
        for k, to in enumerate(targets):
            copy = remote(ps_ref.at[which], box.at[n - 1 - k], ps_send.at[base + k], ps_recv.at[base + n - 1 - k], to)
            copy.start()
            pending.append(copy)
        for k in range(n):
            remote(box.at[k], box.at[k], ps_send.at[base + k], ps_recv.at[base + k], targets[0]).wait_recv()
            total = total + box[k]
        return total

    total = sum(squares[1:], squares[0])
    total = swap_squares(total, 0, [device(0, by) for by in (1, 2, COLOURS)], px_ref)
    total = swap_squares(total, 1, [device(1, by) for by in (1, 2, COLOURS)], py_ref)
    total = swap_squares(total, 2, family, p8_ref)
    mean = jnp.sum(total) / float(sum(a * b for a, b in SHAPE.values()))
    factor = jnp.minimum(1.0, 0.5 * lax.rsqrt(jnp.full((FAMILY, LANES), mean, f32) + 1e-30))

    def spread(n, x):
        gf_ref[pl.ds(pl.multiple_of(n * part, FAMILY), part), :] = x[:part].astype(f32)
        gf_ref[pl.ds(pl.multiple_of(GATED + n * (size - part), FAMILY), size - part), :] = x[part:].astype(f32)

    spread(mine, piece_ref[...])
    for k in range(MATRICES):
        n = lax.rem(mine + k + 1, FAMILY)
        remote(piece_ref, gb_ref.at[n], g8_send.at[k], g8_recv.at[k], family[k]).wait_recv()
        spread(n, gb_ref[n])

    for k, (_, blocks, rows, own, begin, step) in enumerate(TABLE):
        for j in range(blocks):
            lanes = _lanes(j)
            to = slice(begin + j * step, begin + j * step + own)
            g = gf_ref[pl.ds(_flat(k) + j * rows + mine * own, own), :] * factor[:1]
            w = ow_ref[to, :]
            m = 0.9 * m_refs[k][_at(k, lanes)] + 0.1 * g
            v = 0.95 * v_refs[k][_at(k, lanes)] + 0.05 * g * g
            ou_ref[to, :] = w - 0.02 * (m * lax.rsqrt(v + 1e-8) + 0.1 * w)
            gq_ref[to, :] = g
    ob_ref[...] = ou_ref[...].astype(bf16)

    for k in range(MATRICES):
        copy = remote(ob_ref, wb_ref.at[mine], w8_send.at[k], w8_recv.at[6 - k], family[k])
        copy.start()
        w8.append(copy)
    wb_ref[mine] = ob_ref[...]
    for k in range(MATRICES):
        n = lax.rem(mine + k + 1, FAMILY)
        remote(ob_ref, wb_ref.at[n], w8_send.at[k], w8_recv.at[k], family[k]).wait_recv()

    def gathered(n):
        for k, (_, blocks, rows, own, begin, step) in enumerate(TABLE):
            for j in range(blocks):
                to = pl.ds(_flat(k) + j * rows + n * own, own)
                gf_ref[to, :] = wb_ref[n, begin + j * step : begin + (j + 1) * step, :].astype(f32)[:own]

    lax.fori_loop(0, FAMILY, lambda n, _: gathered(n), None)
    here = tuple(at)

    def own_rows(low, high):
        base, n = (0, part) if low < part else (GATED - part, size - part)
        return gf_ref[pl.ds(pl.multiple_of(mine * n, FAMILY) + base + low, high - low), :].astype(bf16)

    for col in range(COLOURS):
        low, high = col * UNIT, (col + 1) * UNIT
        for a, b in ((low, min(high, part)), (max(low, part), high)):
            if a < b:
                wv_ref[(*here, col, slice(a - low, b - low))] = own_rows(a, b)

    outs = []

    def hand_on(col, rel):
        axis = ORDER[col][0]
        q = _near(at[axis] + rel)
        src, dst = wv_ref.at[(*_where(axis, q), col)], out_ref.at[(*_where(axis, q), core, col)]
        n = col * RING + rel
        copy = remote(src, dst, od_send.at[n], od_recv.at[n], partner)
        copy.start()
        local = pltpu.make_async_copy(src, dst, ol_sem.at[n])
        local.start()
        outs.append((copy, local))

    def gather_phase(phase, chunk, done):
        def start(col, d, slot, rel, h):
            copy = hop(2)(phase, col, d, slot, chunk(col, rel, h), chunk(col, rel, h))
            copy.start()
            pending.append(copy)

        def arrived(col, d, slot, rel, h):
            hop(2)(phase, col, d, slot, chunk(col, rel, h), chunk(col, rel, h)).wait_recv()

        for slot in range(2):
            for col in range(COLOURS):
                for d in range(2):
                    start(col, d, slot, 0, d if slot == 0 else 1 - d)
        for col in range(COLOURS):
            done(col, 0)
        for col in range(COLOURS):
            for d, rel in BEHIND:
                arrived(col, d, 0, rel, d)
                start(col, d, 2, rel, d)
        for col in range(COLOURS):
            for d, rel in BEHIND:
                arrived(col, d, 1, rel, 1 - d)
                done(col, rel)
        for col in range(COLOURS):
            for d in range(2):
                arrived(col, d, 2, 2, d)
            done(col, 2)

    cut = UNIT // 2

    def last_chunk(col, rel, h):
        spot = list(at)
        spot[ORDER[col][2]] = _near(at[ORDER[col][2]] + rel)
        return wv_ref.at[(*spot, col, pl.ds(h * cut, cut))]

    def middle_chunk(col, rel, h):
        spot = list(at)
        spot[ORDER[col][1]] = _near(at[ORDER[col][1]] + rel)
        spot[ORDER[col][2]] = _half(h)
        return wv_ref.at[(*spot, col)]

    def whole_chunk(col, rel, h):
        axis = ORDER[col][0]
        return wv_ref.at[(*_where(axis, _near(at[axis] + rel), _half(h)), col)]

    gather_phase(2, last_chunk, lambda col, rel: None)
    gather_phase(1, middle_chunk, lambda col, rel: None)
    gather_phase(0, whole_chunk, hand_on)

    for copy in swaps + gated_sum.sent + other_sum.sent + pending + g8 + w8:
        copy.wait_send()
    for copy, local in outs:
        copy.wait_send()
        local.wait()
    for n, (col, rel) in enumerate((c, r) for c in range(COLOURS) for r in range(RING)):
        axis = ORDER[col][0]
        dst = out_ref.at[(*_where(axis, _near(at[axis] + rel)), 1 - core, col)]
        remote(dst, dst, od_send.at[n], od_recv.at[n], partner).wait_recv()


def sum_step_gather(g, weights, m, v, back):
    vmem, dma = pltpu.VMEM, pltpu.SemaphoreType.DMA
    hbm, local = pl.BlockSpec(memory_space=pl.ANY), pl.BlockSpec(memory_space=vmem)
    cube, sides = (RING, RING, RING), (COLOURS, 2, COLOURS)
    scratch = [vmem((SHAPE[name][0] // GROUPS, SHAPE[name][1]), bf16) for name in NAMES]
    for unit in UNITS:
        row = (unit, LANES)
        scratch += [vmem((*sides, 2, RING, *row), bf16), vmem((COLOURS, RING, RING, *row), f32), vmem((*sides, 2, *row), bf16), vmem((COLOURS, COLOURS, RING, *row), bf16),
                    vmem((COLOURS, RING, *row), f32), vmem((*sides, unit // 2, LANES), bf16), vmem((COLOURS, COLOURS, *row), bf16)]
    own, tile, head = (OWN, LANES), (FAMILY, LANES), (TOKENS, HEAD)
    scratch += [vmem((*cube, COLOURS, UNITS[0], LANES), bf16), vmem((*cube, COLOURS, UNITS[0], LANES), bf16), vmem((*cube, 2, COLOURS, UNITS[1], LANES), bf16),
                vmem((*cube, COLOURS, UNITS[1], LANES), bf16), vmem((COLOURS * UNIT, LANES), bf16), vmem((FAMILY, COLOURS * UNIT, LANES), bf16), vmem((FLAT, LANES), f32),
                vmem((RING, 200, LANES), f32), vmem(own, f32), vmem(own, f32), vmem(own, bf16), vmem((FAMILY, *own), bf16), vmem((*cube, COLOURS, UNIT, LANES), bf16)]
    scratch += [vmem((n, *tile), f32) for n in (COLOURS, COLOURS, COLOURS, MATRICES)]
    scratch += [vmem((TOKENS, (HEADS + 2) * HEAD), bf16), vmem((HEAD, HEADS * BACK), f32), vmem(head, f32), vmem(head, f32), vmem((HEADS, BACK, HEAD), bf16)]
    scratch += [dma((n,)) for n in (162, 162, 24, 24, CHUNKS, MATRICES, MATRICES, MATRICES, 13, 13, MATRICES, MATRICES, CHUNKS, CHUNKS, CHUNKS)]
    return pl.pallas_call(
        _comm,
        out_shape=[jax.ShapeDtypeStruct((*cube, 2, COLOURS, UNIT, LANES), bf16), jax.ShapeDtypeStruct(own, f32)],
        in_specs=[hbm] * FAMILY + [local] * 23,
        out_specs=[hbm, local],
        scratch_shapes=scratch,
        compiler_params=pltpu.CompilerParams(collective_id=0, has_side_effects=True, vmem_limit_bytes=67043328),
    )(g, *[w.reshape(GROUPS, w.shape[1] // GROUPS, w.shape[2]) for w in weights], *_rows(m), *_rows(v), *back)


def _finish(flat_ref, gq_ref, *rest):
    m_refs, v_refs, w_refs, mo_refs, vo_refs = (rest[i : i + MATRICES] for i in range(0, 35, MATRICES))

    @pl.when(pl.program_id(0) == 0)
    def _():
        for k, (_, blocks, _, own, first, step) in enumerate(TABLE):
            for j in range(blocks):
                at = _at(k, _lanes(j))
                g = gq_ref[first + j * step : first + j * step + own, :]
                mo_refs[k][at] = 0.9 * m_refs[k][at] + 0.1 * g
                vo_refs[k][at] = 0.95 * v_refs[k][at] + 0.05 * g * g

    for k, (_, blocks, rows, _, _, _) in enumerate(TABLE):
        lengths = (COLOURS * UNITS[1], GATED) if k < RING else (COLOURS * UNITS[0], 0)
        for j in range(blocks):
            row, to = _flat(k) + j * rows - lengths[1], 0
            while to < rows:
                n, low = row // lengths[0], row % lengths[0]
                some = min(lengths[0] - low, rows - to)
                low += n * COLOURS * UNIT + (COLOURS * UNITS[0] if k < RING else 0)
                w_refs[k][0, to : to + some, _lanes(j)] = flat_ref[0, low : low + some, :]
                row, to = row + some, to + some


def finish(flat, gq, m, v):
    whole = pl.BlockSpec(memory_space=pltpu.VMEM)
    old = [*_rows(m), *_rows(v)]
    shapes = [(1, *SHAPE[name]) for name in NAMES]
    out = pl.pallas_call(
        _finish,
        grid=(GROUPS,),
        out_shape=[jax.ShapeDtypeStruct(shape, jnp.bfloat16) for shape in shapes] + [jax.ShapeDtypeStruct(a.shape, a.dtype) for a in old],
        in_specs=[pl.BlockSpec((1, FLAT, LANES), lambda i: (i, 0, 0)), whole] + [whole] * 14,
        out_specs=[pl.BlockSpec((1, shape[1] // GROUPS, shape[2]), lambda i: (0, i, 0)) for shape in shapes] + [whole] * 14,
        compiler_params=pltpu.CompilerParams(vmem_limit_bytes=VMEM),
    )(flat.reshape(GROUPS, FLAT, LANES), gq, *old)
    moments = [new.reshape(1, *new.shape) if new.ndim == 2 else new.transpose(1, 0, 2) for new in out[MATRICES:]]
    return (*out[:MATRICES], *moments)


def solution(mesh):
    def step(x, dy, *arrays):
        weights, m, v = (arrays[i : i + MATRICES] for i in (0, MATRICES, 14))
        w = dict(zip(NAMES, weights, strict=True))
        plain = {name: w[name][0] for name in ("wq", "wk", "wv", "wo")}
        a, q, k, value, ot, lse, h = attend(x[0], plain)
        g, dh = gated(h, dy[0], w)
        back = (dh, a, q, k, value, ot, lse, _angles(), plain["wo"])
        flat, gq = sum_step_gather(g.reshape(RING, RING, RING, 2, COLOURS, UNITS[0], LANES), weights, m, v, back)
        return finish(flat, gq, m, v)

    states, all_of, cut = P(("rep", "dp")), P(), P(None, "dp")
    return jax.shard_map(
        step,
        mesh=mesh,
        in_specs=(states, states) + (all_of,) * MATRICES + (cut,) * 14,
        out_specs=(P("rep"),) * MATRICES + (P("rep", "dp"),) * 14,
        check_vma=False,
    )
```

```python
import functools

import jax
import jax.numpy as jnp
import numpy as np
from jax import lax
from jax.experimental import pallas as pl
from jax.experimental.pallas import tpu as pltpu
from jax.sharding import PartitionSpec as P

NEG = -1e30
HIDDEN = 2 * NEG
LOG2E = 1.4426950408889634
VMEM = 56 * 2**20
NAMES = ("wq", "wk", "wv", "wo", "w_gate", "w_up", "w_down")
TOKENS, D, HEADS, HEAD, FF = 1024, 640, 8, 128, 3200
SCALE = HEAD**-0.5
E = SCALE * LOG2E
THETA = 10000
f32, bf16 = jnp.float32, jnp.bfloat16


def _dot(a, b, ca=1, cb=0):
    return lax.dot_general(a, b, (((ca,), (cb,)), ((), ())), preferred_element_type=f32)


def _dot_t(a, b):
    return _dot(a, b, 1, 1)


def _lanes(k):
    return slice(k * 128, (k + 1) * 128)


def _scale(wide):
    return lax.rsqrt(jnp.mean(wide * wide, -1, keepdims=True) + 1e-6)


def _normed(wide):
    return wide * _scale(wide)


HALF = HEAD // 2


def _angles():
    angle = np.arange(TOKENS, dtype=np.float32)[:, None] * np.float32(THETA) ** (-np.arange(HALF, dtype=np.float32) / np.float32(HALF))
    return np.concatenate([np.cos(angle), np.sin(angle)], 1).astype(np.float32)


def _spread(angles):
    other = pltpu.roll(angles, HALF, 1)
    low = lax.broadcasted_iota(jnp.int32, angles.shape, 1) < HALF
    return jnp.where(low, angles, other), jnp.where(low, -other, angles)
LANES, GROUPS = 128, 16
BOTH, COLOURS, RING, FAMILY, MATRICES, CHUNKS = 2, 3, 4, 8, 7, 12


BQ, BK = 512, 256


def _attend(x_ref, angle_ref, wq_ref, wk_ref, wv_ref, wo_ref, a_ref, q_ref, k_ref, v_ref, ot_ref, lse_ref, h_ref, ks, vts, top_s, mix_s):
    i = pl.program_id(0)
    a = _normed(x_ref[...].astype(f32)).astype(bf16)
    a_ref[...] = a
    cos, sin = _spread(angle_ref[...])

    def turned(t):
        t = t.astype(bf16).astype(f32)
        return (t * cos + pltpu.roll(t, HALF, 1) * sin).astype(bf16)

    k = turned(_dot(a, wk_ref[...]))
    v = _dot(a, wv_ref[...]).astype(bf16)
    k_ref[...] = k
    v_ref[...] = v
    here = pl.ds(pl.multiple_of(i * BQ, BQ), BQ)
    ks[here, :] = k
    vts[:HEAD, here] = v.T
    vts[HEAD:, here] = jnp.ones((8, BQ), bf16)
    q = _dot(a, wq_ref[...])
    for n in range(HEADS):
        q_ref[n] = turned(q[:, _lanes(n)])
    top_s[...] = jnp.full(top_s.shape, NEG, f32)
    mix_s[...] = jnp.zeros(mix_s.shape, f32)

    def block(j, low, masked):
        keys = pl.ds(pl.multiple_of(j * BK, BK), BK)
        scores = [_dot_t(ks[keys, :], q_ref[n, low:, :]) for n in range(HEADS)]
        if masked:
            hidden = lax.broadcasted_iota(jnp.int32, (BK, BQ - low), 1) < lax.broadcasted_iota(jnp.int32, (BK, BQ - low), 0)
        values = vts[:, keys]
        weights, keeps = [], []
        for n, s in enumerate(scores):
            if masked:
                s = jnp.where(hidden, HIDDEN, s)
            old = top_s[n : n + 1, low:]
            top = jnp.maximum(old, s.max(axis=0, keepdims=True))
            top_s[n : n + 1, low:] = top
            weights.append(jnp.exp2((s - top) * E).astype(bf16))
            keeps.append(jnp.exp2((old - top) * E))
        for n, (p, keep) in enumerate(zip(weights, keeps)):
            mix_s[n, :, low:] = mix_s[n, :, low:] * keep + _dot(values, p)

    per = BQ // BK
    lax.fori_loop(0, per * i, lambda j, _: block(j, 0, False), None)
    for n in range(per):
        block(per * i + n, n * BK, True)
    outs = []
    for n in range(HEADS):
        total = mix_s[n, HEAD : HEAD + 1, :]
        out = (mix_s[n, :HEAD, :] * (1 / total)).astype(bf16)
        ot_ref[_lanes(n), :] = out
        outs.append(out.T)
        lse_ref[n : n + 1, :] = top_s[n : n + 1, :] * SCALE + jnp.log(total)
    more = _dot(jnp.concatenate(outs, axis=1), wo_ref[...]).astype(bf16)
    h_ref[...] = (x_ref[...].astype(f32) + more.astype(f32)).astype(bf16)


def attend(x, w):
    whole = pl.BlockSpec(memory_space=pltpu.VMEM)
    rows = lambda width: pl.BlockSpec((BQ, width), lambda i: (i, 0))
    columns = lambda height: pl.BlockSpec((height, BQ), lambda i: (0, i))
    shape = jax.ShapeDtypeStruct
    return pl.pallas_call(
        _attend,
        grid=(TOKENS // BQ,),
        in_specs=[rows(D), rows(HEAD)] + [whole] * 4,
        out_specs=[rows(D), pl.BlockSpec((HEADS, BQ, HEAD), lambda i: (0, i, 0)), rows(HEAD), rows(HEAD), columns(HEADS * HEAD), columns(HEADS), rows(D)],
        out_shape=[shape((TOKENS, D), bf16), shape((HEADS, TOKENS, HEAD), bf16), shape((TOKENS, HEAD), bf16), shape((TOKENS, HEAD), bf16),
                   shape((HEADS * HEAD, TOKENS), bf16), shape((HEADS, TOKENS), f32), shape((TOKENS, D), bf16)],
        scratch_shapes=[pltpu.VMEM((TOKENS, HEAD), bf16), pltpu.VMEM((HEAD + 8, TOKENS), bf16), pltpu.VMEM((HEADS, BQ), f32),
                        pltpu.VMEM((HEADS, HEAD + 8, BQ), f32)],
        compiler_params=pltpu.CompilerParams(dimension_semantics=("arbitrary",), vmem_limit_bytes=VMEM),
    )(x, _angles(), *[w[name] for name in ("wq", "wk", "wv", "wo")])


BF = 256
LAST = FF // BF
CHUNK = 512


def _gated(h_ref, dy_ref, wg_ref, wu_ref, wd_ref, g_ref, dh_ref, b_s, bt_s, dyt_s, acc_s, hid_s, dg_s, du_s, stage, down_s, zero_s, sem, end_sem):
    j = pl.program_id(0)
    slot = lax.rem(j, 2)
    firsts = [TABLE[NAMES.index(name)][0] for name in ("w_gate", "w_up", "w_down")]
    rows = D // GROUPS
    ends = 3 * FF * D // GROUPS // LANES

    def put(n, at, size):
        where = pl.ds(pl.multiple_of(firsts[n] + at * (rows * BF // LANES), 8), size)
        return pltpu.make_async_copy(stage.at[n, slot, :, pl.ds(0, size)], g_ref.at[:, where], sem.at[n, slot])

    @pl.when(j == 0)
    def _():
        b = _normed(h_ref[...].astype(f32)).astype(bf16)
        b_s[...] = b
        bt_s[...] = b.T
        dyt_s[...] = dy_ref[...].T
        acc_s[...] = jnp.zeros(acc_s.shape, f32)
        zero_s[...] = jnp.zeros(zero_s.shape, bf16)
        pltpu.make_async_copy(zero_s, g_ref.at[:, pl.ds(ends, GATED - ends)], end_sem.at[0]).start()

    left = FF - j * BF
    inside = lax.broadcasted_iota(jnp.int32, (D, BF), 1) < left
    wg, wu = (jnp.where(inside, ref[0], jnp.zeros((), bf16)) for ref in (wg_ref, wu_ref))
    wd = jnp.where(lax.broadcasted_iota(jnp.int32, (BF, D), 0) < left, wd_ref[0], jnp.zeros((), bf16))
    for at in range(0, TOKENS, CHUNK):
        here = slice(at, at + CHUNK)
        gate, up = _dot(b_s[here, :], wg), _dot(b_s[here, :], wu)
        dhid = _dot_t(dy_ref[here, :], wd).astype(bf16).astype(f32)
        share = 1 / (1 + jnp.exp(-gate))
        silu = gate * share
        hid_s[here, :] = (silu * up).astype(bf16)
        dgate = (dhid * up * (share * (1 + gate * (1 - share)))).astype(bf16)
        dup = (dhid * silu).astype(bf16)
        dg_s[here, :] = dgate
        du_s[here, :] = dup
        acc_s[here, :] += _dot_t(dgate, wg) + _dot_t(dup, wu)

    @pl.when(j >= 2)
    def _():
        for n in range(2):
            put(n, j - 2, rows * BF // LANES).wait()

    for n, one in enumerate((dg_s, du_s)):
        term = _dot(bt_s[...], one[...])
        for k in range(BF // LANES):
            stage[n, slot, :, k * rows : (k + 1) * rows, :] = term[:, _lanes(k)].reshape(GROUPS, rows, LANES).astype(bf16)
    term = _dot(dyt_s[...], hid_s[...]).T
    for k in range(D // LANES):
        down_s[k, pl.ds(pl.multiple_of(j * BF, BF), BF), :] = term[:, _lanes(k)].astype(bf16)

    @pl.when(j < LAST)
    def _():
        for n in range(2):
            put(n, j, rows * BF // LANES).start()

    @pl.when(j == LAST)
    def _():
        for n in range(2):
            put(n, j, rows * (FF % BF) // LANES).start()
        per = FF // GROUPS
        for k in range(D // LANES):
            for n in range(GROUPS):
                pltpu.make_async_copy(down_s.at[k, pl.ds(n * per, per)], g_ref.at[n, pl.ds(firsts[2] + k * per, per)], end_sem.at[1]).start()
        for at in range(0, TOKENS, CHUNK):
            here = slice(at, at + CHUNK)
            db = acc_s[here, :].astype(bf16).astype(f32)
            h = h_ref[here, :].astype(f32)
            s = _scale(h)
            through = db * s - h * (s * s * s * jnp.mean(db * h, -1, keepdims=True))
            dh_ref[here, :] = (dy_ref[here, :].astype(f32) + through.astype(bf16).astype(f32)).astype(bf16)
        for n in range(2):
            put(n, j, rows * (FF % BF) // LANES).wait()
            pltpu.make_async_copy(stage.at[n, 1 - slot], stage.at[n, 1 - slot], sem.at[n, 1 - slot]).wait()
        pltpu.make_async_copy(zero_s, g_ref.at[:, pl.ds(ends, GATED - ends)], end_sem.at[0]).wait()
        whole = g_ref.at[:, pl.ds(firsts[2], ends - firsts[2])]
        pltpu.make_async_copy(whole, whole, end_sem.at[1]).wait()


def gated(h, dy, w):
    vmem = pltpu.VMEM
    whole = pl.BlockSpec(memory_space=vmem)
    across = pl.BlockSpec((1, D, BF), lambda j: (0, 0, j))
    pad = GATED - 3 * FF * D // GROUPS // LANES
    return pl.pallas_call(
        _gated,
        grid=(LAST + 1,),
        in_specs=[whole, whole, across, across, pl.BlockSpec((1, BF, D), lambda j: (0, j, 0))],
        out_specs=[pl.BlockSpec(memory_space=pl.ANY), whole],
        out_shape=[jax.ShapeDtypeStruct((GROUPS, GATED, LANES), bf16), jax.ShapeDtypeStruct((TOKENS, D), bf16)],
        scratch_shapes=[vmem((TOKENS, D), bf16), vmem((D, TOKENS), bf16), vmem((D, TOKENS), bf16), vmem((TOKENS, D), f32),
                        vmem((TOKENS, BF), bf16), vmem((TOKENS, BF), bf16), vmem((TOKENS, BF), bf16),
                        vmem((2, 2, GROUPS, D // GROUPS * BF // LANES, LANES), bf16), vmem((D // LANES, (LAST + 1) * BF, LANES), bf16), vmem((GROUPS, pad, LANES), bf16),
                        pltpu.SemaphoreType.DMA((2, 2)), pltpu.SemaphoreType.DMA((2,))],
        compiler_params=pltpu.CompilerParams(dimension_semantics=("arbitrary",), vmem_limit_bytes=VMEM),
    )(h, dy, *[w[name] for name in ("w_gate", "w_up", "w_down")])


BACK = 256


def _back_step(i, dh_ref, q_ref, k_ref, v_ref, ot_ref, lse_ref, angle_ref, wo_ref, dqkv_s, dqt_s, dk_s, dv_s, do_s):
    here = slice(i * BACK, (i + 1) * BACK)
    if i == 0:
        dk_s[...] = jnp.zeros(dk_s.shape, f32)
        dv_s[...] = jnp.zeros(dv_s.shape, f32)
    dqt_s[...] = jnp.zeros(dqt_s.shape, f32)
    dh, wo = dh_ref[here, :], wo_ref[...]
    dot = _dot_t(wo, dh).astype(bf16).astype(f32) * ot_ref[:, here].astype(f32)
    delta = [dot[_lanes(n), :].sum(axis=0, keepdims=True) for n in range(HEADS)]
    dout = _dot_t(dh, wo).astype(bf16)
    for n in range(HEADS):
        do_s[n] = dout[:, _lanes(n)]
    pairs = range(0, HEADS, 2)
    beside = lambda rows, n: jnp.concatenate([rows[n], rows[n + 1]], axis=1)
    lses = [lse_ref[n : n + 1, here] * LOG2E for n in range(HEADS)]

    def block(j, masked):
        keys = pl.ds(j * BACK if masked else pl.multiple_of(j * BACK, BACK), BACK)
        k, v = k_ref[keys, :], v_ref[keys, :]
        kt = k.T
        if masked:
            place = lax.broadcasted_iota(jnp.int32, (BACK, 2 * BACK), 1)
            hidden = jnp.where(place < BACK, place, place - BACK) < lax.broadcasted_iota(jnp.int32, (BACK, 2 * BACK), 0)
        for some in (pairs[:2], pairs[2:]):
            qs = [q_ref[n : n + 2, here, :].reshape(2 * BACK, HEAD) for n in some]
            dos = [do_s[n : n + 2].reshape(2 * BACK, HEAD) for n in some]
            scores = [_dot_t(k, q) for q in qs]
            dps = [_dot_t(v, one) for one in dos]
            for n, q, do, score, dp in zip(some, qs, dos, scores, dps):
                p = jnp.exp2(score * E - beside(lses, n))
                if masked:
                    p = jnp.where(hidden, 0.0, p)
                ds = (p * (dp - beside(delta, n))).astype(bf16)
                dv_s[keys, :] += _dot(p.astype(bf16), do)
                dk_s[keys, :] += _dot(ds, q)
                dqt_s[:, n * BACK : (n + 2) * BACK] += _dot(kt, ds)

    lax.fori_loop(0, i, lambda j, _: block(j, False), None)
    block(i, True)
    both = angle_ref[here, :].T
    cost, sint = both[:HALF], both[HALF:]
    for n in range(HEADS):
        t = (dqt_s[:, n * BACK : (n + 1) * BACK] * SCALE).astype(bf16).astype(f32)
        one, two = t[:HALF], t[HALF:]
        t = jnp.concatenate([one * cost + two * sint, two * cost - one * sint], axis=0)
        dqkv_s[here, _lanes(n)] = t.astype(bf16).T


def _back_put(put, term, first):
    rows = term.shape[0] // GROUPS
    for k in range(term.shape[1] // LANES):
        put(first + k * rows, term[:, _lanes(k)].reshape(GROUPS, rows, LANES))


def _back_qkv(put, a_ref, angle_ref, dqkv_s, dk_s, dv_s):
    wide = HEADS * HEAD
    cos, sin = _spread(angle_ref[...])
    t = (dk_s[...] * SCALE).astype(bf16).astype(f32)
    dqkv_s[:, wide : wide + HEAD] = (t * cos - pltpu.roll(t, HALF, 1) * sin).astype(bf16)
    dqkv_s[:, wide + HEAD :] = dv_s[...].astype(bf16)
    _back_put(put, _dot(a_ref[...].T, dqkv_s[...]), TABLE[0][0])


MESH, ALL = pl.DeviceIdType.MESH, slice(None)
SHAPE = {"wq": (640, 1024), "wk": (640, 128), "wv": (640, 128), "wo": (1024, 640), "w_gate": (640, 3200), "w_up": (640, 3200), "w_down": (3200, 640)}
UNIT = 160
UNITS = (LANES, 32)
GATED, OTHERS = 24 * UNITS[0], 24 * UNITS[1]
FLAT = GATED + OTHERS
ORDER = ((0, 1, 2), (1, 2, 0), (2, 0, 1))
AHEAD, BEHIND = ((0, 1), (1, COLOURS)), ((0, COLOURS), (1, 1))
WAY = (2, 1, COLOURS, 0)


def _table():
    table, flat, mine = [], 0, 0
    for name in NAMES:
        rows, cols = SHAPE[name]
        flat = 0 if name == "w_gate" else flat
        blocks, group, own = cols // LANES, rows // GROUPS, rows // LANES
        table.append((flat, blocks, group, own, mine))
        flat += blocks * group
        mine += blocks * own
    return tuple(table)


TABLE, OWN = _table(), COLOURS * UNIT


def _flat(k):
    return TABLE[k][0] + (GATED if k < RING else 0)


def _at(k, lanes):
    return (ALL, lanes) if TABLE[k][COLOURS] % FAMILY == 0 else (ALL, 0, lanes)


def _rows(moments):
    return [one[0] if one.shape[1] % FAMILY == 0 else one.transpose(1, 0, BOTH) for one in moments]


def _near(q):
    return lax.rem(q, RING)


def _where(axis, q, first=ALL):
    return ((q, first, ALL), (first, q, ALL), (first, ALL, q))[axis]


def _place(axis, q, a, b):
    return ((q, a, b), (a, q, b), (a, b, q))[axis]


def _half(h):
    return pl.ds(BOTH * h, BOTH)


class _Sum:
    def __init__(self, unit, at, hop, swaps, own, other, boxes, final):
        self.unit, self.at, self.hop, self.swaps, self.own, self.other, self.last = unit, at, hop, swaps, own, other, final
        self.ra, self.f, self.rb, self.sb, self.f2, self.rc, self.sc = boxes
        self.sent, self.cut = [], unit // BOTH

    def spot(self, col, rel, h, u):
        axis = ORDER[col][0]
        return _place(axis, _near(self.at[axis] + rel), BOTH * h + lax.div(u, RING), lax.rem(u, RING))

    def chunk(self, phase, col, rel):
        return _near(self.at[ORDER[col][phase]] + rel)

    def rows(self, h):
        return slice(h * self.cut, (h + 1) * self.cut)

    def term(self, phase, col, rel, h, u):
        if phase == 0:
            here = self.spot(col, rel, h, u)
            return self.own(here, col)[...].astype(f32) + self.other[(*here, col)].astype(f32)
        if phase == 1:
            return self.f[col, self.chunk(1, col, rel), BOTH * h + u]
        return self.f2[col, self.chunk(BOTH, col, rel), self.rows(h)]

    def source(self, phase, col, rel, h):
        if phase == 0:
            axis = ORDER[col][0]
            return self.own(_where(axis, self.chunk(0, col, rel), _half(h)), col)
        return self.sb.at[col, rel - 1, _half(h)] if phase == 1 else self.sc.at[col, rel - 1, self.rows(h)]

    def store(self, phase, col, rel, h, u, x):
        x = x.astype(bf16)
        if phase == 0:
            self.own(self.spot(col, rel, h, u), col)[...] = x
        elif phase == 1:
            self.sb[col, rel - 1, BOTH * h + u] = x
        else:
            self.sc[col, rel - 1, self.rows(h)] = x

    def inbox(self, phase, col, d, slot):
        return (self.ra, self.rb, self.rc)[phase].at[col, d, slot]

    def value(self, phase, col, d, slot, u):
        box = self.inbox(phase, col, d, slot)
        box = (box.at[lax.div(u, RING), lax.rem(u, RING)] if phase == 0 else box.at[u] if phase == 1 else box)
        return box[...].astype(f32)

    def final(self, phase, col, h, u, x):
        if phase == 0:
            a, b = BOTH * h + lax.div(u, RING), lax.rem(u, RING)
            self.f[(col, b, a) if col == 1 else (col, a, b)] = x
        elif phase == 1:
            self.f2[col, BOTH * h + u] = x
        else:
            self.last(col, h, x)

    def each(self, phase, body):
        units = (FAMILY, BOTH, 1)[phase]
        if units == 1:
            body(0)
        else:
            lax.fori_loop(0, units, lambda u, _: body(u), None)

    def start(self, phase, col, d, slot, rel, h):
        copy = self.hop(phase, col, d, slot, self.source(phase, col, rel, h), self.inbox(phase, col, d, slot))
        copy.start()
        self.sent.append(copy)

    def arrived(self, phase, col, d, slot):
        box = self.inbox(phase, col, d, slot)
        self.hop(phase, col, d, slot, box, box).wait_recv()

    def ready(self, phase, col, rel):
        if phase == 0:
            for wait in self.swaps[col, rel]:
                wait()

    def far(self, phase):
        for col in range(COLOURS):
            self.ready(phase, col, BOTH)
            for d in range(BOTH):
                self.each(phase, lambda u: self.store(phase, col, BOTH, d, u, self.term(phase, col, BOTH, d, u)))
                self.start(phase, col, d, 0, BOTH, d)

    def straight(self, phase):
        for col in range(COLOURS):
            for d, rel in AHEAD:
                self.ready(phase, col, rel)
                self.each(phase, lambda u: self.store(phase, col, rel, 1 - d, u, self.term(phase, col, rel, 1 - d, u)))
                self.start(phase, col, d, 1, rel, 1 - d)

    def through(self, phase):
        for col in range(COLOURS):
            for d, rel in AHEAD:
                self.arrived(phase, col, d, 0)
                self.each(phase, lambda u: self.store(phase, col, rel, d, u, self.term(phase, col, rel, d, u) + self.value(phase, col, d, 0, u)))
                self.start(phase, col, d, BOTH, rel, d)

    def close(self, phase):
        for col in range(COLOURS):
            self.ready(phase, col, 0)
            for d in range(BOTH):
                for slot in (1, BOTH):
                    self.arrived(phase, col, d, slot)
            for h in range(BOTH):
                self.each(phase, lambda u: self.final(phase, col, h, u, self.term(phase, col, 0, h, u) + self.value(phase, col, 0, BOTH - h, u)
                                                      + self.value(phase, col, 1, 1 + h, u)))


def _comm(g_ref, *rest):
    w_refs, rest = rest[:MATRICES], rest[MATRICES:]
    m_refs, v_refs, rest = rest[:MATRICES], rest[MATRICES:14], rest[14:]
    dh_ref, a_ref, q_ref, k_ref, v_ref, ot_ref, lse_ref, angle_ref, wo_ref, out_ref, gq_ref, *rest = rest
    wn_refs, rest = rest[:MATRICES], rest[MATRICES:]
    boxes, rest = (rest[:MATRICES], rest[MATRICES:14]), rest[14:]
    (s_ref, r0_ref, mine_ref, r1_ref, ga_ref, gb_ref, gf_ref, wt_ref, ow_ref, ou_ref, wb_ref, wv_ref, ps_ref, px_ref, py_ref, p8_ref,
     dqkv_s, dqt_s, dk_s, dv_s, do_s, ring_send, ring_recv, d2d_send, d2d_recv, load_sem, w_sem, ps_send, ps_recv, zs_send, zs_recv,
     zd_send, zd_recv, od_send, od_recv, ol_sem) = rest
    me = lax.axis_index("dp")
    core = lax.rem(me, BOTH)
    at = [lax.rem(lax.div(me, 32), RING), lax.rem(lax.div(me, FAMILY), RING), lax.rem(lax.div(me, BOTH), RING)]
    group = lax.div(me, FAMILY)
    mine = lax.rem(me, FAMILY)

    def device(axis, by):
        return me + (lax.rem(at[axis] + by, RING) - at[axis]) * (32, FAMILY, BOTH)[axis]

    partner = me + 1 - BOTH * core
    family = [group * FAMILY + lax.rem(mine + k, FAMILY) for k in range(1, FAMILY)]
    friends = [device(axis, by) for axis in (0, 1) for by in (1, BOTH, COLOURS)] + family
    barrier = pltpu.get_barrier_semaphore()
    for one in friends:
        pl.semaphore_signal(barrier, inc=1, device_id={"dp": one}, device_id_type=MESH)

    def remote(src, dst, send, recv, to):
        return pltpu.make_async_remote_copy(src_ref=src, dst_ref=dst, send_sem=send, recv_sem=recv, device_id={"dp": to}, device_id_type=MESH)

    def hop(base):
        def make(phase, col, d, slot, src, dst):
            n = (((base * COLOURS + phase) * COLOURS + col) * BOTH + d) * COLOURS + slot
            return remote(src, dst, ring_send.at[n], ring_recv.at[n], device(ORDER[col][phase], 1 if d == 0 else COLOURS))

        return make

    chunks = [(n, col, rel, _where(ORDER[col][0], _near(at[ORDER[col][0]] + rel))) for n, (rel, col) in enumerate((r, c) for r in WAY for c in range(COLOURS))]
    loads, swaps = {}, []
    for n, col, rel, here in chunks:
        loads[n] = pltpu.make_async_copy(g_ref.at[(*here, core, col)], s_ref.at[(*here, col)], load_sem.at[n])
        loads[n].start()
    for k in range(MATRICES):
        pltpu.make_async_copy(w_refs[k].at[group], wn_refs[k], w_sem.at[k]).start()
    pl.semaphore_wait(barrier, len(friends))
    first = {}
    for n, col, rel, here in chunks:
        copy = remote(g_ref.at[(*here, 1 - core, col)], r0_ref.at[(*here, col)], d2d_send.at[n], d2d_recv.at[n], partner)
        copy.start()
        swaps.append(copy)
        first[col, rel] = (loads[n].wait, copy.wait_recv)

    pending, squares = [], []

    class Share:
        def __init__(self, number, box):
            self.number, self.box, self.cut = number, box, box.shape[1] // BOTH

        def block(self, rel):
            return self.box.at[BOTH * _near(at[BOTH] + rel) + core]

        def hop(self, d, slot, rel, h):
            n = (self.number * BOTH + d) * COLOURS + slot
            half = self.block(rel).at[pl.ds(h * self.cut, self.cut)]
            return remote(half, half, zs_send.at[n], zs_recv.at[n], device(BOTH, 1 if d == 0 else COLOURS))

        def over(self, rel, whose):
            n = self.number * RING + rel
            block = self.box.at[BOTH * _near(at[BOTH] + rel) + whose]
            return remote(block, block, zd_send.at[n], zd_recv.at[n], partner)

        def go(self, copy):
            copy.start()
            pending.append(copy)

        def start(self):
            for slot in range(BOTH):
                for d in range(BOTH):
                    self.go(self.hop(d, slot, 0, d if slot == 0 else 1 - d))
            self.go(self.over(0, core))

        def forward(self):
            for d, rel in BEHIND:
                self.hop(d, 0, rel, d).wait_recv()
                self.go(self.hop(d, BOTH, rel, d))

        def cross(self):
            for d, rel in BEHIND:
                self.hop(d, 1, rel, 1 - d).wait_recv()
                self.go(self.over(rel, core))
            for d in range(BOTH):
                self.hop(d, BOTH, BOTH, d).wait_recv()
            self.go(self.over(BOTH, core))

        def finish(self):
            for rel in range(RING):
                self.over(rel, 1 - core).wait_recv()

    gated_share, other_share, new_share = Share(0, ga_ref), Share(1, gb_ref), Share(BOTH, wb_ref)

    def final(box, unit):
        def put(col, h, x):
            x = x.astype(bf16)
            row = col * unit + h * (unit // BOTH)
            box[mine, row : row + unit // BOTH, :] = x
            x = x.astype(f32)
            squares.append(jnp.sum((x * x).reshape(unit // GROUPS, FAMILY, LANES), axis=0))

        return put

    part = UNITS[0] * COLOURS
    gated_sum = _Sum(UNITS[0], at, hop(0), first, lambda here, col: s_ref.at[(*here, col)], r0_ref, boxes[0], final(ga_ref, UNITS[0]))

    def put(row, x):
        unit, end = UNITS[1], row + x.shape[1]
        begin = row
        while row < end:
            n, low = row // unit, row % unit
            size = min(unit - low, end - row)
            z, c, col = n // 6, n // COLOURS % BOTH, n % COLOURS
            mine_ref[:, :, z, c, col, low : low + size, :] = x[:, row - begin : row - begin + size].reshape(RING, RING, size, LANES).astype(bf16)
            row += size

    def back(i):
        _back_step(i, dh_ref, q_ref, k_ref, v_ref, ot_ref, lse_ref, angle_ref, wo_ref, dqkv_s, dqt_s, dk_s, dv_s, do_s)

    back(0)
    _back_put(put, _dot(ot_ref[...], dh_ref[...]), TABLE[COLOURS][0])
    put(OTHERS - 48, jnp.zeros((GROUPS, 48, LANES), f32))
    gated_sum.far(0)
    back(1)
    gated_sum.straight(0)
    back(BOTH)
    gated_sum.through(0)
    back(COLOURS)
    gated_sum.close(0)
    gated_sum.far(1)
    gated_sum.straight(1)
    _back_qkv(put, a_ref, angle_ref, dqkv_s, dk_s, dv_s)

    second = {}
    for n, col, rel, here in chunks:
        copy = remote(mine_ref.at[(*here, 1 - core, col)], r1_ref.at[(*here, col)], d2d_send.at[CHUNKS + n], d2d_recv.at[CHUNKS + n], partner)
        copy.start()
        swaps.append(copy)
        second[col, rel] = (copy.wait_recv,)
    gated_sum.through(1)
    other_sum = _Sum(UNITS[1], at, hop(1), second, lambda here, col: mine_ref.at[(*here[:COLOURS], core, col)], r1_ref, boxes[1], final(gb_ref, UNITS[1]))
    other_sum.far(0)
    gated_sum.close(1)
    gated_sum.far(BOTH)
    gated_sum.straight(BOTH)
    other_sum.straight(0)
    other_sum.through(0)
    gated_sum.through(BOTH)
    other_sum.close(0)
    other_sum.far(1)
    other_sum.straight(1)
    gated_sum.close(BOTH)
    gated_share.start()

    for k, (_, blocks, rows, own, begin) in enumerate(TABLE):
        pltpu.make_async_copy(w_refs[k].at[group], wn_refs[k], w_sem.at[k]).wait()
        for j in range(blocks):
            wt_ref[j % RING, :rows, :] = wn_refs[k][:, _lanes(j)].astype(f32)
            ow_ref[begin + j * own : begin + (j + 1) * own, :] = wt_ref[j % RING, pl.ds(mine * own, own), :]
    other_sum.through(1)
    gated_share.forward()
    other_sum.close(1)
    other_sum.far(BOTH)
    other_sum.straight(BOTH)
    gated_share.cross()
    other_sum.through(BOTH)
    other_sum.close(BOTH)

    size = COLOURS * UNIT
    other_share.start()

    def swap_squares(total, which, targets, box):
        n, base = len(targets), COLOURS * which
        ps_ref[which] = total
        for k, to in enumerate(targets):
            copy = remote(ps_ref.at[which], box.at[n - 1 - k], ps_send.at[base + k], ps_recv.at[base + n - 1 - k], to)
            copy.start()
            pending.append(copy)
        for k in range(n):
            remote(box.at[k], box.at[k], ps_send.at[base + k], ps_recv.at[base + k], targets[0]).wait_recv()
            total = total + box[k]
        return total

    total = sum(squares[1:], squares[0])
    total = swap_squares(total, 0, [device(0, by) for by in (1, BOTH, COLOURS)], px_ref)
    other_share.forward()
    total = swap_squares(total, 1, [device(1, by) for by in (1, BOTH, COLOURS)], py_ref)
    other_share.cross()
    gated_share.finish()
    for n in range(FAMILY):
        gf_ref[n * part : (n + 1) * part, :] = ga_ref[n].astype(f32)
    other_share.finish()
    for n in range(FAMILY):
        gf_ref[GATED + n * (size - part) : GATED + (n + 1) * (size - part), :] = gb_ref[n].astype(f32)
    total = swap_squares(total, BOTH, family, p8_ref)
    mean = jnp.sum(total) / float(sum(a * b for a, b in SHAPE.values()))
    factor = jnp.minimum(1.0, 0.5 * lax.rsqrt(jnp.full((FAMILY, LANES), mean, f32) + 1e-30))

    for k, (_, blocks, rows, own, begin) in enumerate(TABLE):
        for j in range(blocks):
            lanes = _lanes(j)
            to = slice(begin + j * own, begin + (j + 1) * own)
            g = gf_ref[pl.ds(_flat(k) + j * rows + mine * own, own), :] * factor[:1]
            w = ow_ref[to, :]
            m = 0.9 * m_refs[k][_at(k, lanes)] + 0.1 * g
            v = 0.95 * v_refs[k][_at(k, lanes)] + 0.05 * g * g
            ou_ref[to, :] = w - 0.02 * (m * lax.rsqrt(v + 1e-8) + 0.1 * w)
            gq_ref[to, :] = g

    wb_ref[mine] = ou_ref[...].astype(bf16)
    new_share.start()
    new_share.forward()
    new_share.cross()
    new_share.finish()

    def gathered(n):
        ou_ref[...] = wb_ref[n].astype(f32)
        for k, (_, blocks, rows, own, begin) in enumerate(TABLE):
            for j in range(blocks):
                gf_ref[pl.ds(_flat(k) + j * rows + n * own, own), :] = ou_ref[begin + j * own : begin + (j + 1) * own, :]

    lax.fori_loop(0, FAMILY, lambda n, _: gathered(n), None)
    here = tuple(at)

    def own_rows(low, high):
        base, n = (0, part) if low < part else (GATED - part, size - part)
        return gf_ref[pl.ds(pl.multiple_of(mine * n, FAMILY) + base + low, high - low), :].astype(bf16)

    for col in range(COLOURS):
        low, high = col * UNIT, (col + 1) * UNIT
        for a, b in ((low, min(high, part)), (max(low, part), high)):
            if a < b:
                wv_ref[(*here, col, slice(a - low, b - low))] = own_rows(a, b)

    outs = []

    def hand_on(col, rel):
        axis = ORDER[col][0]
        q = _near(at[axis] + rel)
        src, dst = wv_ref.at[(*_where(axis, q), col)], out_ref.at[(*_where(axis, q), core, col)]
        n = col * RING + rel
        copy = remote(src, dst, od_send.at[n], od_recv.at[n], partner)
        copy.start()
        local = pltpu.make_async_copy(src, dst, ol_sem.at[n])
        local.start()
        outs.append((copy, local))

    def gather_phase(phase, chunk, done):
        def start(col, d, slot, rel, h):
            copy = hop(BOTH)(phase, col, d, slot, chunk(col, rel, h), chunk(col, rel, h))
            copy.start()
            pending.append(copy)

        def arrived(col, d, slot, rel, h):
            hop(BOTH)(phase, col, d, slot, chunk(col, rel, h), chunk(col, rel, h)).wait_recv()

        for slot in range(BOTH):
            for col in range(COLOURS):
                for d in range(BOTH):
                    start(col, d, slot, 0, d if slot == 0 else 1 - d)
        for col in range(COLOURS):
            done(col, 0)
        for col in range(COLOURS):
            for d, rel in BEHIND:
                arrived(col, d, 0, rel, d)
                start(col, d, BOTH, rel, d)
        for col in range(COLOURS):
            for d, rel in BEHIND:
                arrived(col, d, 1, rel, 1 - d)
                done(col, rel)
        for col in range(COLOURS):
            for d in range(BOTH):
                arrived(col, d, BOTH, BOTH, d)
            done(col, BOTH)

    cut = UNIT // BOTH

    def last_chunk(col, rel, h):
        spot = list(at)
        spot[ORDER[col][BOTH]] = _near(at[ORDER[col][BOTH]] + rel)
        return wv_ref.at[(*spot, col, pl.ds(h * cut, cut))]

    def middle_chunk(col, rel, h):
        spot = list(at)
        spot[ORDER[col][1]] = _near(at[ORDER[col][1]] + rel)
        spot[ORDER[col][BOTH]] = _half(h)
        return wv_ref.at[(*spot, col)]

    def whole_chunk(col, rel, h):
        axis = ORDER[col][0]
        return wv_ref.at[(*_where(axis, _near(at[axis] + rel), _half(h)), col)]

    gather_phase(BOTH, last_chunk, lambda col, rel: None)
    gather_phase(1, middle_chunk, lambda col, rel: None)
    gather_phase(0, whole_chunk, hand_on)

    for copy in swaps + gated_sum.sent + other_sum.sent + pending:
        copy.wait_send()
    for copy, local in outs:
        copy.wait_send()
        local.wait()
    for n, (col, rel) in enumerate((c, r) for c in range(COLOURS) for r in range(RING)):
        axis = ORDER[col][0]
        dst = out_ref.at[(*_where(axis, _near(at[axis] + rel)), 1 - core, col)]
        remote(dst, dst, od_send.at[n], od_recv.at[n], partner).wait_recv()


def sum_step_gather(g, weights, m, v, back):
    vmem, dma = pltpu.VMEM, pltpu.SemaphoreType.DMA
    hbm, local = pl.BlockSpec(memory_space=pl.ANY), pl.BlockSpec(memory_space=vmem)
    cube, sides = (RING, RING, RING), (COLOURS, BOTH, COLOURS)
    scratch = [vmem((SHAPE[name][0] // GROUPS, SHAPE[name][1]), bf16) for name in NAMES]
    for unit in UNITS:
        row = (unit, LANES)
        scratch += [vmem((*sides, BOTH, RING, *row), bf16), vmem((COLOURS, RING, RING, *row), f32), vmem((*sides, BOTH, *row), bf16), vmem((COLOURS, COLOURS, RING, *row), bf16),
                    vmem((COLOURS, RING, *row), f32), vmem((*sides, unit // BOTH, LANES), bf16), vmem((COLOURS, COLOURS, *row), bf16)]
    own, tile, head = (OWN, LANES), (FAMILY, LANES), (TOKENS, HEAD)
    scratch += [vmem((*cube, COLOURS, UNITS[0], LANES), bf16), vmem((*cube, COLOURS, UNITS[0], LANES), bf16), vmem((*cube, BOTH, COLOURS, UNITS[1], LANES), bf16),
                vmem((*cube, COLOURS, UNITS[1], LANES), bf16), vmem((FAMILY, COLOURS * UNITS[0], LANES), bf16), vmem((FAMILY, COLOURS * UNITS[1], LANES), bf16), vmem((FLAT, LANES), f32),
                vmem((RING, 200, LANES), f32), vmem(own, f32), vmem(own, f32), vmem((FAMILY, *own), bf16), vmem((*cube, COLOURS, UNIT, LANES), bf16)]
    scratch += [vmem((n, *tile), f32) for n in (COLOURS, COLOURS, COLOURS, MATRICES)]
    scratch += [vmem((TOKENS, (HEADS + BOTH) * HEAD), bf16), vmem((HEAD, HEADS * BACK), f32), vmem(head, f32), vmem(head, f32), vmem((HEADS, BACK, HEAD), bf16)]
    scratch += [dma((n,)) for n in (162, 162, 24, 24, CHUNKS, MATRICES, 13, 13, 18, 18, CHUNKS, CHUNKS, CHUNKS, CHUNKS, CHUNKS)]
    return pl.pallas_call(
        _comm,
        out_shape=[jax.ShapeDtypeStruct((*cube, BOTH, COLOURS, UNIT, LANES), bf16), jax.ShapeDtypeStruct(own, f32)],
        in_specs=[hbm] * FAMILY + [local] * 23,
        out_specs=[hbm, local],
        scratch_shapes=scratch,
        compiler_params=pltpu.CompilerParams(collective_id=0, has_side_effects=True, vmem_limit_bytes=67043328),
    )(g, *[w.reshape(GROUPS, w.shape[1] // GROUPS, w.shape[BOTH]) for w in weights], *_rows(m), *_rows(v), *back)


PER = RING


def _finish(flat_ref, gq_ref, *rest):
    m_refs, v_refs, w_refs, mo_refs, vo_refs = (rest[i : i + MATRICES] for i in range(0, 35, MATRICES))

    @pl.when(pl.program_id(0) == 0)
    def _():
        for k, (_, blocks, _, own, first) in enumerate(TABLE):
            for j in range(blocks):
                at = _at(k, _lanes(j))
                g = gq_ref[first + j * own : first + (j + 1) * own, :]
                mo_refs[k][at] = 0.9 * m_refs[k][at] + 0.1 * g
                vo_refs[k][at] = 0.95 * v_refs[k][at] + 0.05 * g * g

    for k, (_, blocks, rows, _, _) in enumerate(TABLE):
        lengths = (COLOURS * UNITS[1], GATED) if k < RING else (COLOURS * UNITS[0], 0)
        for j in range(blocks):
            row, to = _flat(k) + j * rows - lengths[1], 0
            while to < rows:
                n, low = row // lengths[0], row % lengths[0]
                some = min(lengths[0] - low, rows - to)
                low += n * COLOURS * UNIT + (COLOURS * UNITS[0] if k < RING else 0)
                for i in range(PER):
                    w_refs[k][0, i * rows + to : i * rows + to + some, _lanes(j)] = flat_ref[i, low : low + some, :]
                row, to = row + some, to + some


def finish(flat, gq, m, v):
    whole = pl.BlockSpec(memory_space=pltpu.VMEM)
    old = [*_rows(m), *_rows(v)]
    shapes = [(1, *SHAPE[name]) for name in NAMES]
    out = pl.pallas_call(
        _finish,
        grid=(GROUPS // PER,),
        out_shape=[jax.ShapeDtypeStruct(shape, jnp.bfloat16) for shape in shapes] + [jax.ShapeDtypeStruct(a.shape, a.dtype) for a in old],
        in_specs=[pl.BlockSpec((PER, FLAT, LANES), lambda i: (i, 0, 0)), whole] + [whole] * 14,
        out_specs=[pl.BlockSpec((1, shape[1] // GROUPS * PER, shape[BOTH]), lambda i: (0, i, 0)) for shape in shapes] + [whole] * 14,
        compiler_params=pltpu.CompilerParams(vmem_limit_bytes=VMEM),
    )(flat.reshape(GROUPS, FLAT, LANES), gq, *old)
    moments = [new.reshape(1, *new.shape) if new.ndim == BOTH else new.transpose(1, 0, BOTH) for new in out[MATRICES:]]
    return (*out[:MATRICES], *moments)


def solution(mesh):
    def step(x, dy, *arrays):
        weights, m, v = (arrays[i : i + MATRICES] for i in (0, MATRICES, 14))
        w = dict(zip(NAMES, weights, strict=True))
        plain = {name: w[name][0] for name in ("wq", "wk", "wv", "wo")}
        a, q, k, value, ot, lse, h = attend(x[0], plain)
        g, dh = gated(h, dy[0], w)
        back = (dh, a, q, k, value, ot, lse, _angles(), plain["wo"])
        flat, gq = sum_step_gather(g.reshape(RING, RING, RING, 2, COLOURS, UNITS[0], LANES), weights, m, v, back)
        return finish(flat, gq, m, v)

    states, all_of, cut = P(("rep", "dp")), P(), P(None, "dp")
    return jax.shard_map(
        step,
        mesh=mesh,
        in_specs=(states, states) + (all_of,) * MATRICES + (cut,) * 14,
        out_specs=(P("rep"),) * MATRICES + (P("rep", "dp"),) * 14,
        check_vma=False,
    )
```

```python
import functools

import jax
import jax.numpy as jnp
import numpy as np
from jax import lax
from jax.experimental import pallas as pl
from jax.experimental.pallas import tpu as pltpu
from jax.sharding import PartitionSpec as P

NEG = -1e30
HIDDEN = 2 * NEG
LOG2E = 1.4426950408889634
VMEM = 56 * 2**20
NAMES = ("wq", "wk", "wv", "wo", "w_gate", "w_up", "w_down")
TOKENS, D, HEADS, HEAD, FF = 1024, 640, 8, 128, 3200
SCALE = HEAD**-0.5
E = SCALE * LOG2E
THETA = 10000
f32, bf16 = jnp.float32, jnp.bfloat16


def _dot(a, b, ca=1, cb=0):
    return lax.dot_general(a, b, (((ca,), (cb,)), ((), ())), preferred_element_type=f32)


def _dot_t(a, b):
    return _dot(a, b, 1, 1)


def _lanes(k):
    return slice(k * 128, (k + 1) * 128)


def _scale(wide):
    return lax.rsqrt(jnp.mean(wide * wide, -1, keepdims=True) + 1e-6)


def _normed(wide):
    return wide * _scale(wide)


HALF = HEAD // 2


def _angles():
    angle = np.arange(TOKENS, dtype=np.float32)[:, None] * np.float32(THETA) ** (-np.arange(HALF, dtype=np.float32) / np.float32(HALF))
    return np.concatenate([np.cos(angle), np.sin(angle)], 1).astype(np.float32)


def _spread(angles):
    other = pltpu.roll(angles, HALF, 1)
    low = lax.broadcasted_iota(jnp.int32, angles.shape, 1) < HALF
    return jnp.where(low, angles, other), jnp.where(low, -other, angles)
LANES, GROUPS = 128, 16
BOTH, COLOURS, RING, FAMILY, MATRICES, CHUNKS = 2, 3, 4, 8, 7, 12


BQ, BK = 512, 256


def _attend(x_ref, angle_ref, wq_ref, wk_ref, wv_ref, wo_ref, a_ref, q_ref, k_ref, v_ref, ot_ref, lse_ref, h_ref, ks, vts, top_s, mix_s):
    i = pl.program_id(0)
    a = _normed(x_ref[...].astype(f32)).astype(bf16)
    a_ref[...] = a
    cos, sin = _spread(angle_ref[...])

    def turned(t):
        t = t.astype(bf16).astype(f32)
        return (t * cos + pltpu.roll(t, HALF, 1) * sin).astype(bf16)

    k = turned(_dot(a, wk_ref[...]))
    v = _dot(a, wv_ref[...]).astype(bf16)
    k_ref[...] = k
    v_ref[...] = v
    here = pl.ds(pl.multiple_of(i * BQ, BQ), BQ)
    ks[here, :] = k
    vts[:HEAD, here] = v.T
    vts[HEAD:, here] = jnp.ones((8, BQ), bf16)
    q = _dot(a, wq_ref[...])
    for n in range(HEADS):
        q_ref[n] = turned(q[:, _lanes(n)])
    top_s[...] = jnp.full(top_s.shape, NEG, f32)
    mix_s[...] = jnp.zeros(mix_s.shape, f32)

    def block(j, low, masked):
        keys = pl.ds(pl.multiple_of(j * BK, BK), BK)
        scores = [_dot_t(ks[keys, :], q_ref[n, low:, :]) for n in range(HEADS)]
        if masked:
            hidden = lax.broadcasted_iota(jnp.int32, (BK, BQ - low), 1) < lax.broadcasted_iota(jnp.int32, (BK, BQ - low), 0)
        values = vts[:, keys]
        weights, keeps = [], []
        for n, s in enumerate(scores):
            if masked:
                s = jnp.where(hidden, HIDDEN, s)
            old = top_s[n : n + 1, low:]
            top = jnp.maximum(old, s.max(axis=0, keepdims=True))
            top_s[n : n + 1, low:] = top
            weights.append(jnp.exp2((s - top) * E).astype(bf16))
            keeps.append(jnp.exp2((old - top) * E))
        for n, (p, keep) in enumerate(zip(weights, keeps)):
            mix_s[n, :, low:] = mix_s[n, :, low:] * keep + _dot(values, p)

    per = BQ // BK
    lax.fori_loop(0, per * i, lambda j, _: block(j, 0, False), None)
    for n in range(per):
        block(per * i + n, n * BK, True)
    outs = []
    for n in range(HEADS):
        total = mix_s[n, HEAD : HEAD + 1, :]
        out = (mix_s[n, :HEAD, :] * (1 / total)).astype(bf16)
        ot_ref[_lanes(n), :] = out
        outs.append(out.T)
        lse_ref[n : n + 1, :] = top_s[n : n + 1, :] * SCALE + jnp.log(total)
    more = _dot(jnp.concatenate(outs, axis=1), wo_ref[...]).astype(bf16)
    h_ref[...] = (x_ref[...].astype(f32) + more.astype(f32)).astype(bf16)


def attend(x, w):
    whole = pl.BlockSpec(memory_space=pltpu.VMEM)
    rows = lambda width: pl.BlockSpec((BQ, width), lambda i: (i, 0))
    columns = lambda height: pl.BlockSpec((height, BQ), lambda i: (0, i))
    shape = jax.ShapeDtypeStruct
    return pl.pallas_call(
        _attend,
        grid=(TOKENS // BQ,),
        in_specs=[rows(D), rows(HEAD)] + [whole] * 4,
        out_specs=[rows(D), pl.BlockSpec((HEADS, BQ, HEAD), lambda i: (0, i, 0)), rows(HEAD), rows(HEAD), columns(HEADS * HEAD), columns(HEADS), rows(D)],
        out_shape=[shape((TOKENS, D), bf16), shape((HEADS, TOKENS, HEAD), bf16), shape((TOKENS, HEAD), bf16), shape((TOKENS, HEAD), bf16),
                   shape((HEADS * HEAD, TOKENS), bf16), shape((HEADS, TOKENS), f32), shape((TOKENS, D), bf16)],
        scratch_shapes=[pltpu.VMEM((TOKENS, HEAD), bf16), pltpu.VMEM((HEAD + 8, TOKENS), bf16), pltpu.VMEM((HEADS, BQ), f32),
                        pltpu.VMEM((HEADS, HEAD + 8, BQ), f32)],
        compiler_params=pltpu.CompilerParams(dimension_semantics=("arbitrary",), vmem_limit_bytes=VMEM),
    )(x, _angles(), *[w[name] for name in ("wq", "wk", "wv", "wo")])


BF = 256
LAST = FF // BF
CHUNK = 512


def _gated(h_ref, dy_ref, wg_ref, wu_ref, wd_ref, g_ref, dh_ref, b_s, bt_s, dyt_s, acc_s, hid_s, dg_s, du_s, stage, down_s, zero_s, sem, end_sem):
    j = pl.program_id(0)
    slot = lax.rem(j, 2)
    firsts = [TABLE[NAMES.index(name)][0] for name in ("w_gate", "w_up", "w_down")]
    rows = D // GROUPS
    ends = 3 * FF * D // GROUPS // LANES

    def put(n, at, size):
        where = pl.ds(pl.multiple_of(firsts[n] + at * (rows * BF // LANES), 8), size)
        return pltpu.make_async_copy(stage.at[n, slot, :, pl.ds(0, size)], g_ref.at[:, where], sem.at[n, slot])

    @pl.when(j == 0)
    def _():
        b = _normed(h_ref[...].astype(f32)).astype(bf16)
        b_s[...] = b
        bt_s[...] = b.T
        dyt_s[...] = dy_ref[...].T
        acc_s[...] = jnp.zeros(acc_s.shape, f32)
        zero_s[...] = jnp.zeros(zero_s.shape, bf16)
        pltpu.make_async_copy(zero_s, g_ref.at[:, pl.ds(ends, GATED - ends)], end_sem.at[0]).start()

    left = FF - j * BF
    inside = lax.broadcasted_iota(jnp.int32, (D, BF), 1) < left
    wg, wu = (jnp.where(inside, ref[0], jnp.zeros((), bf16)) for ref in (wg_ref, wu_ref))
    wd = jnp.where(lax.broadcasted_iota(jnp.int32, (BF, D), 0) < left, wd_ref[0], jnp.zeros((), bf16))
    for at in range(0, TOKENS, CHUNK):
        here = slice(at, at + CHUNK)
        gate, up = _dot(b_s[here, :], wg), _dot(b_s[here, :], wu)
        dhid = _dot_t(dy_ref[here, :], wd).astype(bf16).astype(f32)
        share = 1 / (1 + jnp.exp(-gate))
        silu = gate * share
        hid_s[here, :] = (silu * up).astype(bf16)
        dgate = (dhid * up * (share * (1 + gate * (1 - share)))).astype(bf16)
        dup = (dhid * silu).astype(bf16)
        dg_s[here, :] = dgate
        du_s[here, :] = dup
        acc_s[:, here] += _dot_t(wg, dgate) + _dot_t(wu, dup)

    @pl.when(j >= 2)
    def _():
        for n in range(2):
            put(n, j - 2, rows * BF // LANES).wait()

    for n, one in enumerate((dg_s, du_s)):
        term = _dot(bt_s[...], one[...])
        for k in range(BF // LANES):
            stage[n, slot, :, k * rows : (k + 1) * rows, :] = term[:, _lanes(k)].reshape(GROUPS, rows, LANES).astype(bf16)
    term = _dot(dyt_s[...], hid_s[...]).T
    for k in range(D // LANES):
        down_s[k, pl.ds(pl.multiple_of(j * BF, BF), BF), :] = term[:, _lanes(k)].astype(bf16)

    @pl.when(j < LAST)
    def _():
        for n in range(2):
            put(n, j, rows * BF // LANES).start()

    @pl.when(j == LAST)
    def _():
        for n in range(2):
            put(n, j, rows * (FF % BF) // LANES).start()
        per = FF // GROUPS
        for k in range(D // LANES):
            for n in range(GROUPS):
                pltpu.make_async_copy(down_s.at[k, pl.ds(n * per, per)], g_ref.at[n, pl.ds(firsts[2] + k * per, per)], end_sem.at[1]).start()
        for at in range(0, TOKENS, CHUNK):
            here = slice(at, at + CHUNK)
            db = acc_s[:, here].T.astype(bf16).astype(f32)
            h = h_ref[here, :].astype(f32)
            s = _scale(h)
            through = db * s - h * (s * s * s * jnp.mean(db * h, -1, keepdims=True))
            dh_ref[here, :] = (dy_ref[here, :].astype(f32) + through.astype(bf16).astype(f32)).astype(bf16)
        for n in range(2):
            put(n, j, rows * (FF % BF) // LANES).wait()
            pltpu.make_async_copy(stage.at[n, 1 - slot], stage.at[n, 1 - slot], sem.at[n, 1 - slot]).wait()
        pltpu.make_async_copy(zero_s, g_ref.at[:, pl.ds(ends, GATED - ends)], end_sem.at[0]).wait()
        whole = g_ref.at[:, pl.ds(firsts[2], ends - firsts[2])]
        pltpu.make_async_copy(whole, whole, end_sem.at[1]).wait()


def gated(h, dy, w):
    vmem = pltpu.VMEM
    whole = pl.BlockSpec(memory_space=vmem)
    across = pl.BlockSpec((1, D, BF), lambda j: (0, 0, j))
    pad = GATED - 3 * FF * D // GROUPS // LANES
    return pl.pallas_call(
        _gated,
        grid=(LAST + 1,),
        in_specs=[whole, whole, across, across, pl.BlockSpec((1, BF, D), lambda j: (0, j, 0))],
        out_specs=[pl.BlockSpec(memory_space=pl.ANY), whole],
        out_shape=[jax.ShapeDtypeStruct((GROUPS, GATED, LANES), bf16), jax.ShapeDtypeStruct((TOKENS, D), bf16)],
        scratch_shapes=[vmem((TOKENS, D), bf16), vmem((D, TOKENS), bf16), vmem((D, TOKENS), bf16), vmem((D, TOKENS), f32),
                        vmem((TOKENS, BF), bf16), vmem((TOKENS, BF), bf16), vmem((TOKENS, BF), bf16),
                        vmem((2, 2, GROUPS, D // GROUPS * BF // LANES, LANES), bf16), vmem((D // LANES, (LAST + 1) * BF, LANES), bf16), vmem((GROUPS, pad, LANES), bf16),
                        pltpu.SemaphoreType.DMA((2, 2)), pltpu.SemaphoreType.DMA((2,))],
        compiler_params=pltpu.CompilerParams(dimension_semantics=("arbitrary",), vmem_limit_bytes=VMEM),
    )(h, dy, *[w[name] for name in ("w_gate", "w_up", "w_down")])


BACK = 256


def _back_step(i, dh_ref, q_ref, k_ref, v_ref, ot_ref, lse_ref, angle_ref, wo_ref, dqkv_s, dqt_s, dk_s, dv_s, do_s):
    here = slice(i * BACK, (i + 1) * BACK)
    if i == 0:
        dk_s[...] = jnp.zeros(dk_s.shape, f32)
        dv_s[...] = jnp.zeros(dv_s.shape, f32)
    dqt_s[...] = jnp.zeros(dqt_s.shape, f32)
    dh, wo = dh_ref[here, :], wo_ref[...]
    dot = _dot_t(wo, dh).astype(bf16).astype(f32) * ot_ref[:, here].astype(f32)
    delta = [dot[_lanes(n), :].sum(axis=0, keepdims=True) for n in range(HEADS)]
    dout = _dot_t(dh, wo).astype(bf16)
    for n in range(HEADS):
        do_s[n] = dout[:, _lanes(n)]
    pairs = range(0, HEADS, 2)
    beside = lambda rows, n: jnp.concatenate([rows[n], rows[n + 1]], axis=1)
    lses = [lse_ref[n : n + 1, here] * LOG2E for n in range(HEADS)]

    def block(j, masked):
        keys = pl.ds(j * BACK if masked else pl.multiple_of(j * BACK, BACK), BACK)
        k, v = k_ref[keys, :], v_ref[keys, :]
        kt = k.T
        if masked:
            place = lax.broadcasted_iota(jnp.int32, (BACK, 2 * BACK), 1)
            hidden = jnp.where(place < BACK, place, place - BACK) < lax.broadcasted_iota(jnp.int32, (BACK, 2 * BACK), 0)
        for some in (pairs[:2], pairs[2:]):
            qs = [q_ref[n : n + 2, here, :].reshape(2 * BACK, HEAD) for n in some]
            dos = [do_s[n : n + 2].reshape(2 * BACK, HEAD) for n in some]
            scores = [_dot_t(k, q) for q in qs]
            dps = [_dot_t(v, one) for one in dos]
            for n, q, do, score, dp in zip(some, qs, dos, scores, dps):
                p = jnp.exp2(score * E - beside(lses, n))
                if masked:
                    p = jnp.where(hidden, 0.0, p)
                ds = (p * (dp - beside(delta, n))).astype(bf16)
                dv_s[keys, :] += _dot(p.astype(bf16), do)
                dk_s[keys, :] += _dot(ds, q)
                dqt_s[:, n * BACK : (n + 2) * BACK] += _dot(kt, ds)

    lax.fori_loop(0, i, lambda j, _: block(j, False), None)
    block(i, True)
    both = angle_ref[here, :].T
    cost, sint = both[:HALF], both[HALF:]
    for n in range(HEADS):
        t = (dqt_s[:, n * BACK : (n + 1) * BACK] * SCALE).astype(bf16).astype(f32)
        one, two = t[:HALF], t[HALF:]
        t = jnp.concatenate([one * cost + two * sint, two * cost - one * sint], axis=0)
        dqkv_s[here, _lanes(n)] = t.astype(bf16).T


def _back_put(put, term, first):
    rows = term.shape[0] // GROUPS
    for k in range(term.shape[1] // LANES):
        put(first + k * rows, term[:, _lanes(k)].reshape(GROUPS, rows, LANES))


def _back_qkv(put, a_ref, angle_ref, dqkv_s, dk_s, dv_s):
    wide = HEADS * HEAD
    cos, sin = _spread(angle_ref[...])
    t = (dk_s[...] * SCALE).astype(bf16).astype(f32)
    dqkv_s[:, wide : wide + HEAD] = (t * cos - pltpu.roll(t, HALF, 1) * sin).astype(bf16)
    dqkv_s[:, wide + HEAD :] = dv_s[...].astype(bf16)
    _back_put(put, _dot(a_ref[...].T, dqkv_s[...]), TABLE[0][0])


MESH, ALL = pl.DeviceIdType.MESH, slice(None)
SHAPE = {"wq": (640, 1024), "wk": (640, 128), "wv": (640, 128), "wo": (1024, 640), "w_gate": (640, 3200), "w_up": (640, 3200), "w_down": (3200, 640)}
UNIT = 160
UNITS = (LANES, 32)
GATED, OTHERS = 24 * UNITS[0], 24 * UNITS[1]
FLAT = GATED + OTHERS
ORDER = ((0, 1, 2), (1, 2, 0), (2, 0, 1))
AHEAD, BEHIND = ((0, 1), (1, COLOURS)), ((0, COLOURS), (1, 1))
WAY = (2, 1, COLOURS, 0)


def _table():
    table, flat, mine = [], 0, 0
    for name in NAMES:
        rows, cols = SHAPE[name]
        flat = 0 if name == "w_gate" else flat
        blocks, group, own = cols // LANES, rows // GROUPS, rows // LANES
        table.append((flat, blocks, group, own, mine))
        flat += blocks * group
        mine += blocks * own
    return tuple(table)


TABLE, OWN = _table(), COLOURS * UNIT


def _flat(k):
    return TABLE[k][0] + (GATED if k < RING else 0)


def _at(k, lanes):
    return (ALL, lanes) if TABLE[k][COLOURS] % FAMILY == 0 else (ALL, 0, lanes)


def _rows(moments):
    return [one[0] if one.shape[1] % FAMILY == 0 else one.transpose(1, 0, BOTH) for one in moments]


def _near(q):
    return lax.rem(q, RING)


def _where(axis, q, first=ALL):
    return ((q, first, ALL), (first, q, ALL), (first, ALL, q))[axis]


def _place(axis, q, a, b):
    return ((q, a, b), (a, q, b), (a, b, q))[axis]


def _half(h):
    return pl.ds(BOTH * h, BOTH)


class _Sum:
    def __init__(self, unit, at, hop, swaps, own, other, boxes, final):
        self.unit, self.at, self.hop, self.swaps, self.own, self.other, self.last = unit, at, hop, swaps, own, other, final
        self.ra, self.f, self.rb, self.sb, self.f2, self.rc, self.sc = boxes
        self.sent, self.cut = [], unit // BOTH

    def spot(self, col, rel, h, u):
        axis = ORDER[col][0]
        return _place(axis, _near(self.at[axis] + rel), BOTH * h + lax.div(u, RING), lax.rem(u, RING))

    def chunk(self, phase, col, rel):
        return _near(self.at[ORDER[col][phase]] + rel)

    def rows(self, h):
        return slice(h * self.cut, (h + 1) * self.cut)

    def term(self, phase, col, rel, h, u):
        if phase == 0:
            here = self.spot(col, rel, h, u)
            return self.own(here, col)[...].astype(f32) + self.other[(*here, col)].astype(f32)
        if phase == 1:
            return self.f[col, self.chunk(1, col, rel), BOTH * h + u]
        return self.f2[col, self.chunk(BOTH, col, rel), self.rows(h)]

    def source(self, phase, col, rel, h):
        if phase == 0:
            axis = ORDER[col][0]
            return self.own(_where(axis, self.chunk(0, col, rel), _half(h)), col)
        return self.sb.at[col, rel - 1, _half(h)] if phase == 1 else self.sc.at[col, rel - 1, self.rows(h)]

    def store(self, phase, col, rel, h, u, x):
        x = x.astype(bf16)
        if phase == 0:
            self.own(self.spot(col, rel, h, u), col)[...] = x
        elif phase == 1:
            self.sb[col, rel - 1, BOTH * h + u] = x
        else:
            self.sc[col, rel - 1, self.rows(h)] = x

    def inbox(self, phase, col, d, slot):
        return (self.ra, self.rb, self.rc)[phase].at[col, d, slot]

    def value(self, phase, col, d, slot, u):
        box = self.inbox(phase, col, d, slot)
        box = (box.at[lax.div(u, RING), lax.rem(u, RING)] if phase == 0 else box.at[u] if phase == 1 else box)
        return box[...].astype(f32)

    def final(self, phase, col, h, u, x):
        if phase == 0:
            a, b = BOTH * h + lax.div(u, RING), lax.rem(u, RING)
            self.f[(col, b, a) if col == 1 else (col, a, b)] = x
        elif phase == 1:
            self.f2[col, BOTH * h + u] = x
        else:
            self.last(col, h, x)

    def each(self, phase, body):
        units = (FAMILY, BOTH, 1)[phase]
        if units == 1:
            body(0)
        else:
            lax.fori_loop(0, units, lambda u, _: body(u), None)

    def start(self, phase, col, d, slot, rel, h):
        copy = self.hop(phase, col, d, slot, self.source(phase, col, rel, h), self.inbox(phase, col, d, slot))
        copy.start()
        self.sent.append(copy)

    def arrived(self, phase, col, d, slot):
        box = self.inbox(phase, col, d, slot)
        self.hop(phase, col, d, slot, box, box).wait_recv()

    def ready(self, phase, col, rel):
        if phase == 0:
            for wait in self.swaps[col, rel]:
                wait()

    def far(self, phase):
        for col in range(COLOURS):
            self.ready(phase, col, BOTH)
            for d in range(BOTH):
                self.each(phase, lambda u: self.store(phase, col, BOTH, d, u, self.term(phase, col, BOTH, d, u)))
                self.start(phase, col, d, 0, BOTH, d)

    def straight(self, phase):
        for col in range(COLOURS):
            for d, rel in AHEAD:
                self.ready(phase, col, rel)
                self.each(phase, lambda u: self.store(phase, col, rel, 1 - d, u, self.term(phase, col, rel, 1 - d, u)))
                self.start(phase, col, d, 1, rel, 1 - d)

    def through(self, phase):
        for col in range(COLOURS):
            for d, rel in AHEAD:
                self.arrived(phase, col, d, 0)
                self.each(phase, lambda u: self.store(phase, col, rel, d, u, self.term(phase, col, rel, d, u) + self.value(phase, col, d, 0, u)))
                self.start(phase, col, d, BOTH, rel, d)

    def close(self, phase):
        for col in range(COLOURS):
            self.ready(phase, col, 0)
            for d in range(BOTH):
                for slot in (1, BOTH):
                    self.arrived(phase, col, d, slot)
            for h in range(BOTH):
                self.each(phase, lambda u: self.final(phase, col, h, u, self.term(phase, col, 0, h, u) + self.value(phase, col, 0, BOTH - h, u)
                                                      + self.value(phase, col, 1, 1 + h, u)))


def _comm(g_ref, *rest):
    w_refs, rest = rest[:MATRICES], rest[MATRICES:]
    given, (out_ref, gq_ref, *rest) = rest[:23], rest[23:]
    held, rest = rest[:23], rest[23:]
    m_refs, v_refs = held[:MATRICES], held[MATRICES:14]
    dh_ref, a_ref, q_ref, k_ref, v_ref, ot_ref, lse_ref, angle_ref, wo_ref = held[14:]
    wn_refs, rest = rest[:MATRICES], rest[MATRICES:]
    boxes, rest = (rest[:MATRICES], rest[MATRICES:14]), rest[14:]
    (s_ref, r0_ref, mine_ref, r1_ref, ga_ref, gb_ref, gf_ref, wt_ref, ow_ref, ou_ref, wb_ref, wv_ref, ps_ref, px_ref, py_ref, p8_ref,
     dqkv_s, dqt_s, dk_s, dv_s, do_s, ring_send, ring_recv, d2d_send, d2d_recv, load_sem, fetch_sem, w_sem, ps_send, ps_recv, zs_send, zs_recv,
     zd_send, zd_recv, od_send, od_recv, ol_sem) = rest
    me = lax.axis_index("dp")
    core = lax.rem(me, BOTH)
    at = [lax.rem(lax.div(me, 32), RING), lax.rem(lax.div(me, FAMILY), RING), lax.rem(lax.div(me, BOTH), RING)]
    group = lax.div(me, FAMILY)
    mine = lax.rem(me, FAMILY)

    def device(axis, by):
        return me + (lax.rem(at[axis] + by, RING) - at[axis]) * (32, FAMILY, BOTH)[axis]

    partner = me + 1 - BOTH * core
    family = [group * FAMILY + lax.rem(mine + k, FAMILY) for k in range(1, FAMILY)]
    friends = [device(axis, by) for axis in (0, 1) for by in (1, BOTH, COLOURS)] + family
    barrier = pltpu.get_barrier_semaphore()
    for one in friends:
        pl.semaphore_signal(barrier, inc=1, device_id={"dp": one}, device_id_type=MESH)

    def remote(src, dst, send, recv, to):
        return pltpu.make_async_remote_copy(src_ref=src, dst_ref=dst, send_sem=send, recv_sem=recv, device_id={"dp": to}, device_id_type=MESH)

    def hop(base):
        def make(phase, col, d, slot, src, dst):
            n = (((base * COLOURS + phase) * COLOURS + col) * BOTH + d) * COLOURS + slot
            return remote(src, dst, ring_send.at[n], ring_recv.at[n], device(ORDER[col][phase], 1 if d == 0 else COLOURS))

        return make

    chunks = [(n, col, rel, _where(ORDER[col][0], _near(at[ORDER[col][0]] + rel))) for n, (rel, col) in enumerate((r, c) for r in WAY for c in range(COLOURS))]
    loads, swaps = {}, []
    fetched = [pltpu.make_async_copy(src, dst, fetch_sem.at[n]) for n, (src, dst) in enumerate(zip(given, held))]
    for copy in fetched[14:]:
        copy.start()
    for n, col, rel, here in chunks:
        loads[n] = pltpu.make_async_copy(g_ref.at[(*here, core, col)], s_ref.at[(*here, col)], load_sem.at[n])
        loads[n].start()
    pl.semaphore_wait(barrier, len(friends))
    first = {}
    for n, col, rel, here in chunks:
        copy = remote(g_ref.at[(*here, 1 - core, col)], r0_ref.at[(*here, col)], d2d_send.at[n], d2d_recv.at[n], partner)
        copy.start()
        swaps.append(copy)
        first[col, rel] = (loads[n].wait, copy.wait_recv)
    for k in range(MATRICES):
        pltpu.make_async_copy(w_refs[k].at[group], wn_refs[k], w_sem.at[k]).start()
    for copy in fetched[:14]:
        copy.start()

    pending, squares = [], []

    class Share:
        def __init__(self, number, box):
            self.number, self.box, self.cut = number, box, box.shape[1] // BOTH

        def block(self, rel):
            return self.box.at[BOTH * _near(at[BOTH] + rel) + core]

        def hop(self, d, slot, rel, h):
            n = (self.number * BOTH + d) * COLOURS + slot
            half = self.block(rel).at[pl.ds(h * self.cut, self.cut)]
            return remote(half, half, zs_send.at[n], zs_recv.at[n], device(BOTH, 1 if d == 0 else COLOURS))

        def over(self, rel, whose):
            n = self.number * RING + rel
            block = self.box.at[BOTH * _near(at[BOTH] + rel) + whose]
            return remote(block, block, zd_send.at[n], zd_recv.at[n], partner)

        def go(self, copy):
            copy.start()
            pending.append(copy)

        def start(self):
            for slot in range(BOTH):
                for d in range(BOTH):
                    self.go(self.hop(d, slot, 0, d if slot == 0 else 1 - d))
            self.go(self.over(0, core))

        def forward(self):
            for d, rel in BEHIND:
                self.hop(d, 0, rel, d).wait_recv()
                self.go(self.hop(d, BOTH, rel, d))

        def cross(self):
            for d, rel in BEHIND:
                self.hop(d, 1, rel, 1 - d).wait_recv()
                self.go(self.over(rel, core))
            for d in range(BOTH):
                self.hop(d, BOTH, BOTH, d).wait_recv()
            self.go(self.over(BOTH, core))

        def finish(self):
            for rel in range(RING):
                self.over(rel, 1 - core).wait_recv()

    gated_share, other_share, new_share = Share(0, ga_ref), Share(1, gb_ref), Share(BOTH, wb_ref)

    def final(box, unit):
        def put(col, h, x):
            x = x.astype(bf16)
            row = col * unit + h * (unit // BOTH)
            box[mine, row : row + unit // BOTH, :] = x
            x = x.astype(f32)
            squares.append(jnp.sum((x * x).reshape(unit // GROUPS, FAMILY, LANES), axis=0))

        return put

    part = UNITS[0] * COLOURS
    gated_sum = _Sum(UNITS[0], at, hop(0), first, lambda here, col: s_ref.at[(*here, col)], r0_ref, boxes[0], final(ga_ref, UNITS[0]))

    def put(row, x):
        unit, end = UNITS[1], row + x.shape[1]
        begin = row
        while row < end:
            n, low = row // unit, row % unit
            size = min(unit - low, end - row)
            z, c, col = n // 6, n // COLOURS % BOTH, n % COLOURS
            mine_ref[:, :, z, c, col, low : low + size, :] = x[:, row - begin : row - begin + size].reshape(RING, RING, size, LANES).astype(bf16)
            row += size

    def back(i):
        _back_step(i, dh_ref, q_ref, k_ref, v_ref, ot_ref, lse_ref, angle_ref, wo_ref, dqkv_s, dqt_s, dk_s, dv_s, do_s)

    for copy in fetched[14:]:
        copy.wait()
    back(0)
    gated_sum.far(0)
    _back_put(put, _dot(ot_ref[...], dh_ref[...]), TABLE[COLOURS][0])
    put(OTHERS - 48, jnp.zeros((GROUPS, 48, LANES), f32))
    gated_sum.straight(0)
    back(1)
    gated_sum.through(0)
    back(BOTH)
    gated_sum.close(0)
    gated_sum.far(1)
    gated_sum.straight(1)
    back(COLOURS)
    gated_sum.through(1)
    gated_sum.close(1)
    gated_sum.far(BOTH)
    gated_sum.straight(BOTH)
    _back_qkv(put, a_ref, angle_ref, dqkv_s, dk_s, dv_s)

    second = {}
    for n, col, rel, here in chunks:
        copy = remote(mine_ref.at[(*here, 1 - core, col)], r1_ref.at[(*here, col)], d2d_send.at[CHUNKS + n], d2d_recv.at[CHUNKS + n], partner)
        copy.start()
        swaps.append(copy)
        second[col, rel] = (copy.wait_recv,)
    gated_sum.through(BOTH)
    other_sum = _Sum(UNITS[1], at, hop(1), second, lambda here, col: mine_ref.at[(*here[:COLOURS], core, col)], r1_ref, boxes[1], final(gb_ref, UNITS[1]))
    other_sum.far(0)
    gated_sum.close(BOTH)
    gated_share.start()
    other_sum.straight(0)
    other_sum.through(0)
    gated_share.forward()
    other_sum.close(0)
    other_sum.far(1)
    other_sum.straight(1)

    for k, (_, blocks, rows, own, begin) in enumerate(TABLE):
        pltpu.make_async_copy(w_refs[k].at[group], wn_refs[k], w_sem.at[k]).wait()
        for j in range(blocks):
            wt_ref[j % RING, :rows, :] = wn_refs[k][:, _lanes(j)].astype(f32)
            ow_ref[begin + j * own : begin + (j + 1) * own, :] = wt_ref[j % RING, pl.ds(mine * own, own), :]
    other_sum.through(1)
    gated_share.cross()
    other_sum.close(1)
    other_sum.far(BOTH)
    other_sum.straight(BOTH)
    other_sum.through(BOTH)
    other_sum.close(BOTH)

    size = COLOURS * UNIT
    other_share.start()

    def swap_squares(total, which, targets, box):
        n, base = len(targets), COLOURS * which
        ps_ref[which] = total
        for k, to in enumerate(targets):
            copy = remote(ps_ref.at[which], box.at[n - 1 - k], ps_send.at[base + k], ps_recv.at[base + n - 1 - k], to)
            copy.start()
            pending.append(copy)
        for k in range(n):
            remote(box.at[k], box.at[k], ps_send.at[base + k], ps_recv.at[base + k], targets[0]).wait_recv()
            total = total + box[k]
        return total

    total = sum(squares[1:], squares[0])
    total = swap_squares(total, 0, [device(0, by) for by in (1, BOTH, COLOURS)], px_ref)
    other_share.forward()
    total = swap_squares(total, 1, [device(1, by) for by in (1, BOTH, COLOURS)], py_ref)
    other_share.cross()
    gated_share.finish()
    for n in range(FAMILY):
        gf_ref[n * part : (n + 1) * part, :] = ga_ref[n].astype(f32)
    other_share.finish()
    for n in range(FAMILY):
        gf_ref[GATED + n * (size - part) : GATED + (n + 1) * (size - part), :] = gb_ref[n].astype(f32)
    total = swap_squares(total, BOTH, family, p8_ref)
    mean = jnp.sum(total) / float(sum(a * b for a, b in SHAPE.values()))
    factor = jnp.minimum(1.0, 0.5 * lax.rsqrt(jnp.full((FAMILY, LANES), mean, f32) + 1e-30))

    for copy in fetched[:14]:
        copy.wait()
    for k, (_, blocks, rows, own, begin) in enumerate(TABLE):
        for j in range(blocks):
            lanes = _lanes(j)
            to = slice(begin + j * own, begin + (j + 1) * own)
            g = gf_ref[pl.ds(_flat(k) + j * rows + mine * own, own), :] * factor[:1]
            w = ow_ref[to, :]
            m = 0.9 * m_refs[k][_at(k, lanes)] + 0.1 * g
            v = 0.95 * v_refs[k][_at(k, lanes)] + 0.05 * g * g
            ou_ref[to, :] = w - 0.02 * (m * lax.rsqrt(v + 1e-8) + 0.1 * w)
            gq_ref[to, :] = g

    wb_ref[mine] = ou_ref[...].astype(bf16)
    new_share.start()
    new_share.forward()
    new_share.cross()
    new_share.finish()

    def gathered(n):
        ou_ref[...] = wb_ref[n].astype(f32)
        for k, (_, blocks, rows, own, begin) in enumerate(TABLE):
            for j in range(blocks):
                gf_ref[pl.ds(_flat(k) + j * rows + n * own, own), :] = ou_ref[begin + j * own : begin + (j + 1) * own, :]

    lax.fori_loop(0, FAMILY, lambda n, _: gathered(n), None)
    here = tuple(at)

    def own_rows(low, high):
        base, n = (0, part) if low < part else (GATED - part, size - part)
        return gf_ref[pl.ds(pl.multiple_of(mine * n, FAMILY) + base + low, high - low), :].astype(bf16)

    for col in range(COLOURS):
        low, high = col * UNIT, (col + 1) * UNIT
        for a, b in ((low, min(high, part)), (max(low, part), high)):
            if a < b:
                wv_ref[(*here, col, slice(a - low, b - low))] = own_rows(a, b)

    outs = []

    def hand_on(col, rel):
        axis = ORDER[col][0]
        q = _near(at[axis] + rel)
        src, dst = wv_ref.at[(*_where(axis, q), col)], out_ref.at[(*_where(axis, q), core, col)]
        n = col * RING + rel
        copy = remote(src, dst, od_send.at[n], od_recv.at[n], partner)
        copy.start()
        local = pltpu.make_async_copy(src, dst, ol_sem.at[n])
        local.start()
        outs.append((copy, local))

    def gather_phase(phase, chunk, done):
        def start(col, d, slot, rel, h):
            copy = hop(BOTH)(phase, col, d, slot, chunk(col, rel, h), chunk(col, rel, h))
            copy.start()
            pending.append(copy)

        def arrived(col, d, slot, rel, h):
            hop(BOTH)(phase, col, d, slot, chunk(col, rel, h), chunk(col, rel, h)).wait_recv()

        for slot in range(BOTH):
            for col in range(COLOURS):
                for d in range(BOTH):
                    start(col, d, slot, 0, d if slot == 0 else 1 - d)
        for col in range(COLOURS):
            done(col, 0)
        for col in range(COLOURS):
            for d, rel in BEHIND:
                arrived(col, d, 0, rel, d)
                start(col, d, BOTH, rel, d)
        for col in range(COLOURS):
            for d, rel in BEHIND:
                arrived(col, d, 1, rel, 1 - d)
                done(col, rel)
        for col in range(COLOURS):
            for d in range(BOTH):
                arrived(col, d, BOTH, BOTH, d)
            done(col, BOTH)

    cut = UNIT // BOTH

    def last_chunk(col, rel, h):
        spot = list(at)
        spot[ORDER[col][BOTH]] = _near(at[ORDER[col][BOTH]] + rel)
        return wv_ref.at[(*spot, col, pl.ds(h * cut, cut))]

    def middle_chunk(col, rel, h):
        spot = list(at)
        spot[ORDER[col][1]] = _near(at[ORDER[col][1]] + rel)
        spot[ORDER[col][BOTH]] = _half(h)
        return wv_ref.at[(*spot, col)]

    def whole_chunk(col, rel, h):
        axis = ORDER[col][0]
        return wv_ref.at[(*_where(axis, _near(at[axis] + rel), _half(h)), col)]

    gather_phase(BOTH, last_chunk, lambda col, rel: None)
    gather_phase(1, middle_chunk, lambda col, rel: None)
    gather_phase(0, whole_chunk, hand_on)

    for copy in swaps + gated_sum.sent + other_sum.sent + pending:
        copy.wait_send()
    for copy, local in outs:
        copy.wait_send()
        local.wait()
    for n, (col, rel) in enumerate((c, r) for c in range(COLOURS) for r in range(RING)):
        axis = ORDER[col][0]
        dst = out_ref.at[(*_where(axis, _near(at[axis] + rel)), 1 - core, col)]
        remote(dst, dst, od_send.at[n], od_recv.at[n], partner).wait_recv()


def sum_step_gather(g, weights, m, v, back):
    vmem, dma = pltpu.VMEM, pltpu.SemaphoreType.DMA
    hbm, local = pl.BlockSpec(memory_space=pl.ANY), pl.BlockSpec(memory_space=vmem)
    cube, sides = (RING, RING, RING), (COLOURS, BOTH, COLOURS)
    given = [*_rows(m), *_rows(v), *back]
    scratch = [vmem(one.shape, one.dtype) for one in given] + [vmem((SHAPE[name][0] // GROUPS, SHAPE[name][1]), bf16) for name in NAMES]
    for unit in UNITS:
        row = (unit, LANES)
        scratch += [vmem((*sides, BOTH, RING, *row), bf16), vmem((COLOURS, RING, RING, *row), f32), vmem((*sides, BOTH, *row), bf16), vmem((COLOURS, COLOURS, RING, *row), bf16),
                    vmem((COLOURS, RING, *row), f32), vmem((*sides, unit // BOTH, LANES), bf16), vmem((COLOURS, COLOURS, *row), bf16)]
    own, tile, head = (OWN, LANES), (FAMILY, LANES), (TOKENS, HEAD)
    scratch += [vmem((*cube, COLOURS, UNITS[0], LANES), bf16), vmem((*cube, COLOURS, UNITS[0], LANES), bf16), vmem((*cube, BOTH, COLOURS, UNITS[1], LANES), bf16),
                vmem((*cube, COLOURS, UNITS[1], LANES), bf16), vmem((FAMILY, COLOURS * UNITS[0], LANES), bf16), vmem((FAMILY, COLOURS * UNITS[1], LANES), bf16), vmem((FLAT, LANES), f32),
                vmem((RING, 200, LANES), f32), vmem(own, f32), vmem(own, f32), vmem((FAMILY, *own), bf16), vmem((*cube, COLOURS, UNIT, LANES), bf16)]
    scratch += [vmem((n, *tile), f32) for n in (COLOURS, COLOURS, COLOURS, MATRICES)]
    scratch += [vmem((TOKENS, (HEADS + BOTH) * HEAD), bf16), vmem((HEAD, HEADS * BACK), f32), vmem(head, f32), vmem(head, f32), vmem((HEADS, BACK, HEAD), bf16)]
    scratch += [dma((n,)) for n in (162, 162, 24, 24, CHUNKS, 23, MATRICES, 13, 13, 18, 18, CHUNKS, CHUNKS, CHUNKS, CHUNKS, CHUNKS)]
    return pl.pallas_call(
        _comm,
        out_shape=[jax.ShapeDtypeStruct((*cube, BOTH, COLOURS, UNIT, LANES), bf16), jax.ShapeDtypeStruct(own, f32)],
        in_specs=[hbm] * 31,
        out_specs=[hbm, local],
        scratch_shapes=scratch,
        compiler_params=pltpu.CompilerParams(collective_id=0, has_side_effects=True, vmem_limit_bytes=67043328),
    )(g, *[w.reshape(GROUPS, w.shape[1] // GROUPS, w.shape[BOTH]) for w in weights], *given)


PER = RING


def _finish(flat_ref, gq_ref, *rest):
    m_refs, v_refs, w_refs, mo_refs, vo_refs = (rest[i : i + MATRICES] for i in range(0, 35, MATRICES))

    @pl.when(pl.program_id(0) == 0)
    def _():
        for k, (_, blocks, _, own, first) in enumerate(TABLE):
            for j in range(blocks):
                at = _at(k, _lanes(j))
                g = gq_ref[first + j * own : first + (j + 1) * own, :]
                mo_refs[k][at] = 0.9 * m_refs[k][at] + 0.1 * g
                vo_refs[k][at] = 0.95 * v_refs[k][at] + 0.05 * g * g

    for k, (_, blocks, rows, _, _) in enumerate(TABLE):
        lengths = (COLOURS * UNITS[1], GATED) if k < RING else (COLOURS * UNITS[0], 0)
        for j in range(blocks):
            row, to = _flat(k) + j * rows - lengths[1], 0
            while to < rows:
                n, low = row // lengths[0], row % lengths[0]
                some = min(lengths[0] - low, rows - to)
                low += n * COLOURS * UNIT + (COLOURS * UNITS[0] if k < RING else 0)
                for i in range(PER):
                    w_refs[k][0, i * rows + to : i * rows + to + some, _lanes(j)] = flat_ref[i, low : low + some, :]
                row, to = row + some, to + some


def finish(flat, gq, m, v):
    whole = pl.BlockSpec(memory_space=pltpu.VMEM)
    old = [*_rows(m), *_rows(v)]
    shapes = [(1, *SHAPE[name]) for name in NAMES]
    out = pl.pallas_call(
        _finish,
        grid=(GROUPS // PER,),
        out_shape=[jax.ShapeDtypeStruct(shape, jnp.bfloat16) for shape in shapes] + [jax.ShapeDtypeStruct(a.shape, a.dtype) for a in old],
        in_specs=[pl.BlockSpec((PER, FLAT, LANES), lambda i: (i, 0, 0)), whole] + [whole] * 14,
        out_specs=[pl.BlockSpec((1, shape[1] // GROUPS * PER, shape[BOTH]), lambda i: (0, i, 0)) for shape in shapes] + [whole] * 14,
        compiler_params=pltpu.CompilerParams(vmem_limit_bytes=VMEM),
    )(flat.reshape(GROUPS, FLAT, LANES), gq, *old)
    moments = [new.reshape(1, *new.shape) if new.ndim == BOTH else new.transpose(1, 0, BOTH) for new in out[MATRICES:]]
    return (*out[:MATRICES], *moments)


def solution(mesh):
    def step(x, dy, *arrays):
        weights, m, v = (arrays[i : i + MATRICES] for i in (0, MATRICES, 14))
        w = dict(zip(NAMES, weights, strict=True))
        plain = {name: w[name][0] for name in ("wq", "wk", "wv", "wo")}
        a, q, k, value, ot, lse, h = attend(x[0], plain)
        g, dh = gated(h, dy[0], w)
        back = (dh, a, q, k, value, ot, lse, _angles(), plain["wo"])
        flat, gq = sum_step_gather(g.reshape(RING, RING, RING, 2, COLOURS, UNITS[0], LANES), weights, m, v, back)
        return finish(flat, gq, m, v)

    states, all_of, cut = P(("rep", "dp")), P(), P(None, "dp")
    return jax.shard_map(
        step,
        mesh=mesh,
        in_specs=(states, states) + (all_of,) * MATRICES + (cut,) * 14,
        out_specs=(P("rep"),) * MATRICES + (P("rep", "dp"),) * 14,
        check_vma=False,
    )
```

```python
import functools

import jax
import jax.numpy as jnp
import numpy as np
from jax import lax
from jax.experimental import pallas as pl
from jax.experimental.pallas import tpu as pltpu
from jax.sharding import PartitionSpec as P

NEG = -1e30
HIDDEN = 2 * NEG
LOG2E = 1.4426950408889634
VMEM = 56 * 2**20
NAMES = ("wq", "wk", "wv", "wo", "w_gate", "w_up", "w_down")
TOKENS, D, HEADS, HEAD, FF = 1024, 640, 8, 128, 3200
SCALE = HEAD**-0.5
E = SCALE * LOG2E
THETA = 10000
f32, bf16 = jnp.float32, jnp.bfloat16


def _dot(a, b, ca=1, cb=0):
    return lax.dot_general(a, b, (((ca,), (cb,)), ((), ())), preferred_element_type=f32)


def _dot_t(a, b):
    return _dot(a, b, 1, 1)


def _lanes(k):
    return slice(k * 128, (k + 1) * 128)


def _scale(wide):
    return lax.rsqrt(jnp.mean(wide * wide, -1, keepdims=True) + 1e-6)


def _normed(wide):
    return wide * _scale(wide)


HALF = HEAD // 2


def _angles():
    angle = np.arange(TOKENS, dtype=np.float32)[:, None] * np.float32(THETA) ** (-np.arange(HALF, dtype=np.float32) / np.float32(HALF))
    return np.concatenate([np.cos(angle), np.sin(angle)], 1).astype(np.float32)


def _spread(angles):
    other = pltpu.roll(angles, HALF, 1)
    low = lax.broadcasted_iota(jnp.int32, angles.shape, 1) < HALF
    return jnp.where(low, angles, other), jnp.where(low, -other, angles)
LANES, GROUPS = 128, 16
BOTH, COLOURS, RING, FAMILY, MATRICES, CHUNKS = 2, 3, 4, 8, 7, 12


BQ, BK = 1024, 256


def _attend(x_ref, angle_ref, wq_ref, wk_ref, wv_ref, wo_ref, a_ref, q_ref, k_ref, v_ref, ot_ref, lse_ref, h_ref, ks, vts, top_s, mix_s):
    i = pl.program_id(0)
    a = _normed(x_ref[...].astype(f32)).astype(bf16)
    a_ref[...] = a
    cos, sin = _spread(angle_ref[...])

    def turned(t):
        t = t.astype(bf16).astype(f32)
        return (t * cos + pltpu.roll(t, HALF, 1) * sin).astype(bf16)

    k = turned(_dot(a, wk_ref[...]))
    v = _dot(a, wv_ref[...]).astype(bf16)
    k_ref[...] = k
    v_ref[...] = v
    here = pl.ds(pl.multiple_of(i * BQ, BQ), BQ)
    ks[here, :] = k
    vts[:HEAD, here] = v.T
    vts[HEAD:, here] = jnp.ones((8, BQ), bf16)
    q = _dot(a, wq_ref[...])
    for n in range(HEADS):
        q_ref[n] = turned(q[:, _lanes(n)])
    top_s[...] = jnp.full(top_s.shape, NEG, f32)
    mix_s[...] = jnp.zeros(mix_s.shape, f32)

    def block(j, low, masked):
        keys = pl.ds(pl.multiple_of(j * BK, BK), BK)
        scores = [_dot_t(ks[keys, :], q_ref[n, low:, :]) for n in range(HEADS)]
        if masked:
            hidden = lax.broadcasted_iota(jnp.int32, (BK, BQ - low), 1) < lax.broadcasted_iota(jnp.int32, (BK, BQ - low), 0)
        values = vts[:, keys]
        weights, keeps = [], []
        for n, s in enumerate(scores):
            if masked:
                s = jnp.where(hidden, HIDDEN, s)
            old = top_s[n : n + 1, low:]
            top = jnp.maximum(old, s.max(axis=0, keepdims=True))
            top_s[n : n + 1, low:] = top
            weights.append(jnp.exp2((s - top) * E).astype(bf16))
            keeps.append(jnp.exp2((old - top) * E))
        for n, (p, keep) in enumerate(zip(weights, keeps)):
            mix_s[n, :, low:] = mix_s[n, :, low:] * keep + _dot(values, p)

    per = BQ // BK
    lax.fori_loop(0, per * i, lambda j, _: block(j, 0, False), None)
    for n in range(per):
        block(per * i + n, n * BK, True)
    outs = []
    for n in range(HEADS):
        total = mix_s[n, HEAD : HEAD + 1, :]
        out = (mix_s[n, :HEAD, :] * (1 / total)).astype(bf16)
        ot_ref[_lanes(n), :] = out
        outs.append(out.T)
        lse_ref[n : n + 1, :] = top_s[n : n + 1, :] * SCALE + jnp.log(total)
    more = _dot(jnp.concatenate(outs, axis=1), wo_ref[...]).astype(bf16)
    h_ref[...] = (x_ref[...].astype(f32) + more.astype(f32)).astype(bf16)


def attend(x, w):
    whole = pl.BlockSpec(memory_space=pltpu.VMEM)
    rows = lambda width: pl.BlockSpec((BQ, width), lambda i: (i, 0))
    columns = lambda height: pl.BlockSpec((height, BQ), lambda i: (0, i))
    shape = jax.ShapeDtypeStruct
    return pl.pallas_call(
        _attend,
        grid=(TOKENS // BQ,),
        in_specs=[rows(D), rows(HEAD)] + [whole] * 4,
        out_specs=[rows(D), pl.BlockSpec((HEADS, BQ, HEAD), lambda i: (0, i, 0)), rows(HEAD), rows(HEAD), columns(HEADS * HEAD), columns(HEADS), rows(D)],
        out_shape=[shape((TOKENS, D), bf16), shape((HEADS, TOKENS, HEAD), bf16), shape((TOKENS, HEAD), bf16), shape((TOKENS, HEAD), bf16),
                   shape((HEADS * HEAD, TOKENS), bf16), shape((HEADS, TOKENS), f32), shape((TOKENS, D), bf16)],
        scratch_shapes=[pltpu.VMEM((TOKENS, HEAD), bf16), pltpu.VMEM((HEAD + 8, TOKENS), bf16), pltpu.VMEM((HEADS, BQ), f32),
                        pltpu.VMEM((HEADS, HEAD + 8, BQ), f32)],
        compiler_params=pltpu.CompilerParams(dimension_semantics=("arbitrary",), vmem_limit_bytes=VMEM),
    )(x, _angles(), *[w[name] for name in ("wq", "wk", "wv", "wo")])


BF = 256
LAST = FF // BF
CHUNK = 512


def _gated(h_ref, dy_ref, wg_ref, wu_ref, wd_ref, g_ref, dh_ref, b_s, bt_s, dyt_s, acc_s, hid_s, dg_s, du_s, stage, down_s, zero_s, sem, end_sem):
    j = pl.program_id(0)
    slot = lax.rem(j, 2)
    firsts = [TABLE[NAMES.index(name)][0] for name in ("w_gate", "w_up", "w_down")]
    rows = D // GROUPS
    ends = 3 * FF * D // GROUPS // LANES

    def put(n, at, size):
        where = pl.ds(pl.multiple_of(firsts[n] + at * (rows * BF // LANES), 8), size)
        return pltpu.make_async_copy(stage.at[n, slot, :, pl.ds(0, size)], g_ref.at[:, where], sem.at[n, slot])

    @pl.when(j == 0)
    def _():
        b = _normed(h_ref[...].astype(f32)).astype(bf16)
        b_s[...] = b
        bt_s[...] = b.T
        dyt_s[...] = dy_ref[...].T
        acc_s[...] = jnp.zeros(acc_s.shape, f32)
        zero_s[...] = jnp.zeros(zero_s.shape, bf16)
        pltpu.make_async_copy(zero_s, g_ref.at[:, pl.ds(ends, GATED - ends)], end_sem.at[0]).start()

    left = FF - j * BF
    inside = lax.broadcasted_iota(jnp.int32, (D, BF), 1) < left
    wg, wu = (jnp.where(inside, ref[0], jnp.zeros((), bf16)) for ref in (wg_ref, wu_ref))
    wd = jnp.where(lax.broadcasted_iota(jnp.int32, (BF, D), 0) < left, wd_ref[0], jnp.zeros((), bf16))
    for at in range(0, TOKENS, CHUNK):
        here = slice(at, at + CHUNK)
        gate, up = _dot(b_s[here, :], wg), _dot(b_s[here, :], wu)
        dhid = _dot_t(dy_ref[here, :], wd).astype(bf16).astype(f32)
        share = 1 / (1 + jnp.exp(-gate))
        silu = gate * share
        hid_s[here, :] = (silu * up).astype(bf16)
        dgate = (dhid * up * (share * (1 + gate * (1 - share)))).astype(bf16)
        dup = (dhid * silu).astype(bf16)
        dg_s[here, :] = dgate
        du_s[here, :] = dup
        acc_s[here, :] += _dot_t(dgate, wg) + _dot_t(dup, wu)

    @pl.when(j >= 2)
    def _():
        for n in range(2):
            put(n, j - 2, rows * BF // LANES).wait()

    for n, one in enumerate((dg_s, du_s)):
        term = _dot(bt_s[...], one[...])
        for k in range(BF // LANES):
            stage[n, slot, :, k * rows : (k + 1) * rows, :] = term[:, _lanes(k)].reshape(GROUPS, rows, LANES).astype(bf16)
    term = _dot(dyt_s[...], hid_s[...]).T
    for k in range(D // LANES):
        down_s[k, pl.ds(pl.multiple_of(j * BF, BF), BF), :] = term[:, _lanes(k)].astype(bf16)

    @pl.when(j < LAST)
    def _():
        for n in range(2):
            put(n, j, rows * BF // LANES).start()

    @pl.when(j == LAST)
    def _():
        for n in range(2):
            put(n, j, rows * (FF % BF) // LANES).start()
        per = FF // GROUPS
        for k in range(D // LANES):
            for n in range(GROUPS):
                pltpu.make_async_copy(down_s.at[k, pl.ds(n * per, per)], g_ref.at[n, pl.ds(firsts[2] + k * per, per)], end_sem.at[1]).start()
        for at in range(0, TOKENS, CHUNK):
            here = slice(at, at + CHUNK)
            db = acc_s[here, :].astype(bf16).astype(f32)
            h = h_ref[here, :].astype(f32)
            s = _scale(h)
            through = db * s - h * (s * s * s * jnp.mean(db * h, -1, keepdims=True))
            dh_ref[here, :] = (dy_ref[here, :].astype(f32) + through.astype(bf16).astype(f32)).astype(bf16)
        for n in range(2):
            put(n, j, rows * (FF % BF) // LANES).wait()
            pltpu.make_async_copy(stage.at[n, 1 - slot], stage.at[n, 1 - slot], sem.at[n, 1 - slot]).wait()
        pltpu.make_async_copy(zero_s, g_ref.at[:, pl.ds(ends, GATED - ends)], end_sem.at[0]).wait()
        whole = g_ref.at[:, pl.ds(firsts[2], ends - firsts[2])]
        pltpu.make_async_copy(whole, whole, end_sem.at[1]).wait()


def gated(h, dy, w):
    vmem = pltpu.VMEM
    whole = pl.BlockSpec(memory_space=vmem)
    across = pl.BlockSpec((1, D, BF), lambda j: (0, 0, j))
    pad = GATED - 3 * FF * D // GROUPS // LANES
    return pl.pallas_call(
        _gated,
        grid=(LAST + 1,),
        in_specs=[whole, whole, across, across, pl.BlockSpec((1, BF, D), lambda j: (0, j, 0))],
        out_specs=[pl.BlockSpec(memory_space=pl.ANY), whole],
        out_shape=[jax.ShapeDtypeStruct((GROUPS, GATED, LANES), bf16), jax.ShapeDtypeStruct((TOKENS, D), bf16)],
        scratch_shapes=[vmem((TOKENS, D), bf16), vmem((D, TOKENS), bf16), vmem((D, TOKENS), bf16), vmem((TOKENS, D), f32),
                        vmem((TOKENS, BF), bf16), vmem((TOKENS, BF), bf16), vmem((TOKENS, BF), bf16),
                        vmem((2, 2, GROUPS, D // GROUPS * BF // LANES, LANES), bf16), vmem((D // LANES, (LAST + 1) * BF, LANES), bf16), vmem((GROUPS, pad, LANES), bf16),
                        pltpu.SemaphoreType.DMA((2, 2)), pltpu.SemaphoreType.DMA((2,))],
        compiler_params=pltpu.CompilerParams(dimension_semantics=("arbitrary",), vmem_limit_bytes=VMEM),
    )(h, dy, *[w[name] for name in ("w_gate", "w_up", "w_down")])


BACK = 256


def _back_step(i, dh_ref, q_ref, k_ref, v_ref, ot_ref, lse_ref, angle_ref, wo_ref, dqkv_s, dqt_s, dk_s, dv_s, do_s):
    here = pl.ds(pl.multiple_of(i * BACK, BACK), BACK)
    dqt_s[...] = jnp.zeros(dqt_s.shape, f32)
    dh, wo = dh_ref[here, :], wo_ref[...]
    dot = _dot_t(wo, dh).astype(bf16).astype(f32) * ot_ref[:, here].astype(f32)
    delta = [dot[_lanes(n), :].sum(axis=0, keepdims=True) for n in range(HEADS)]
    dout = _dot_t(dh, wo).astype(bf16)
    for n in range(HEADS):
        do_s[n] = dout[:, _lanes(n)]
    pairs = range(0, HEADS, 2)
    beside = lambda rows, n: jnp.concatenate([rows[n], rows[n + 1]], axis=1)
    lses = [lse_ref[n : n + 1, here] * LOG2E for n in range(HEADS)]

    def block(j, masked):
        keys = pl.ds(pl.multiple_of(j * BACK, BACK), BACK)
        k, v = k_ref[keys, :], v_ref[keys, :]
        kt = k.T
        if masked:
            place = lax.broadcasted_iota(jnp.int32, (BACK, 2 * BACK), 1)
            hidden = jnp.where(place < BACK, place, place - BACK) < lax.broadcasted_iota(jnp.int32, (BACK, 2 * BACK), 0)
        for some in (pairs[:2], pairs[2:]):
            qs = [q_ref[n : n + 2, here, :].reshape(2 * BACK, HEAD) for n in some]
            dos = [do_s[n : n + 2].reshape(2 * BACK, HEAD) for n in some]
            scores = [_dot_t(k, q) for q in qs]
            dps = [_dot_t(v, one) for one in dos]
            for n, q, do, score, dp in zip(some, qs, dos, scores, dps):
                p = jnp.exp2(score * E - beside(lses, n))
                if masked:
                    p = jnp.where(hidden, 0.0, p)
                ds = (p * (dp - beside(delta, n))).astype(bf16)
                dv_s[keys, :] += _dot(p.astype(bf16), do)
                dk_s[keys, :] += _dot(ds, q)
                dqt_s[:, n * BACK : (n + 2) * BACK] += _dot(kt, ds)

    lax.fori_loop(0, i, lambda j, _: block(j, False), None)
    block(i, True)
    both = angle_ref[here, :].T
    cost, sint = both[:HALF], both[HALF:]
    for n in range(HEADS):
        t = (dqt_s[:, n * BACK : (n + 1) * BACK] * SCALE).astype(bf16).astype(f32)
        one, two = t[:HALF], t[HALF:]
        t = jnp.concatenate([one * cost + two * sint, two * cost - one * sint], axis=0)
        dqkv_s[here, _lanes(n)] = t.astype(bf16).T


def _back_put(put, term, first):
    rows = term.shape[0] // GROUPS
    for k in range(term.shape[1] // LANES):
        put(first + k * rows, term[:, _lanes(k)].reshape(GROUPS, rows, LANES))


def _back_qkv(put, a_ref, angle_ref, dqkv_s, dk_s, dv_s):
    wide = HEADS * HEAD
    cos, sin = _spread(angle_ref[...])
    t = (dk_s[...] * SCALE).astype(bf16).astype(f32)
    dqkv_s[:, wide : wide + HEAD] = (t * cos - pltpu.roll(t, HALF, 1) * sin).astype(bf16)
    dqkv_s[:, wide + HEAD :] = dv_s[...].astype(bf16)
    _back_put(put, _dot(a_ref[...].T, dqkv_s[...]), TABLE[0][0])


MESH, ALL = pl.DeviceIdType.MESH, slice(None)
SHAPE = {"wq": (640, 1024), "wk": (640, 128), "wv": (640, 128), "wo": (1024, 640), "w_gate": (640, 3200), "w_up": (640, 3200), "w_down": (3200, 640)}
UNIT = 160
UNITS = (LANES, 32)
GATED, OTHERS = 24 * UNITS[0], 24 * UNITS[1]
FLAT = GATED + OTHERS
ORDER = ((0, 1, 2), (1, 2, 0), (2, 0, 1))
AHEAD, BEHIND = ((0, 1), (1, COLOURS)), ((0, COLOURS), (1, 1))
WAY = (2, 1, COLOURS, 0)


def _table():
    table, flat, mine = [], 0, 0
    for name in NAMES:
        rows, cols = SHAPE[name]
        flat = 0 if name == "w_gate" else flat
        blocks, group, own = cols // LANES, rows // GROUPS, rows // LANES
        table.append((flat, blocks, group, own, mine))
        flat += blocks * group
        mine += blocks * own
    return tuple(table)


TABLE, OWN = _table(), COLOURS * UNIT


def _flat(k):
    return TABLE[k][0] + (GATED if k < RING else 0)


def _at(k, lanes):
    return (ALL, lanes) if TABLE[k][COLOURS] % FAMILY == 0 else (ALL, 0, lanes)


def _rows(moments):
    return [one[0] if one.shape[1] % FAMILY == 0 else one.transpose(1, 0, BOTH) for one in moments]


def _near(q):
    return lax.rem(q, RING)


def _where(axis, q, first=ALL):
    return ((q, first, ALL), (first, q, ALL), (first, ALL, q))[axis]


def _place(axis, q, a, b):
    return ((q, a, b), (a, q, b), (a, b, q))[axis]


def _half(h):
    return pl.ds(BOTH * h, BOTH)


class _Sum:
    def __init__(self, unit, at, hop, swaps, own, other, boxes, final):
        self.unit, self.at, self.hop, self.swaps, self.own, self.other, self.last = unit, at, hop, swaps, own, other, final
        self.ra, self.f, self.rb, self.sb, self.f2, self.rc, self.sc = boxes
        self.sent, self.cut = [], unit // BOTH

    def spot(self, col, rel, h, u):
        axis = ORDER[col][0]
        return _place(axis, _near(self.at[axis] + rel), BOTH * h + lax.div(u, RING), lax.rem(u, RING))

    def chunk(self, phase, col, rel):
        return _near(self.at[ORDER[col][phase]] + rel)

    def rows(self, h):
        return slice(h * self.cut, (h + 1) * self.cut)

    def term(self, phase, col, rel, h, u):
        if phase == 0:
            here = self.spot(col, rel, h, u)
            return self.own(here, col)[...].astype(f32) + self.other[(*here, col)].astype(f32)
        if phase == 1:
            return self.f[col, self.chunk(1, col, rel), BOTH * h + u]
        return self.f2[col, self.chunk(BOTH, col, rel), self.rows(h)]

    def source(self, phase, col, rel, h):
        if phase == 0:
            axis = ORDER[col][0]
            return self.own(_where(axis, self.chunk(0, col, rel), _half(h)), col)
        return self.sb.at[col, rel - 1, _half(h)] if phase == 1 else self.sc.at[col, rel - 1, self.rows(h)]

    def store(self, phase, col, rel, h, u, x):
        x = x.astype(bf16)
        if phase == 0:
            self.own(self.spot(col, rel, h, u), col)[...] = x
        elif phase == 1:
            self.sb[col, rel - 1, BOTH * h + u] = x
        else:
            self.sc[col, rel - 1, self.rows(h)] = x

    def inbox(self, phase, col, d, slot):
        return (self.ra, self.rb, self.rc)[phase].at[col, d, slot]

    def value(self, phase, col, d, slot, u):
        box = self.inbox(phase, col, d, slot)
        box = (box.at[lax.div(u, RING), lax.rem(u, RING)] if phase == 0 else box.at[u] if phase == 1 else box)
        return box[...].astype(f32)

    def final(self, phase, col, h, u, x):
        if phase == 0:
            a, b = BOTH * h + lax.div(u, RING), lax.rem(u, RING)
            self.f[(col, b, a) if col == 1 else (col, a, b)] = x
        elif phase == 1:
            self.f2[col, BOTH * h + u] = x
        else:
            self.last(col, h, x)

    def each(self, phase, body):
        units = (FAMILY, BOTH, 1)[phase]
        if units == 1:
            body(0)
        else:
            lax.fori_loop(0, units, lambda u, _: body(u), None)

    def copy(self, phase, col, d, slot, rel, h):
        return self.hop(phase, col, d, slot, self.source(phase, col, rel, h), self.inbox(phase, col, d, slot))

    def start(self, *what):
        self.copy(*what).start()
        self.sent.append(what)

    def drain(self):
        for what in self.sent:
            self.copy(*what).wait_send()

    def arrived(self, phase, col, d, slot):
        box = self.inbox(phase, col, d, slot)
        self.hop(phase, col, d, slot, box, box).wait_recv()

    def ready(self, phase, col, rel):
        if phase == 0:
            for wait in self.swaps[col, rel]:
                wait()

    def far(self, phase):
        for col in range(COLOURS):
            self.ready(phase, col, BOTH)
            for d in range(BOTH):
                self.each(phase, lambda u: self.store(phase, col, BOTH, d, u, self.term(phase, col, BOTH, d, u)))
                self.start(phase, col, d, 0, BOTH, d)

    def straight(self, phase):
        for col in range(COLOURS):
            for d, rel in AHEAD:
                self.ready(phase, col, rel)
                self.each(phase, lambda u: self.store(phase, col, rel, 1 - d, u, self.term(phase, col, rel, 1 - d, u)))
                self.start(phase, col, d, 1, rel, 1 - d)

    def through(self, phase):
        for col in range(COLOURS):
            for d, rel in AHEAD:
                self.arrived(phase, col, d, 0)
                self.each(phase, lambda u: self.store(phase, col, rel, d, u, self.term(phase, col, rel, d, u) + self.value(phase, col, d, 0, u)))
                self.start(phase, col, d, BOTH, rel, d)

    def close(self, phase):
        for col in range(COLOURS):
            self.ready(phase, col, 0)
            for d in range(BOTH):
                for slot in (1, BOTH):
                    self.arrived(phase, col, d, slot)
            for h in range(BOTH):
                self.each(phase, lambda u: self.final(phase, col, h, u, self.term(phase, col, 0, h, u) + self.value(phase, col, 0, BOTH - h, u)
                                                      + self.value(phase, col, 1, 1 + h, u)))


def _comm(g_ref, *rest):
    w_refs, rest = rest[:MATRICES], rest[MATRICES:]
    m_refs, v_refs, rest = rest[:MATRICES], rest[MATRICES:14], rest[14:]
    dh_ref, a_ref, q_ref, k_ref, v_ref, ot_ref, lse_ref, angle_ref, wo_ref, out_ref, gq_ref, *rest = rest
    wn_refs, rest = rest[:MATRICES], rest[MATRICES:]
    boxes, rest = (rest[:MATRICES], rest[MATRICES:14]), rest[14:]
    (s_ref, r0_ref, mine_ref, r1_ref, ga_ref, gb_ref, gf_ref, wt_ref, ow_ref, ou_ref, wb_ref, wv_ref, ps_ref, px_ref, py_ref, p8_ref,
     dqkv_s, dqt_s, dk_s, dv_s, do_s, ring_send, ring_recv, d2d_send, d2d_recv, load_sem, w_sem, ps_send, ps_recv, zs_send, zs_recv,
     zd_send, zd_recv, od_send, od_recv, ol_sem) = rest
    me = lax.axis_index("dp")
    core = lax.rem(me, BOTH)
    at = [lax.rem(lax.div(me, 32), RING), lax.rem(lax.div(me, FAMILY), RING), lax.rem(lax.div(me, BOTH), RING)]
    group = lax.div(me, FAMILY)
    mine = lax.rem(me, FAMILY)

    def device(axis, by):
        return me + (lax.rem(at[axis] + by, RING) - at[axis]) * (32, FAMILY, BOTH)[axis]

    partner = me + 1 - BOTH * core
    family = [group * FAMILY + lax.rem(mine + k, FAMILY) for k in range(1, FAMILY)]
    friends = [device(axis, by) for axis in (0, 1) for by in (1, BOTH, COLOURS)] + family
    barrier = pltpu.get_barrier_semaphore()
    for one in friends:
        pl.semaphore_signal(barrier, inc=1, device_id={"dp": one}, device_id_type=MESH)

    def remote(src, dst, send, recv, to):
        return pltpu.make_async_remote_copy(src_ref=src, dst_ref=dst, send_sem=send, recv_sem=recv, device_id={"dp": to}, device_id_type=MESH)

    def hop(base):
        def make(phase, col, d, slot, src, dst):
            n = (((base * COLOURS + phase) * COLOURS + col) * BOTH + d) * COLOURS + slot
            return remote(src, dst, ring_send.at[n], ring_recv.at[n], device(ORDER[col][phase], 1 if d == 0 else COLOURS))

        return make

    chunks = [(n, col, rel, _where(ORDER[col][0], _near(at[ORDER[col][0]] + rel))) for n, (rel, col) in enumerate((r, c) for r in WAY for c in range(COLOURS))]
    loads, swaps = {}, []
    for n, col, rel, here in chunks:
        loads[n] = pltpu.make_async_copy(g_ref.at[(*here, core, col)], s_ref.at[(*here, col)], load_sem.at[n])
        loads[n].start()
    for k in range(MATRICES):
        pltpu.make_async_copy(w_refs[k].at[group], wn_refs[k], w_sem.at[k]).start()
    pl.semaphore_wait(barrier, len(friends))
    first = {}
    for n, col, rel, here in chunks:
        copy = remote(g_ref.at[(*here, 1 - core, col)], r0_ref.at[(*here, col)], d2d_send.at[n], d2d_recv.at[n], partner)
        copy.start()
        swaps.append(copy)
        first[col, rel] = (loads[n].wait, copy.wait_recv)

    pending, squares = [], []

    class Share:
        def __init__(self, number, box):
            self.number, self.box, self.cut = number, box, box.shape[1] // BOTH

        def block(self, rel):
            return self.box.at[BOTH * _near(at[BOTH] + rel) + core]

        def hop(self, d, slot, rel, h):
            n = (self.number * BOTH + d) * COLOURS + slot
            half = self.block(rel).at[pl.ds(h * self.cut, self.cut)]
            return remote(half, half, zs_send.at[n], zs_recv.at[n], device(BOTH, 1 if d == 0 else COLOURS))

        def over(self, rel, whose):
            n = self.number * RING + rel
            block = self.box.at[BOTH * _near(at[BOTH] + rel) + whose]
            return remote(block, block, zd_send.at[n], zd_recv.at[n], partner)

        def go(self, copy):
            copy.start()
            pending.append(copy)

        def start(self):
            for slot in range(BOTH):
                for d in range(BOTH):
                    self.go(self.hop(d, slot, 0, d if slot == 0 else 1 - d))
            self.go(self.over(0, core))

        def forward(self):
            for d, rel in BEHIND:
                self.hop(d, 0, rel, d).wait_recv()
                self.go(self.hop(d, BOTH, rel, d))

        def cross(self):
            for d, rel in BEHIND:
                self.hop(d, 1, rel, 1 - d).wait_recv()
                self.go(self.over(rel, core))
            for d in range(BOTH):
                self.hop(d, BOTH, BOTH, d).wait_recv()
            self.go(self.over(BOTH, core))

        def finish(self):
            for rel in range(RING):
                self.over(rel, 1 - core).wait_recv()

    gated_share, other_share, new_share = Share(0, ga_ref), Share(1, gb_ref), Share(BOTH, wb_ref)

    def final(box, unit):
        def put(col, h, x):
            x = x.astype(bf16)
            row = col * unit + h * (unit // BOTH)
            box[mine, row : row + unit // BOTH, :] = x
            x = x.astype(f32)
            squares.append(jnp.sum((x * x).reshape(unit // GROUPS, FAMILY, LANES), axis=0))

        return put

    part = UNITS[0] * COLOURS
    gated_sum = _Sum(UNITS[0], at, hop(0), first, lambda here, col: s_ref.at[(*here, col)], r0_ref, boxes[0], final(ga_ref, UNITS[0]))

    def put(row, x):
        unit, end = UNITS[1], row + x.shape[1]
        begin = row
        while row < end:
            n, low = row // unit, row % unit
            size = min(unit - low, end - row)
            z, c, col = n // 6, n // COLOURS % BOTH, n % COLOURS
            mine_ref[:, :, z, c, col, low : low + size, :] = x[:, row - begin : row - begin + size].reshape(RING, RING, size, LANES).astype(bf16)
            row += size

    def back(i):
        _back_step(i, dh_ref, q_ref, k_ref, v_ref, ot_ref, lse_ref, angle_ref, wo_ref, dqkv_s, dqt_s, dk_s, dv_s, do_s)

    dk_s[...] = jnp.zeros(dk_s.shape, f32)
    dv_s[...] = jnp.zeros(dv_s.shape, f32)
    _back_put(put, _dot(ot_ref[...], dh_ref[...]), TABLE[COLOURS][0])
    put(OTHERS - 48, jnp.zeros((GROUPS, 48, LANES), f32))

    def back_and_sum(i):
        back(i)
        for n, part_of in enumerate((gated_sum.far, gated_sum.straight, gated_sum.through)):
            pl.when(i == n)(functools.partial(part_of, 0))

    lax.fori_loop(0, TOKENS // BACK, lambda i, _: back_and_sum(i), None)
    gated_sum.close(0)
    gated_sum.far(1)
    gated_sum.straight(1)
    _back_qkv(put, a_ref, angle_ref, dqkv_s, dk_s, dv_s)

    second = {}
    for n, col, rel, here in chunks:
        copy = remote(mine_ref.at[(*here, 1 - core, col)], r1_ref.at[(*here, col)], d2d_send.at[CHUNKS + n], d2d_recv.at[CHUNKS + n], partner)
        copy.start()
        swaps.append(copy)
        second[col, rel] = (copy.wait_recv,)
    gated_sum.through(1)
    other_sum = _Sum(UNITS[1], at, hop(1), second, lambda here, col: mine_ref.at[(*here[:COLOURS], core, col)], r1_ref, boxes[1], final(gb_ref, UNITS[1]))
    other_sum.far(0)
    gated_sum.close(1)
    gated_sum.far(BOTH)
    gated_sum.straight(BOTH)
    other_sum.straight(0)
    other_sum.through(0)
    gated_sum.through(BOTH)
    other_sum.close(0)
    other_sum.far(1)
    other_sum.straight(1)
    gated_sum.close(BOTH)
    gated_share.start()

    for k, (_, blocks, rows, own, begin) in enumerate(TABLE):
        pltpu.make_async_copy(w_refs[k].at[group], wn_refs[k], w_sem.at[k]).wait()
        for j in range(blocks):
            wt_ref[j % RING, :rows, :] = wn_refs[k][:, _lanes(j)].astype(f32)
            ow_ref[begin + j * own : begin + (j + 1) * own, :] = wt_ref[j % RING, pl.ds(mine * own, own), :]
    other_sum.through(1)
    gated_share.forward()
    other_sum.close(1)
    other_sum.far(BOTH)
    other_sum.straight(BOTH)
    gated_share.cross()
    other_sum.through(BOTH)
    other_sum.close(BOTH)

    size = COLOURS * UNIT
    other_share.start()

    def swap_squares(total, which, targets, box):
        n, base = len(targets), COLOURS * which
        ps_ref[which] = total
        for k, to in enumerate(targets):
            copy = remote(ps_ref.at[which], box.at[n - 1 - k], ps_send.at[base + k], ps_recv.at[base + n - 1 - k], to)
            copy.start()
            pending.append(copy)
        for k in range(n):
            remote(box.at[k], box.at[k], ps_send.at[base + k], ps_recv.at[base + k], targets[0]).wait_recv()
            total = total + box[k]
        return total

    total = sum(squares[1:], squares[0])
    total = swap_squares(total, 0, [device(0, by) for by in (1, BOTH, COLOURS)], px_ref)
    other_share.forward()
    total = swap_squares(total, 1, [device(1, by) for by in (1, BOTH, COLOURS)], py_ref)
    other_share.cross()
    gated_share.finish()
    for n in range(FAMILY):
        gf_ref[n * part : (n + 1) * part, :] = ga_ref[n].astype(f32)
    other_share.finish()
    for n in range(FAMILY):
        gf_ref[GATED + n * (size - part) : GATED + (n + 1) * (size - part), :] = gb_ref[n].astype(f32)
    total = swap_squares(total, BOTH, family, p8_ref)
    mean = jnp.sum(total) / float(sum(a * b for a, b in SHAPE.values()))
    factor = jnp.minimum(1.0, 0.5 * lax.rsqrt(jnp.full((FAMILY, LANES), mean, f32) + 1e-30))

    for k, (_, blocks, rows, own, begin) in enumerate(TABLE):
        for j in range(blocks):
            lanes = _lanes(j)
            to = slice(begin + j * own, begin + (j + 1) * own)
            g = gf_ref[pl.ds(_flat(k) + j * rows + mine * own, own), :] * factor[:1]
            w = ow_ref[to, :]
            m = 0.9 * m_refs[k][_at(k, lanes)] + 0.1 * g
            v = 0.95 * v_refs[k][_at(k, lanes)] + 0.05 * g * g
            ou_ref[to, :] = w - 0.02 * (m * lax.rsqrt(v + 1e-8) + 0.1 * w)
            gq_ref[to, :] = g

    wb_ref[mine] = ou_ref[...].astype(bf16)
    new_share.start()
    new_share.forward()
    new_share.cross()
    new_share.finish()

    def gathered(n):
        ou_ref[...] = wb_ref[n].astype(f32)
        for k, (_, blocks, rows, own, begin) in enumerate(TABLE):
            for j in range(blocks):
                gf_ref[pl.ds(_flat(k) + j * rows + n * own, own), :] = ou_ref[begin + j * own : begin + (j + 1) * own, :]

    lax.fori_loop(0, FAMILY, lambda n, _: gathered(n), None)
    here = tuple(at)

    def own_rows(low, high):
        base, n = (0, part) if low < part else (GATED - part, size - part)
        return gf_ref[pl.ds(pl.multiple_of(mine * n, FAMILY) + base + low, high - low), :].astype(bf16)

    for col in range(COLOURS):
        low, high = col * UNIT, (col + 1) * UNIT
        for a, b in ((low, min(high, part)), (max(low, part), high)):
            if a < b:
                wv_ref[(*here, col, slice(a - low, b - low))] = own_rows(a, b)

    outs = []

    def hand_on(col, rel):
        axis = ORDER[col][0]
        q = _near(at[axis] + rel)
        src, dst = wv_ref.at[(*_where(axis, q), col)], out_ref.at[(*_where(axis, q), core, col)]
        n = col * RING + rel
        copy = remote(src, dst, od_send.at[n], od_recv.at[n], partner)
        copy.start()
        local = pltpu.make_async_copy(src, dst, ol_sem.at[n])
        local.start()
        outs.append((copy, local))

    def gather_phase(phase, chunk, done):
        def start(col, d, slot, rel, h):
            copy = hop(BOTH)(phase, col, d, slot, chunk(col, rel, h), chunk(col, rel, h))
            copy.start()
            pending.append(copy)

        def arrived(col, d, slot, rel, h):
            hop(BOTH)(phase, col, d, slot, chunk(col, rel, h), chunk(col, rel, h)).wait_recv()

        for slot in range(BOTH):
            for col in range(COLOURS):
                for d in range(BOTH):
                    start(col, d, slot, 0, d if slot == 0 else 1 - d)
        for col in range(COLOURS):
            done(col, 0)
        for col in range(COLOURS):
            for d, rel in BEHIND:
                arrived(col, d, 0, rel, d)
                start(col, d, BOTH, rel, d)
        for col in range(COLOURS):
            for d, rel in BEHIND:
                arrived(col, d, 1, rel, 1 - d)
                done(col, rel)
        for col in range(COLOURS):
            for d in range(BOTH):
                arrived(col, d, BOTH, BOTH, d)
            done(col, BOTH)

    cut = UNIT // BOTH

    def last_chunk(col, rel, h):
        spot = list(at)
        spot[ORDER[col][BOTH]] = _near(at[ORDER[col][BOTH]] + rel)
        return wv_ref.at[(*spot, col, pl.ds(h * cut, cut))]

    def middle_chunk(col, rel, h):
        spot = list(at)
        spot[ORDER[col][1]] = _near(at[ORDER[col][1]] + rel)
        spot[ORDER[col][BOTH]] = _half(h)
        return wv_ref.at[(*spot, col)]

    def whole_chunk(col, rel, h):
        axis = ORDER[col][0]
        return wv_ref.at[(*_where(axis, _near(at[axis] + rel), _half(h)), col)]

    gather_phase(BOTH, last_chunk, lambda col, rel: None)
    gather_phase(1, middle_chunk, lambda col, rel: None)
    gather_phase(0, whole_chunk, hand_on)

    gated_sum.drain()
    other_sum.drain()
    for copy in swaps + pending:
        copy.wait_send()
    for copy, local in outs:
        copy.wait_send()
        local.wait()
    for n, (col, rel) in enumerate((c, r) for c in range(COLOURS) for r in range(RING)):
        axis = ORDER[col][0]
        dst = out_ref.at[(*_where(axis, _near(at[axis] + rel)), 1 - core, col)]
        remote(dst, dst, od_send.at[n], od_recv.at[n], partner).wait_recv()


def sum_step_gather(g, weights, m, v, back):
    vmem, dma = pltpu.VMEM, pltpu.SemaphoreType.DMA
    hbm, local = pl.BlockSpec(memory_space=pl.ANY), pl.BlockSpec(memory_space=vmem)
    cube, sides = (RING, RING, RING), (COLOURS, BOTH, COLOURS)
    scratch = [vmem((SHAPE[name][0] // GROUPS, SHAPE[name][1]), bf16) for name in NAMES]
    for unit in UNITS:
        row = (unit, LANES)
        scratch += [vmem((*sides, BOTH, RING, *row), bf16), vmem((COLOURS, RING, RING, *row), f32), vmem((*sides, BOTH, *row), bf16), vmem((COLOURS, COLOURS, RING, *row), bf16),
                    vmem((COLOURS, RING, *row), f32), vmem((*sides, unit // BOTH, LANES), bf16), vmem((COLOURS, COLOURS, *row), bf16)]
    own, tile, head = (OWN, LANES), (FAMILY, LANES), (TOKENS, HEAD)
    scratch += [vmem((*cube, COLOURS, UNITS[0], LANES), bf16), vmem((*cube, COLOURS, UNITS[0], LANES), bf16), vmem((*cube, BOTH, COLOURS, UNITS[1], LANES), bf16),
                vmem((*cube, COLOURS, UNITS[1], LANES), bf16), vmem((FAMILY, COLOURS * UNITS[0], LANES), bf16), vmem((FAMILY, COLOURS * UNITS[1], LANES), bf16), vmem((FLAT, LANES), f32),
                vmem((RING, 200, LANES), f32), vmem(own, f32), vmem(own, f32), vmem((FAMILY, *own), bf16), vmem((*cube, COLOURS, UNIT, LANES), bf16)]
    scratch += [vmem((n, *tile), f32) for n in (COLOURS, COLOURS, COLOURS, MATRICES)]
    scratch += [vmem((TOKENS, (HEADS + BOTH) * HEAD), bf16), vmem((HEAD, HEADS * BACK), f32), vmem(head, f32), vmem(head, f32), vmem((HEADS, BACK, HEAD), bf16)]
    scratch += [dma((n,)) for n in (162, 162, 24, 24, CHUNKS, MATRICES, 13, 13, 18, 18, CHUNKS, CHUNKS, CHUNKS, CHUNKS, CHUNKS)]
    return pl.pallas_call(
        _comm,
        out_shape=[jax.ShapeDtypeStruct((*cube, BOTH, COLOURS, UNIT, LANES), bf16), jax.ShapeDtypeStruct(own, f32)],
        in_specs=[hbm] * FAMILY + [local] * 23,
        out_specs=[hbm, local],
        scratch_shapes=scratch,
        compiler_params=pltpu.CompilerParams(collective_id=0, has_side_effects=True, vmem_limit_bytes=67043328),
    )(g, *[w.reshape(GROUPS, w.shape[1] // GROUPS, w.shape[BOTH]) for w in weights], *_rows(m), *_rows(v), *back)


PER = RING


def _finish(flat_ref, gq_ref, *rest):
    m_refs, v_refs, w_refs, mo_refs, vo_refs = (rest[i : i + MATRICES] for i in range(0, 35, MATRICES))

    @pl.when(pl.program_id(0) == 0)
    def _():
        for k, (_, blocks, _, own, first) in enumerate(TABLE):
            for j in range(blocks):
                at = _at(k, _lanes(j))
                g = gq_ref[first + j * own : first + (j + 1) * own, :]
                mo_refs[k][at] = 0.9 * m_refs[k][at] + 0.1 * g
                vo_refs[k][at] = 0.95 * v_refs[k][at] + 0.05 * g * g

    for k, (_, blocks, rows, _, _) in enumerate(TABLE):
        lengths = (COLOURS * UNITS[1], GATED) if k < RING else (COLOURS * UNITS[0], 0)
        for j in range(blocks):
            row, to = _flat(k) + j * rows - lengths[1], 0
            while to < rows:
                n, low = row // lengths[0], row % lengths[0]
                some = min(lengths[0] - low, rows - to)
                low += n * COLOURS * UNIT + (COLOURS * UNITS[0] if k < RING else 0)
                for i in range(PER):
                    w_refs[k][0, i * rows + to : i * rows + to + some, _lanes(j)] = flat_ref[i, low : low + some, :]
                row, to = row + some, to + some


def finish(flat, gq, m, v):
    whole = pl.BlockSpec(memory_space=pltpu.VMEM)
    old = [*_rows(m), *_rows(v)]
    shapes = [(1, *SHAPE[name]) for name in NAMES]
    out = pl.pallas_call(
        _finish,
        grid=(GROUPS // PER,),
        out_shape=[jax.ShapeDtypeStruct(shape, jnp.bfloat16) for shape in shapes] + [jax.ShapeDtypeStruct(a.shape, a.dtype) for a in old],
        in_specs=[pl.BlockSpec((PER, FLAT, LANES), lambda i: (i, 0, 0)), whole] + [whole] * 14,
        out_specs=[pl.BlockSpec((1, shape[1] // GROUPS * PER, shape[BOTH]), lambda i: (0, i, 0)) for shape in shapes] + [whole] * 14,
        compiler_params=pltpu.CompilerParams(vmem_limit_bytes=VMEM),
    )(flat.reshape(GROUPS, FLAT, LANES), gq, *old)
    moments = [new.reshape(1, *new.shape) if new.ndim == BOTH else new.transpose(1, 0, BOTH) for new in out[MATRICES:]]
    return (*out[:MATRICES], *moments)


def solution(mesh):
    def step(x, dy, *arrays):
        weights, m, v = (arrays[i : i + MATRICES] for i in (0, MATRICES, 14))
        w = dict(zip(NAMES, weights, strict=True))
        plain = {name: w[name][0] for name in ("wq", "wk", "wv", "wo")}
        a, q, k, value, ot, lse, h = attend(x[0], plain)
        g, dh = gated(h, dy[0], w)
        back = (dh, a, q, k, value, ot, lse, _angles(), plain["wo"])
        flat, gq = sum_step_gather(g.reshape(RING, RING, RING, 2, COLOURS, UNITS[0], LANES), weights, m, v, back)
        return finish(flat, gq, m, v)

    states, all_of, cut = P(("rep", "dp")), P(), P(None, "dp")
    return jax.shard_map(
        step,
        mesh=mesh,
        in_specs=(states, states) + (all_of,) * MATRICES + (cut,) * 14,
        out_specs=(P("rep"),) * MATRICES + (P("rep", "dp"),) * 14,
        check_vma=False,
    )
```

```python
import functools

import jax
import jax.numpy as jnp
import numpy as np
from jax import lax
from jax.experimental import pallas as pl
from jax.experimental.pallas import tpu as pltpu
from jax.sharding import PartitionSpec as P

NEG = -1e30
HIDDEN = 2 * NEG
LOG2E = 1.4426950408889634
VMEM = 56 * 2**20
NAMES = ("wq", "wk", "wv", "wo", "w_gate", "w_up", "w_down")
TOKENS, D, HEADS, HEAD, FF = 1024, 640, 8, 128, 3200
SCALE = HEAD**-0.5
E = SCALE * LOG2E
THETA = 10000
f32, bf16 = jnp.float32, jnp.bfloat16


def _dot(a, b, ca=1, cb=0):
    return lax.dot_general(a, b, (((ca,), (cb,)), ((), ())), preferred_element_type=f32)


def _dot_t(a, b):
    return _dot(a, b, 1, 1)


def _lanes(k):
    return slice(k * 128, (k + 1) * 128)


def _scale(wide):
    return lax.rsqrt(jnp.mean(wide * wide, -1, keepdims=True) + 1e-6)


def _normed(wide):
    return wide * _scale(wide)


HALF = HEAD // 2


def _angles():
    angle = np.arange(TOKENS, dtype=np.float32)[:, None] * np.float32(THETA) ** (-np.arange(HALF, dtype=np.float32) / np.float32(HALF))
    return np.concatenate([np.cos(angle), np.sin(angle)], 1).astype(np.float32)


def _spread(angles):
    other = pltpu.roll(angles, HALF, 1)
    low = lax.broadcasted_iota(jnp.int32, angles.shape, 1) < HALF
    return jnp.where(low, angles, other), jnp.where(low, -other, angles)
LANES, GROUPS = 128, 16
BOTH, COLOURS, RING, FAMILY, MATRICES, CHUNKS = 2, 3, 4, 8, 7, 12


BQ, BK = 1024, 256


def _attend(x_ref, angle_ref, wq_ref, wk_ref, wv_ref, wo_ref, a_ref, q_ref, k_ref, v_ref, ot_ref, lse_ref, h_ref, ks, vts, top_s, mix_s):
    i = pl.program_id(0)
    a = _normed(x_ref[...].astype(f32)).astype(bf16)
    a_ref[...] = a
    cos, sin = _spread(angle_ref[...])

    def turned(t):
        t = t.astype(bf16).astype(f32)
        return (t * cos + pltpu.roll(t, HALF, 1) * sin).astype(bf16)

    k = turned(_dot(a, wk_ref[...]))
    v = _dot(a, wv_ref[...]).astype(bf16)
    k_ref[...] = k
    v_ref[...] = v
    here = pl.ds(pl.multiple_of(i * BQ, BQ), BQ)
    ks[here, :] = k
    vts[:HEAD, here] = v.T
    vts[HEAD:, here] = jnp.ones((8, BQ), bf16)
    q = _dot(a, wq_ref[...])
    for n in range(HEADS):
        q_ref[n] = turned(q[:, _lanes(n)])
    top_s[...] = jnp.full(top_s.shape, NEG, f32)
    mix_s[...] = jnp.zeros(mix_s.shape, f32)

    def block(j, low, masked):
        keys = pl.ds(pl.multiple_of(j * BK, BK), BK)
        scores = [_dot_t(ks[keys, :], q_ref[n, low:, :]) for n in range(HEADS)]
        if masked:
            hidden = lax.broadcasted_iota(jnp.int32, (BK, BQ - low), 1) < lax.broadcasted_iota(jnp.int32, (BK, BQ - low), 0)
        values = vts[:, keys]
        weights, keeps = [], []
        for n, s in enumerate(scores):
            if masked:
                s = jnp.where(hidden, HIDDEN, s)
            old = top_s[n : n + 1, low:]
            top = jnp.maximum(old, s.max(axis=0, keepdims=True))
            top_s[n : n + 1, low:] = top
            weights.append(jnp.exp2((s - top) * E).astype(bf16))
            keeps.append(jnp.exp2((old - top) * E))
        for n, (p, keep) in enumerate(zip(weights, keeps)):
            mix_s[n, :, low:] = mix_s[n, :, low:] * keep + _dot(values, p)

    per = BQ // BK
    lax.fori_loop(0, per * i, lambda j, _: block(j, 0, False), None)
    for n in range(per):
        block(per * i + n, n * BK, True)
    outs = []
    for n in range(HEADS):
        total = mix_s[n, HEAD : HEAD + 1, :]
        out = (mix_s[n, :HEAD, :] * (1 / total)).astype(bf16)
        ot_ref[_lanes(n), :] = out
        outs.append(out.T)
        lse_ref[n : n + 1, :] = top_s[n : n + 1, :] * SCALE + jnp.log(total)
    more = _dot(jnp.concatenate(outs, axis=1), wo_ref[...]).astype(bf16)
    h_ref[...] = (x_ref[...].astype(f32) + more.astype(f32)).astype(bf16)


def attend(x, w):
    whole = pl.BlockSpec(memory_space=pltpu.VMEM)
    rows = lambda width: pl.BlockSpec((BQ, width), lambda i: (i, 0))
    columns = lambda height: pl.BlockSpec((height, BQ), lambda i: (0, i))
    shape = jax.ShapeDtypeStruct
    return pl.pallas_call(
        _attend,
        grid=(TOKENS // BQ,),
        in_specs=[rows(D), rows(HEAD)] + [whole] * 4,
        out_specs=[rows(D), pl.BlockSpec((HEADS, BQ, HEAD), lambda i: (0, i, 0)), rows(HEAD), rows(HEAD), columns(HEADS * HEAD), columns(HEADS), rows(D)],
        out_shape=[shape((TOKENS, D), bf16), shape((HEADS, TOKENS, HEAD), bf16), shape((TOKENS, HEAD), bf16), shape((TOKENS, HEAD), bf16),
                   shape((HEADS * HEAD, TOKENS), bf16), shape((HEADS, TOKENS), f32), shape((TOKENS, D), bf16)],
        scratch_shapes=[pltpu.VMEM((TOKENS, HEAD), bf16), pltpu.VMEM((HEAD + 8, TOKENS), bf16), pltpu.VMEM((HEADS, BQ), f32),
                        pltpu.VMEM((HEADS, HEAD + 8, BQ), f32)],
        compiler_params=pltpu.CompilerParams(dimension_semantics=("arbitrary",), vmem_limit_bytes=VMEM),
    )(x, _angles(), *[w[name] for name in ("wq", "wk", "wv", "wo")])


BF = 256
LAST = FF // BF
CHUNK = 512


def _gated(h_ref, dy_ref, wg_ref, wu_ref, wd_ref, g_ref, dh_ref, b_s, bt_s, dyt_s, acc_s, hid_s, dg_s, du_s, stage, down_s, zero_s, sem, end_sem):
    j = pl.program_id(0)
    slot = lax.rem(j, 2)
    firsts = [TABLE[NAMES.index(name)][0] for name in ("w_gate", "w_up", "w_down")]
    rows = D // GROUPS
    ends = 3 * FF * D // GROUPS // LANES

    def put(n, at, size):
        where = pl.ds(pl.multiple_of(firsts[n] + at * (rows * BF // LANES), 8), size)
        return pltpu.make_async_copy(stage.at[n, slot, :, pl.ds(0, size)], g_ref.at[:, where], sem.at[n, slot])

    @pl.when(j == 0)
    def _():
        b = _normed(h_ref[...].astype(f32)).astype(bf16)
        b_s[...] = b
        bt_s[...] = b.T
        dyt_s[...] = dy_ref[...].T
        acc_s[...] = jnp.zeros(acc_s.shape, f32)
        zero_s[...] = jnp.zeros(zero_s.shape, bf16)
        pltpu.make_async_copy(zero_s, g_ref.at[:, pl.ds(ends, GATED - ends)], end_sem.at[0]).start()

    left = FF - j * BF
    inside = lax.broadcasted_iota(jnp.int32, (D, BF), 1) < left
    wg, wu = (jnp.where(inside, ref[0], jnp.zeros((), bf16)) for ref in (wg_ref, wu_ref))
    wd = jnp.where(lax.broadcasted_iota(jnp.int32, (BF, D), 0) < left, wd_ref[0], jnp.zeros((), bf16))
    for at in range(0, TOKENS, CHUNK):
        here = slice(at, at + CHUNK)
        gate, up = _dot(b_s[here, :], wg), _dot(b_s[here, :], wu)
        dhid = _dot_t(dy_ref[here, :], wd).astype(bf16).astype(f32)
        share = 1 / (1 + jnp.exp(-gate))
        silu = gate * share
        hid_s[here, :] = (silu * up).astype(bf16)
        dgate = (dhid * up * (share * (1 + gate * (1 - share)))).astype(bf16)
        dup = (dhid * silu).astype(bf16)
        dg_s[here, :] = dgate
        du_s[here, :] = dup
        acc_s[here, :] += _dot_t(dgate, wg) + _dot_t(dup, wu)

    @pl.when(j >= 2)
    def _():
        for n in range(2):
            put(n, j - 2, rows * BF // LANES).wait()

    for n, one in enumerate((dg_s, du_s)):
        term = _dot(bt_s[...], one[...])
        for k in range(BF // LANES):
            stage[n, slot, :, k * rows : (k + 1) * rows, :] = term[:, _lanes(k)].reshape(GROUPS, rows, LANES).astype(bf16)
    term = _dot(dyt_s[...], hid_s[...]).T
    for k in range(D // LANES):
        down_s[k, pl.ds(pl.multiple_of(j * BF, BF), BF), :] = term[:, _lanes(k)].astype(bf16)

    @pl.when(j < LAST)
    def _():
        for n in range(2):
            put(n, j, rows * BF // LANES).start()

    @pl.when(j == LAST)
    def _():
        for n in range(2):
            put(n, j, rows * (FF % BF) // LANES).start()
        per = FF // GROUPS
        for k in range(D // LANES):
            for n in range(GROUPS):
                pltpu.make_async_copy(down_s.at[k, pl.ds(n * per, per)], g_ref.at[n, pl.ds(firsts[2] + k * per, per)], end_sem.at[1]).start()
        for at in range(0, TOKENS, CHUNK):
            here = slice(at, at + CHUNK)
            db = acc_s[here, :].astype(bf16).astype(f32)
            h = h_ref[here, :].astype(f32)
            s = _scale(h)
            through = db * s - h * (s * s * s * jnp.mean(db * h, -1, keepdims=True))
            dh_ref[here, :] = (dy_ref[here, :].astype(f32) + through.astype(bf16).astype(f32)).astype(bf16)
        for n in range(2):
            put(n, j, rows * (FF % BF) // LANES).wait()
            pltpu.make_async_copy(stage.at[n, 1 - slot], stage.at[n, 1 - slot], sem.at[n, 1 - slot]).wait()
        pltpu.make_async_copy(zero_s, g_ref.at[:, pl.ds(ends, GATED - ends)], end_sem.at[0]).wait()
        whole = g_ref.at[:, pl.ds(firsts[2], ends - firsts[2])]
        pltpu.make_async_copy(whole, whole, end_sem.at[1]).wait()


def gated(h, dy, w):
    vmem = pltpu.VMEM
    whole = pl.BlockSpec(memory_space=vmem)
    across = pl.BlockSpec((1, D, BF), lambda j: (0, 0, j))
    pad = GATED - 3 * FF * D // GROUPS // LANES
    return pl.pallas_call(
        _gated,
        grid=(LAST + 1,),
        in_specs=[whole, whole, across, across, pl.BlockSpec((1, BF, D), lambda j: (0, j, 0))],
        out_specs=[pl.BlockSpec(memory_space=pl.ANY), whole],
        out_shape=[jax.ShapeDtypeStruct((GROUPS, GATED, LANES), bf16), jax.ShapeDtypeStruct((TOKENS, D), bf16)],
        scratch_shapes=[vmem((TOKENS, D), bf16), vmem((D, TOKENS), bf16), vmem((D, TOKENS), bf16), vmem((TOKENS, D), f32),
                        vmem((TOKENS, BF), bf16), vmem((TOKENS, BF), bf16), vmem((TOKENS, BF), bf16),
                        vmem((2, 2, GROUPS, D // GROUPS * BF // LANES, LANES), bf16), vmem((D // LANES, (LAST + 1) * BF, LANES), bf16), vmem((GROUPS, pad, LANES), bf16),
                        pltpu.SemaphoreType.DMA((2, 2)), pltpu.SemaphoreType.DMA((2,))],
        compiler_params=pltpu.CompilerParams(dimension_semantics=("arbitrary",), vmem_limit_bytes=VMEM),
    )(h, dy, *[w[name] for name in ("w_gate", "w_up", "w_down")])


BACK = 256


def _back_step(i, dh_ref, q_ref, k_ref, v_ref, ot_ref, lse_ref, angle_ref, wo_ref, dqkv_s, dqt_s, dk_s, dv_s, do_s):
    here = pl.ds(pl.multiple_of(i * BACK, BACK), BACK)
    dqt_s[...] = jnp.zeros(dqt_s.shape, f32)
    dh, wo = dh_ref[here, :], wo_ref[...]
    dot = _dot_t(wo, dh).astype(bf16).astype(f32) * ot_ref[:, here].astype(f32)
    delta = [dot[_lanes(n), :].sum(axis=0, keepdims=True) for n in range(HEADS)]
    dout = _dot_t(dh, wo).astype(bf16)
    for n in range(HEADS):
        do_s[n] = dout[:, _lanes(n)]
    pairs = range(0, HEADS, 2)
    beside = lambda rows, n: jnp.concatenate([rows[n], rows[n + 1]], axis=1)
    lses = [lse_ref[n : n + 1, here] * LOG2E for n in range(HEADS)]

    def block(j, masked):
        keys = pl.ds(pl.multiple_of(j * BACK, BACK), BACK)
        k, v = k_ref[keys, :], v_ref[keys, :]
        kt = k.T
        if masked:
            place = lax.broadcasted_iota(jnp.int32, (BACK, 2 * BACK), 1)
            hidden = jnp.where(place < BACK, place, place - BACK) < lax.broadcasted_iota(jnp.int32, (BACK, 2 * BACK), 0)
        for some in (pairs[:2], pairs[2:]):
            qs = [q_ref[n : n + 2, here, :].reshape(2 * BACK, HEAD) for n in some]
            dos = [do_s[n : n + 2].reshape(2 * BACK, HEAD) for n in some]
            scores = [_dot_t(k, q) for q in qs]
            dps = [_dot_t(v, one) for one in dos]
            for n, q, do, score, dp in zip(some, qs, dos, scores, dps):
                p = jnp.exp2(score * E - beside(lses, n))
                if masked:
                    p = jnp.where(hidden, 0.0, p)
                ds = (p * (dp - beside(delta, n))).astype(bf16)
                dv_s[keys, :] += _dot(p.astype(bf16), do)
                dk_s[keys, :] += _dot(ds, q)
                dqt_s[:, n * BACK : (n + 2) * BACK] += _dot(kt, ds)

    lax.fori_loop(0, i, lambda j, _: block(j, False), None)
    block(i, True)
    both = angle_ref[here, :].T
    cost, sint = both[:HALF], both[HALF:]
    for n in range(HEADS):
        t = (dqt_s[:, n * BACK : (n + 1) * BACK] * SCALE).astype(bf16).astype(f32)
        one, two = t[:HALF], t[HALF:]
        t = jnp.concatenate([one * cost + two * sint, two * cost - one * sint], axis=0)
        dqkv_s[here, _lanes(n)] = t.astype(bf16).T


def _back_put(put, term, first):
    rows = term.shape[0] // GROUPS
    for k in range(term.shape[1] // LANES):
        put(first + k * rows, term[:, _lanes(k)].reshape(GROUPS, rows, LANES))


def _back_qkv(put, a_ref, angle_ref, dqkv_s, dk_s, dv_s):
    wide = HEADS * HEAD
    cos, sin = _spread(angle_ref[...])
    t = (dk_s[...] * SCALE).astype(bf16).astype(f32)
    dqkv_s[:, wide : wide + HEAD] = (t * cos - pltpu.roll(t, HALF, 1) * sin).astype(bf16)
    dqkv_s[:, wide + HEAD :] = dv_s[...].astype(bf16)
    _back_put(put, _dot(a_ref[...].T, dqkv_s[...]), TABLE[0][0])


MESH, ALL = pl.DeviceIdType.MESH, slice(None)
SHAPE = {"wq": (640, 1024), "wk": (640, 128), "wv": (640, 128), "wo": (1024, 640), "w_gate": (640, 3200), "w_up": (640, 3200), "w_down": (3200, 640)}
UNIT = 160
UNITS = (LANES, 32)
GATED, OTHERS = 24 * UNITS[0], 24 * UNITS[1]
FLAT = GATED + OTHERS
ORDER = ((0, 1, 2), (1, 2, 0), (2, 0, 1))
AHEAD, BEHIND = ((0, 1), (1, COLOURS)), ((0, COLOURS), (1, 1))
WAY = (2, 1, COLOURS, 0)


def _table():
    table, flat, mine = [], 0, 0
    for name in NAMES:
        rows, cols = SHAPE[name]
        flat = 0 if name == "w_gate" else flat
        blocks, group, own = cols // LANES, rows // GROUPS, rows // LANES
        table.append((flat, blocks, group, own, mine))
        flat += blocks * group
        mine += blocks * own
    return tuple(table)


TABLE, OWN = _table(), COLOURS * UNIT


def _flat(k):
    return TABLE[k][0] + (GATED if k < RING else 0)


def _at(k, lanes):
    return (ALL, lanes) if TABLE[k][COLOURS] % FAMILY == 0 else (ALL, 0, lanes)


def _rows(moments):
    return [one[0] if one.shape[1] % FAMILY == 0 else one.transpose(1, 0, BOTH) for one in moments]


def _near(q):
    return lax.rem(q, RING)


def _where(axis, q, first=ALL):
    return ((q, first, ALL), (first, q, ALL), (first, ALL, q))[axis]


def _place(axis, q, a, b):
    return ((q, a, b), (a, q, b), (a, b, q))[axis]


def _half(h):
    return pl.ds(BOTH * h, BOTH)


class _Sum:
    def __init__(self, unit, at, hop, swaps, own, other, boxes, final):
        self.unit, self.at, self.hop, self.swaps, self.own, self.other, self.last = unit, at, hop, swaps, own, other, final
        self.ra, self.f, self.rb, self.sb, self.f2, self.rc, self.sc = boxes
        self.sent, self.cut = [], unit // BOTH

    def spot(self, col, rel, h, u):
        axis = ORDER[col][0]
        return _place(axis, _near(self.at[axis] + rel), BOTH * h + lax.div(u, RING), lax.rem(u, RING))

    def chunk(self, phase, col, rel):
        return _near(self.at[ORDER[col][phase]] + rel)

    def rows(self, h):
        return slice(h * self.cut, (h + 1) * self.cut)

    def term(self, phase, col, rel, h, u):
        if phase == 0:
            here = self.spot(col, rel, h, u)
            return self.own(here, col)[...].astype(f32) + self.other[(*here, col)].astype(f32)
        if phase == 1:
            return self.f[col, self.chunk(1, col, rel), BOTH * h + u]
        return self.f2[col, self.chunk(BOTH, col, rel), self.rows(h)]

    def source(self, phase, col, rel, h):
        if phase == 0:
            axis = ORDER[col][0]
            return self.own(_where(axis, self.chunk(0, col, rel), _half(h)), col)
        return self.sb.at[col, rel - 1, _half(h)] if phase == 1 else self.sc.at[col, rel - 1, self.rows(h)]

    def store(self, phase, col, rel, h, u, x):
        x = x.astype(bf16)
        if phase == 0:
            self.own(self.spot(col, rel, h, u), col)[...] = x
        elif phase == 1:
            self.sb[col, rel - 1, BOTH * h + u] = x
        else:
            self.sc[col, rel - 1, self.rows(h)] = x

    def inbox(self, phase, col, d, slot):
        return (self.ra, self.rb, self.rc)[phase].at[col, d, slot]

    def value(self, phase, col, d, slot, u):
        box = self.inbox(phase, col, d, slot)
        box = (box.at[lax.div(u, RING), lax.rem(u, RING)] if phase == 0 else box.at[u] if phase == 1 else box)
        return box[...].astype(f32)

    def final(self, phase, col, h, u, x):
        if phase == 0:
            a, b = BOTH * h + lax.div(u, RING), lax.rem(u, RING)
            self.f[(col, b, a) if col == 1 else (col, a, b)] = x
        elif phase == 1:
            self.f2[col, BOTH * h + u] = x
        else:
            self.last(col, h, x)

    def each(self, phase, body):
        units = (FAMILY, BOTH, 1)[phase]
        if units == 1:
            body(0)
        else:
            lax.fori_loop(0, units, lambda u, _: body(u), None)

    def copy(self, phase, col, d, slot, rel, h, by=None):
        return self.hop(phase, col, d, slot, self.source(phase, col, rel, h), self.inbox(phase, col, d, slot), by)

    def start(self, *what):
        self.copy(*what).start()
        self.sent.append(what)

    def drain(self):
        for what in self.sent:
            self.copy(*what).wait_send()

    def arrived(self, phase, col, d, slot):
        box = self.inbox(phase, col, d, slot)
        self.hop(phase, col, d, slot, box, box).wait_recv()

    def ready(self, phase, col, rel):
        if phase == 0:
            for wait in self.swaps[col, rel]:
                wait()

    def far(self, phase):
        for col in range(COLOURS):
            self.ready(phase, col, BOTH)
            for d in range(BOTH):
                self.each(phase, lambda u: self.store(phase, col, BOTH, d, u, self.term(phase, col, BOTH, d, u)))
                self.start(phase, col, d, 0, BOTH, d)

    def straight(self, phase):
        for col in range(COLOURS):
            for d, rel in AHEAD:
                self.ready(phase, col, rel)
                self.each(phase, lambda u: self.store(phase, col, rel, 1 - d, u, self.term(phase, col, rel, 1 - d, u)))
                self.start(phase, col, d, 1, rel, 1 - d)

    def through(self, phase):
        for col in range(COLOURS):
            for d, rel in AHEAD:
                self.arrived(phase, col, d, 0)
                self.each(phase, lambda u: self.store(phase, col, rel, d, u, self.term(phase, col, rel, d, u) + self.value(phase, col, d, 0, u)))
                self.start(phase, col, d, BOTH, rel, d)

    def direct(self, phase):
        for rel in WAY[:COLOURS]:
            for col in range(COLOURS):
                for h in range(BOTH):
                    self.each(phase, lambda u: self.store(phase, col, rel, h, u, self.term(phase, col, rel, h, u)))
                    self.start(phase, col, h, rel - 1, rel, h, rel)

    def close_direct(self, phase):
        for col in range(COLOURS):
            for h in range(BOTH):
                for slot in range(COLOURS):
                    self.arrived(phase, col, h, slot)
                self.each(phase, lambda u: self.final(phase, col, h, u, sum((self.value(phase, col, h, slot, u) for slot in range(COLOURS)),
                                                                            self.term(phase, col, 0, h, u))))

    def close(self, phase):
        for col in range(COLOURS):
            self.ready(phase, col, 0)
            for d in range(BOTH):
                for slot in (1, BOTH):
                    self.arrived(phase, col, d, slot)
            for h in range(BOTH):
                self.each(phase, lambda u: self.final(phase, col, h, u, self.term(phase, col, 0, h, u) + self.value(phase, col, 0, BOTH - h, u)
                                                      + self.value(phase, col, 1, 1 + h, u)))


def _comm(g_ref, *rest):
    w_refs, rest = rest[:MATRICES], rest[MATRICES:]
    m_refs, v_refs, rest = rest[:MATRICES], rest[MATRICES:14], rest[14:]
    dh_ref, a_ref, q_ref, k_ref, v_ref, ot_ref, lse_ref, angle_ref, wo_ref, out_ref, gq_ref, *rest = rest
    wn_refs, rest = rest[:MATRICES], rest[MATRICES:]
    boxes, rest = (rest[:MATRICES], rest[MATRICES:14]), rest[14:]
    (s_ref, r0_ref, mine_ref, r1_ref, ga_ref, gb_ref, gf_ref, wt_ref, ow_ref, ou_ref, wb_ref, wv_ref, ps_ref, px_ref, py_ref, p8_ref,
     dqkv_s, dqt_s, dk_s, dv_s, do_s, ring_send, ring_recv, d2d_send, d2d_recv, load_sem, w_sem, ps_send, ps_recv, zs_send, zs_recv,
     zd_send, zd_recv, od_send, od_recv, ol_sem) = rest
    me = lax.axis_index("dp")
    core = lax.rem(me, BOTH)
    at = [lax.rem(lax.div(me, 32), RING), lax.rem(lax.div(me, FAMILY), RING), lax.rem(lax.div(me, BOTH), RING)]
    group = lax.div(me, FAMILY)
    mine = lax.rem(me, FAMILY)

    def device(axis, by):
        return me + (lax.rem(at[axis] + by, RING) - at[axis]) * (32, FAMILY, BOTH)[axis]

    partner = me + 1 - BOTH * core
    family = [group * FAMILY + lax.rem(mine + k, FAMILY) for k in range(1, FAMILY)]
    friends = [device(axis, by) for axis in (0, 1) for by in (1, BOTH, COLOURS)] + family
    barrier = pltpu.get_barrier_semaphore()
    for one in friends:
        pl.semaphore_signal(barrier, inc=1, device_id={"dp": one}, device_id_type=MESH)

    def remote(src, dst, send, recv, to):
        return pltpu.make_async_remote_copy(src_ref=src, dst_ref=dst, send_sem=send, recv_sem=recv, device_id={"dp": to}, device_id_type=MESH)

    def hop(base):
        def make(phase, col, d, slot, src, dst, by=None):
            n = (((base * COLOURS + phase) * COLOURS + col) * BOTH + d) * COLOURS + slot
            return remote(src, dst, ring_send.at[n], ring_recv.at[n], device(ORDER[col][phase], by or AHEAD[d][1]))

        return make

    chunks = [(n, col, rel, _where(ORDER[col][0], _near(at[ORDER[col][0]] + rel))) for n, (rel, col) in enumerate((r, c) for r in WAY for c in range(COLOURS))]
    loads, swaps = {}, []
    for n, col, rel, here in chunks:
        loads[n] = pltpu.make_async_copy(g_ref.at[(*here, core, col)], s_ref.at[(*here, col)], load_sem.at[n])
        loads[n].start()
    for k in range(MATRICES):
        pltpu.make_async_copy(w_refs[k].at[group], wn_refs[k], w_sem.at[k]).start()
    pl.semaphore_wait(barrier, len(friends))
    first = {}
    for n, col, rel, here in chunks:
        copy = remote(g_ref.at[(*here, 1 - core, col)], r0_ref.at[(*here, col)], d2d_send.at[n], d2d_recv.at[n], partner)
        copy.start()
        swaps.append(copy)
        first[col, rel] = (loads[n].wait, copy.wait_recv)

    pending, squares = [], []

    class Share:
        def __init__(self, number, box):
            self.number, self.box, self.cut = number, box, box.shape[1] // BOTH

        def block(self, rel):
            return self.box.at[BOTH * _near(at[BOTH] + rel) + core]

        def hop(self, d, slot, rel, h):
            n = (self.number * BOTH + d) * COLOURS + slot
            half = self.block(rel).at[pl.ds(h * self.cut, self.cut)]
            return remote(half, half, zs_send.at[n], zs_recv.at[n], device(BOTH, 1 if d == 0 else COLOURS))

        def over(self, rel, whose):
            n = self.number * RING + rel
            block = self.box.at[BOTH * _near(at[BOTH] + rel) + whose]
            return remote(block, block, zd_send.at[n], zd_recv.at[n], partner)

        def go(self, copy):
            copy.start()
            pending.append(copy)

        def start(self):
            for slot in range(BOTH):
                for d in range(BOTH):
                    self.go(self.hop(d, slot, 0, d if slot == 0 else 1 - d))
            self.go(self.over(0, core))

        def forward(self):
            for d, rel in BEHIND:
                self.hop(d, 0, rel, d).wait_recv()
                self.go(self.hop(d, BOTH, rel, d))

        def cross(self):
            for d, rel in BEHIND:
                self.hop(d, 1, rel, 1 - d).wait_recv()
                self.go(self.over(rel, core))
            for d in range(BOTH):
                self.hop(d, BOTH, BOTH, d).wait_recv()
            self.go(self.over(BOTH, core))

        def finish(self):
            for rel in range(RING):
                self.over(rel, 1 - core).wait_recv()

    gated_share, other_share, new_share = Share(0, ga_ref), Share(1, gb_ref), Share(BOTH, wb_ref)

    def final(box, unit):
        def put(col, h, x):
            x = x.astype(bf16)
            row = col * unit + h * (unit // BOTH)
            box[mine, row : row + unit // BOTH, :] = x
            x = x.astype(f32)
            squares.append(jnp.sum((x * x).reshape(unit // GROUPS, FAMILY, LANES), axis=0))

        return put

    part = UNITS[0] * COLOURS
    gated_sum = _Sum(UNITS[0], at, hop(0), first, lambda here, col: s_ref.at[(*here, col)], r0_ref, boxes[0], final(ga_ref, UNITS[0]))

    def put(row, x):
        unit, end = UNITS[1], row + x.shape[1]
        begin = row
        while row < end:
            n, low = row // unit, row % unit
            size = min(unit - low, end - row)
            z, c, col = n // 6, n // COLOURS % BOTH, n % COLOURS
            mine_ref[:, :, z, c, col, low : low + size, :] = x[:, row - begin : row - begin + size].reshape(RING, RING, size, LANES).astype(bf16)
            row += size

    def back(i):
        _back_step(i, dh_ref, q_ref, k_ref, v_ref, ot_ref, lse_ref, angle_ref, wo_ref, dqkv_s, dqt_s, dk_s, dv_s, do_s)

    dk_s[...] = jnp.zeros(dk_s.shape, f32)
    dv_s[...] = jnp.zeros(dv_s.shape, f32)
    _back_put(put, _dot(ot_ref[...], dh_ref[...]), TABLE[COLOURS][0])
    put(OTHERS - 48, jnp.zeros((GROUPS, 48, LANES), f32))

    def back_and_sum(i):
        back(i)
        for n, part_of in enumerate((gated_sum.far, gated_sum.straight, gated_sum.through)):
            pl.when(i == n)(functools.partial(part_of, 0))

    lax.fori_loop(0, TOKENS // BACK, lambda i, _: back_and_sum(i), None)
    gated_sum.close(0)
    gated_sum.far(1)
    gated_sum.straight(1)
    _back_qkv(put, a_ref, angle_ref, dqkv_s, dk_s, dv_s)

    second = {}
    for n, col, rel, here in chunks:
        copy = remote(mine_ref.at[(*here, 1 - core, col)], r1_ref.at[(*here, col)], d2d_send.at[CHUNKS + n], d2d_recv.at[CHUNKS + n], partner)
        copy.start()
        swaps.append(copy)
        second[col, rel] = (copy.wait_recv,)
    gated_sum.through(1)
    other_sum = _Sum(UNITS[1], at, hop(1), second, lambda here, col: mine_ref.at[(*here[:COLOURS], core, col)], r1_ref, boxes[1], final(gb_ref, UNITS[1]))
    other_sum.far(0)
    gated_sum.close(1)
    gated_sum.direct(BOTH)
    other_sum.straight(0)
    other_sum.through(0)
    gated_sum.close_direct(BOTH)
    gated_share.start()
    other_sum.close(0)
    other_sum.direct(1)

    for k, (_, blocks, rows, own, begin) in enumerate(TABLE):
        pltpu.make_async_copy(w_refs[k].at[group], wn_refs[k], w_sem.at[k]).wait()
        for j in range(blocks):
            wt_ref[j % RING, :rows, :] = wn_refs[k][:, _lanes(j)].astype(f32)
            ow_ref[begin + j * own : begin + (j + 1) * own, :] = wt_ref[j % RING, pl.ds(mine * own, own), :]
    gated_share.forward()
    other_sum.close_direct(1)
    other_sum.direct(BOTH)
    gated_share.cross()
    other_sum.close_direct(BOTH)

    size = COLOURS * UNIT
    other_share.start()

    def swap_squares(total, which, targets, box):
        n, base = len(targets), COLOURS * which
        ps_ref[which] = total
        for k, to in enumerate(targets):
            copy = remote(ps_ref.at[which], box.at[n - 1 - k], ps_send.at[base + k], ps_recv.at[base + n - 1 - k], to)
            copy.start()
            pending.append(copy)
        for k in range(n):
            remote(box.at[k], box.at[k], ps_send.at[base + k], ps_recv.at[base + k], targets[0]).wait_recv()
            total = total + box[k]
        return total

    total = sum(squares[1:], squares[0])
    total = swap_squares(total, 0, [device(0, by) for by in (1, BOTH, COLOURS)], px_ref)
    other_share.forward()
    total = swap_squares(total, 1, [device(1, by) for by in (1, BOTH, COLOURS)], py_ref)
    other_share.cross()
    gated_share.finish()
    for n in range(FAMILY):
        gf_ref[n * part : (n + 1) * part, :] = ga_ref[n].astype(f32)
    other_share.finish()
    for n in range(FAMILY):
        gf_ref[GATED + n * (size - part) : GATED + (n + 1) * (size - part), :] = gb_ref[n].astype(f32)
    total = swap_squares(total, BOTH, family, p8_ref)
    mean = jnp.sum(total) / float(sum(a * b for a, b in SHAPE.values()))
    factor = jnp.minimum(1.0, 0.5 * lax.rsqrt(jnp.full((FAMILY, LANES), mean, f32) + 1e-30))

    for k, (_, blocks, rows, own, begin) in enumerate(TABLE):
        for j in range(blocks):
            lanes = _lanes(j)
            to = slice(begin + j * own, begin + (j + 1) * own)
            g = gf_ref[pl.ds(_flat(k) + j * rows + mine * own, own), :] * factor[:1]
            w = ow_ref[to, :]
            m = 0.9 * m_refs[k][_at(k, lanes)] + 0.1 * g
            v = 0.95 * v_refs[k][_at(k, lanes)] + 0.05 * g * g
            ou_ref[to, :] = w - 0.02 * (m * lax.rsqrt(v + 1e-8) + 0.1 * w)
            gq_ref[to, :] = g

    wb_ref[mine] = ou_ref[...].astype(bf16)
    new_share.start()
    new_share.forward()
    new_share.cross()
    new_share.finish()

    def gathered(n):
        ou_ref[...] = wb_ref[n].astype(f32)
        for k, (_, blocks, rows, own, begin) in enumerate(TABLE):
            for j in range(blocks):
                gf_ref[pl.ds(_flat(k) + j * rows + n * own, own), :] = ou_ref[begin + j * own : begin + (j + 1) * own, :]

    lax.fori_loop(0, FAMILY, lambda n, _: gathered(n), None)
    here = tuple(at)

    def own_rows(low, high):
        base, n = (0, part) if low < part else (GATED - part, size - part)
        return gf_ref[pl.ds(pl.multiple_of(mine * n, FAMILY) + base + low, high - low), :].astype(bf16)

    for col in range(COLOURS):
        low, high = col * UNIT, (col + 1) * UNIT
        for a, b in ((low, min(high, part)), (max(low, part), high)):
            if a < b:
                wv_ref[(*here, col, slice(a - low, b - low))] = own_rows(a, b)

    outs = []

    def hand_on(col, rel):
        axis = ORDER[col][0]
        q = _near(at[axis] + rel)
        src, dst = wv_ref.at[(*_where(axis, q), col)], out_ref.at[(*_where(axis, q), core, col)]
        n = col * RING + rel
        copy = remote(src, dst, od_send.at[n], od_recv.at[n], partner)
        copy.start()
        local = pltpu.make_async_copy(src, dst, ol_sem.at[n])
        local.start()
        outs.append((copy, local))

    def gather_phase(phase, chunk, done):
        def start(col, d, slot, rel, h):
            copy = hop(BOTH)(phase, col, d, slot, chunk(col, rel, h), chunk(col, rel, h))
            copy.start()
            pending.append(copy)

        def arrived(col, d, slot, rel, h):
            hop(BOTH)(phase, col, d, slot, chunk(col, rel, h), chunk(col, rel, h)).wait_recv()

        for slot in range(BOTH):
            for col in range(COLOURS):
                for d in range(BOTH):
                    start(col, d, slot, 0, d if slot == 0 else 1 - d)
        for col in range(COLOURS):
            done(col, 0)
        for col in range(COLOURS):
            for d, rel in BEHIND:
                arrived(col, d, 0, rel, d)
                start(col, d, BOTH, rel, d)
        for col in range(COLOURS):
            for d, rel in BEHIND:
                arrived(col, d, 1, rel, 1 - d)
                done(col, rel)
        for col in range(COLOURS):
            for d in range(BOTH):
                arrived(col, d, BOTH, BOTH, d)
            done(col, BOTH)

    def unit(col, rel):
        spot = list(at)
        spot[ORDER[col][BOTH]] = _near(at[ORDER[col][BOTH]] + rel)
        return wv_ref.at[(*spot, col)]

    def middle_chunk(col, rel, h):
        spot = list(at)
        spot[ORDER[col][1]] = _near(at[ORDER[col][1]] + rel)
        spot[ORDER[col][BOTH]] = _half(h)
        return wv_ref.at[(*spot, col)]

    def whole_chunk(col, rel, h):
        axis = ORDER[col][0]
        return wv_ref.at[(*_where(axis, _near(at[axis] + rel), _half(h)), col)]

    for rel in WAY[:COLOURS]:
        for col in range(COLOURS):
            copy = hop(BOTH)(BOTH, col, 0, rel - 1, unit(col, 0), unit(col, 0), rel)
            copy.start()
            pending.append(copy)
    for rel in WAY[:COLOURS]:
        for col in range(COLOURS):
            hop(BOTH)(BOTH, col, 0, rel - 1, unit(col, RING - rel), unit(col, RING - rel)).wait_recv()
    gather_phase(1, middle_chunk, lambda col, rel: None)
    gather_phase(0, whole_chunk, hand_on)

    gated_sum.drain()
    other_sum.drain()
    for copy in swaps + pending:
        copy.wait_send()
    for copy, local in outs:
        copy.wait_send()
        local.wait()
    for n, (col, rel) in enumerate((c, r) for c in range(COLOURS) for r in range(RING)):
        axis = ORDER[col][0]
        dst = out_ref.at[(*_where(axis, _near(at[axis] + rel)), 1 - core, col)]
        remote(dst, dst, od_send.at[n], od_recv.at[n], partner).wait_recv()


def sum_step_gather(g, weights, m, v, back):
    vmem, dma = pltpu.VMEM, pltpu.SemaphoreType.DMA
    hbm, local = pl.BlockSpec(memory_space=pl.ANY), pl.BlockSpec(memory_space=vmem)
    cube, sides = (RING, RING, RING), (COLOURS, BOTH, COLOURS)
    scratch = [vmem((SHAPE[name][0] // GROUPS, SHAPE[name][1]), bf16) for name in NAMES]
    for unit in UNITS:
        row = (unit, LANES)
        scratch += [vmem((*sides, BOTH, RING, *row), bf16), vmem((COLOURS, RING, RING, *row), f32), vmem((*sides, BOTH, *row), bf16), vmem((COLOURS, COLOURS, RING, *row), bf16),
                    vmem((COLOURS, RING, *row), f32), vmem((*sides, unit // BOTH, LANES), bf16), vmem((COLOURS, COLOURS, *row), bf16)]
    own, tile, head = (OWN, LANES), (FAMILY, LANES), (TOKENS, HEAD)
    scratch += [vmem((*cube, COLOURS, UNITS[0], LANES), bf16), vmem((*cube, COLOURS, UNITS[0], LANES), bf16), vmem((*cube, BOTH, COLOURS, UNITS[1], LANES), bf16),
                vmem((*cube, COLOURS, UNITS[1], LANES), bf16), vmem((FAMILY, COLOURS * UNITS[0], LANES), bf16), vmem((FAMILY, COLOURS * UNITS[1], LANES), bf16), vmem((FLAT, LANES), f32),
                vmem((RING, 200, LANES), f32), vmem(own, f32), vmem(own, f32), vmem((FAMILY, *own), bf16), vmem((*cube, COLOURS, UNIT, LANES), bf16)]
    scratch += [vmem((n, *tile), f32) for n in (COLOURS, COLOURS, COLOURS, MATRICES)]
    scratch += [vmem((TOKENS, (HEADS + BOTH) * HEAD), bf16), vmem((HEAD, HEADS * BACK), f32), vmem(head, f32), vmem(head, f32), vmem((HEADS, BACK, HEAD), bf16)]
    scratch += [dma((n,)) for n in (162, 162, 24, 24, CHUNKS, MATRICES, 13, 13, 18, 18, CHUNKS, CHUNKS, CHUNKS, CHUNKS, CHUNKS)]
    return pl.pallas_call(
        _comm,
        out_shape=[jax.ShapeDtypeStruct((*cube, BOTH, COLOURS, UNIT, LANES), bf16), jax.ShapeDtypeStruct(own, f32)],
        in_specs=[hbm] * FAMILY + [local] * 23,
        out_specs=[hbm, local],
        scratch_shapes=scratch,
        compiler_params=pltpu.CompilerParams(collective_id=0, has_side_effects=True, vmem_limit_bytes=67043328),
    )(g, *[w.reshape(GROUPS, w.shape[1] // GROUPS, w.shape[BOTH]) for w in weights], *_rows(m), *_rows(v), *back)


PER = RING


def _finish(flat_ref, gq_ref, *rest):
    m_refs, v_refs, w_refs, mo_refs, vo_refs = (rest[i : i + MATRICES] for i in range(0, 35, MATRICES))

    @pl.when(pl.program_id(0) == 0)
    def _():
        for k, (_, blocks, _, own, first) in enumerate(TABLE):
            for j in range(blocks):
                at = _at(k, _lanes(j))
                g = gq_ref[first + j * own : first + (j + 1) * own, :]
                mo_refs[k][at] = 0.9 * m_refs[k][at] + 0.1 * g
                vo_refs[k][at] = 0.95 * v_refs[k][at] + 0.05 * g * g

    for k, (_, blocks, rows, _, _) in enumerate(TABLE):
        lengths = (COLOURS * UNITS[1], GATED) if k < RING else (COLOURS * UNITS[0], 0)
        for j in range(blocks):
            row, to = _flat(k) + j * rows - lengths[1], 0
            while to < rows:
                n, low = row // lengths[0], row % lengths[0]
                some = min(lengths[0] - low, rows - to)
                low += n * COLOURS * UNIT + (COLOURS * UNITS[0] if k < RING else 0)
                for i in range(PER):
                    w_refs[k][0, i * rows + to : i * rows + to + some, _lanes(j)] = flat_ref[i, low : low + some, :]
                row, to = row + some, to + some


def finish(flat, gq, m, v):
    whole = pl.BlockSpec(memory_space=pltpu.VMEM)
    old = [*_rows(m), *_rows(v)]
    shapes = [(1, *SHAPE[name]) for name in NAMES]
    out = pl.pallas_call(
        _finish,
        grid=(GROUPS // PER,),
        out_shape=[jax.ShapeDtypeStruct(shape, jnp.bfloat16) for shape in shapes] + [jax.ShapeDtypeStruct(a.shape, a.dtype) for a in old],
        in_specs=[pl.BlockSpec((PER, FLAT, LANES), lambda i: (i, 0, 0)), whole] + [whole] * 14,
        out_specs=[pl.BlockSpec((1, shape[1] // GROUPS * PER, shape[BOTH]), lambda i: (0, i, 0)) for shape in shapes] + [whole] * 14,
        compiler_params=pltpu.CompilerParams(vmem_limit_bytes=VMEM),
    )(flat.reshape(GROUPS, FLAT, LANES), gq, *old)
    moments = [new.reshape(1, *new.shape) if new.ndim == BOTH else new.transpose(1, 0, BOTH) for new in out[MATRICES:]]
    return (*out[:MATRICES], *moments)


def solution(mesh):
    def step(x, dy, *arrays):
        weights, m, v = (arrays[i : i + MATRICES] for i in (0, MATRICES, 14))
        w = dict(zip(NAMES, weights, strict=True))
        plain = {name: w[name][0] for name in ("wq", "wk", "wv", "wo")}
        a, q, k, value, ot, lse, h = attend(x[0], plain)
        g, dh = gated(h, dy[0], w)
        back = (dh, a, q, k, value, ot, lse, _angles(), plain["wo"])
        flat, gq = sum_step_gather(g.reshape(RING, RING, RING, 2, COLOURS, UNITS[0], LANES), weights, m, v, back)
        return finish(flat, gq, m, v)

    states, all_of, cut = P(("rep", "dp")), P(), P(None, "dp")
    return jax.shard_map(
        step,
        mesh=mesh,
        in_specs=(states, states) + (all_of,) * MATRICES + (cut,) * 14,
        out_specs=(P("rep"),) * MATRICES + (P("rep", "dp"),) * 14,
        check_vma=False,
    )
```
